32 devices in a mesh: dp: 8 (over z, y), rep: 4 (over x, core).
Axes of the slice: x: 2, y: 2, z: 4, core: 2. Of those that a mesh axis runs over, the one named last changes fastest.
Arguments:
- tokens: bfloat16 [32768, 768], P(('dp', 'rep')), may hold values from -6 to 6
- qkv_weight: bfloat16 [768, 2304], P('dp'), may hold values from -0.21875 to 0.21875
- out_weight: bfloat16 [768, 768], P('dp'), may hold values from -0.875 to 0.875
- up_weight: bfloat16 [768, 3072], P('dp'), may hold values from -0.21875 to 0.21875
- down_weight: bfloat16 [3072, 768], P('dp'), may hold values from -0.109375 to 0.109375
- norm_gains: bfloat16 [2, 768], P(None, 'dp'), may hold values from 0.5 to 1.5
- bias_rows: bfloat16 [6, 768], P(None, 'dp'), may hold values from -3 to 3
- ff_bias: bfloat16 [3072], P('dp'), may hold values from -3 to 3
- lengths: int32 [288], replicated, may hold values from 32 to 512, as said below
- owners: int32 [288], replicated, may hold values from 0 to 31, as said below
- cotangent: bfloat16 [32768, 768], P(('dp', 'rep')), may hold values from -6 to 6
Outputs:
- output: bfloat16 [32768, 768], P(('dp', 'rep'))
- grad_tokens: float32 [32768, 768], P(('dp', 'rep'))
- grad_qkv: float32 [768, 2304], P('dp')
- grad_out_weight: float32 [768, 768], P('dp')
- grad_up_weight: float32 [768, 3072], P('dp')
- grad_down_weight: float32 [3072, 768], P('dp')
- grad_norm_gains: float32 [2, 768], P(None, 'dp')
- grad_bias_rows: float32 [6, 768], P(None, 'dp')
- grad_ff_bias: float32 [3072], P('dp')
The draws below stay inside these ranges and needn't reach their ends.
Inputs may be any that keep to these rules, and one draw needn't show every extreme that they name: Passage p holds lengths[p] tokens and belongs to device owners[p]. Every device holds exactly 9 passages, at most one of them longer than 64; a device's passages hold at most 1024 tokens together, and some device's hold exactly 1024. `owners`: each device number appears exactly 9 times.
All inputs are finite; a program needn't handle non-finite values.
Results may differ from the reference program's by a relative error of at most 0.017.
Values may be sent and summed in bfloat16 or wider, within the bound.
A program may use at most 192 MiB of HBM per device.

```python
import jax
import jax.numpy as jnp
from jax import lax

D = 768
HEADS = 12
HD = 64
FF = 3072
LONG = 512
SHORT_HI = 64
PASS_DEV = 9
TOK_DEV = 1024
PASSAGES = 288
TOKENS = 32768
N_DP = 8
N_REP = 4


def passage_table(key):
    device_count = PASSAGES // PASS_DEV
    keys_all = jax.random.split(jax.random.fold_in(key, 7), 4)
    short_len = jax.random.randint(keys_all[0], (device_count, PASS_DEV), SHORT_HI // 2, SHORT_HI + 1)
    long_flag = jax.random.randint(keys_all[1], (device_count,), 0, 2)
    hot_device = jax.random.randint(keys_all[2], (), 0, device_count)
    leading = jnp.where(long_flag == 1, LONG, short_len[:, 0])
    len_table = short_len.at[:, 0].set(leading)
    hot_row = jnp.full((device_count, PASS_DEV), SHORT_HI, jnp.int32).at[:, 0].set(LONG)
    is_hot = (jnp.arange(device_count) == hot_device)[:, None]
    len_table = jnp.where(is_hot, hot_row, len_table)
    placement_order = jax.random.permutation(keys_all[3], PASSAGES)
    return (len_table.reshape(-1), placement_order)


def draw_lengths(key, part):
    flat_table, placement_order = passage_table(key)
    return flat_table[placement_order].astype(jnp.int32)


def draw_owners(key, part):
    flat_table, placement_order = passage_table(key)
    return (placement_order // PASS_DEV).astype(jnp.int32)


def levels(own_key, extent, cuts, smallest, largest):
    gain = 1.0
    for dim, blocks in cuts:
        draws = jax.random.uniform(jax.random.fold_in(jax.random.fold_in(own_key, 6), dim), (blocks,), jnp.float32, smallest / len(cuts), largest / len(cuts))
        gain = gain * jnp.repeat(jnp.exp(draws), extent[dim] // blocks).reshape((-1,) + (1,) * (len(extent) - 1 - dim))
    return gain


def gaussian(own_key, shape, scale, bound, cuts=(), kind=jnp.bfloat16):
    values = scale * jax.random.normal(own_key, shape, jnp.float32)
    if cuts:
        values = values * levels(own_key, shape, cuts, -0.22, 0.18)
    return jnp.clip(values, -bound, bound).astype(kind)


def setup_inputs(seed: int = 0) -> dict:
    seeds = jax.random.split(jax.random.key(seed), 12)
    tokens = gaussian(seeds[0], (TOKENS, D), 1.0, 6.0, ((0, 32),))
    qkv_weight = gaussian(seeds[1], (D, 3 * D), D ** -0.5, 0.21875, ((0, 8),))
    out_weight = gaussian(seeds[2], (D, D), (D // 16) ** -0.5, 0.875, ((0, 8),))
    up_weight = gaussian(seeds[3], (D, FF), D ** -0.5, 0.21875, ((0, 8),))
    down_weight = gaussian(seeds[4], (FF, D), FF ** -0.5, 0.109375, ((0, 8),))
    norm_gains = jnp.clip(1.0 + 0.1 * jax.random.normal(seeds[5], (2, D), jnp.float32), 0.5, 1.5).astype(jnp.bfloat16)
    bias_rows = gaussian(seeds[6], (6, D), 0.5, 3.0, ((1, 8),))
    ff_bias = gaussian(seeds[7], (FF,), 0.5, 3.0, ((0, 8),))
    lengths = draw_lengths(jax.random.fold_in(seeds[11], 71), 0)
    owners = draw_owners(jax.random.fold_in(seeds[11], 71), 0)
    cotangent = gaussian(seeds[10], (TOKENS, D), 1.0, 6.0, ((0, 32),))
    return {"tokens": tokens, "qkv_weight": qkv_weight, "out_weight": out_weight, "up_weight": up_weight, "down_weight": down_weight, "norm_gains": norm_gains, "bias_rows": bias_rows, "ff_bias": ff_bias, "lengths": lengths, "owners": owners, "cotangent": cotangent}


@jax.custom_vjp
def low(v):
    return lax.optimization_barrier(v.astype(jnp.bfloat16)).astype(jnp.float32)

@jax.custom_vjp
def low_back(v):
    return v

def low_keep(v):
    return (low(v), None)

def low_pass(kept, grad):
    return (grad,)

def back_keep(v):
    return (v, None)

def back_low(kept, grad):
    return (low(grad),)
low.defvjp(low_keep, low_pass)
low_back.defvjp(back_keep, back_low)
norm_eps = 1e-06
masked_score = -1000000000.0

def token_segments(lengths, owners, device, row_count):
    own_mask = owners == device
    own_sizes = jnp.where(own_mask, lengths, 0).astype(jnp.int32)
    end_points = jnp.cumsum(own_sizes).astype(jnp.int32)
    start_points = jnp.where(own_mask, end_points - own_sizes, row_count).astype(jnp.int32)
    start_marks = jnp.zeros((row_count + 1,), jnp.int32).at[start_points].add(jnp.ones_like(start_points))
    segment = jnp.cumsum(start_marks[:row_count]).astype(jnp.int32)
    live_rows = jnp.arange(row_count, dtype=jnp.int32) < end_points[-1]
    return (segment, live_rows)

def normalize(residual, gain_row, shift_row):
    center = residual - lax.optimization_barrier(jnp.mean(residual, axis=-1, keepdims=True))
    scale_inv = lax.rsqrt(lax.optimization_barrier(jnp.mean(center * center, axis=-1, keepdims=True)) + norm_eps)
    return center * scale_inv * gain_row + shift_row

def device_attention(pieces):
    queries, keys_all, values_all, segment, live_rows = pieces
    row_count = queries.shape[0]
    query_heads = queries.reshape(row_count, HEADS, HD)
    key_heads = keys_all.reshape(row_count, HEADS, HD)
    value_heads = values_all.reshape(row_count, HEADS, HD)
    scores = jnp.einsum('qhd,khd->hqk', query_heads, key_heads, precision=lax.Precision.HIGHEST) * HD ** (-0.5)
    scores = low_back(scores)
    same_segment = (segment[:, None] == segment[None, :]) & live_rows[:, None] & live_rows[None, :]
    allowed = same_segment | jnp.eye(row_count, dtype=bool)
    scores = jnp.where(allowed[None], scores, masked_score)
    row_max = lax.optimization_barrier(jnp.max(scores, axis=-1, keepdims=True))
    exp_scores = jnp.exp(scores - row_max)
    attn_probs = low(exp_scores / lax.optimization_barrier(jnp.sum(exp_scores, axis=-1, keepdims=True)))
    attended = jnp.einsum('hqk,khd->qhd', attn_probs, value_heads, precision=lax.Precision.HIGHEST)
    return attended.reshape(row_count, D)

def layer_forward(tokens, qkv_weight, out_weight, up_weight, down_weight, norm_gains, bias_rows, ff_bias, segment, live_rows):
    highest = lax.Precision.HIGHEST
    token_count = tokens.shape[0]
    blocks = token_count // TOK_DEV
    zero_bias = jnp.zeros((D,), jnp.float32)
    head_bias = jnp.concatenate([bias_rows[0], zero_bias, bias_rows[1]])
    projected = low_back(low(jnp.dot(tokens, qkv_weight, precision=highest) + head_bias))
    queries = projected[:, :D].reshape(blocks, TOK_DEV, D)
    keys_all = projected[:, D:2 * D].reshape(blocks, TOK_DEV, D)
    values_all = projected[:, 2 * D:].reshape(blocks, TOK_DEV, D)
    mixed_rows = lax.map(jax.checkpoint(device_attention), (queries, keys_all, values_all, segment, live_rows))
    mixed_rows = low_back(low(mixed_rows.reshape(token_count, D)))
    branch = low_back(jnp.dot(mixed_rows, out_weight, precision=highest) + bias_rows[2])
    first_norm = normalize(tokens + branch, norm_gains[0], bias_rows[4])
    inner_pre = low_back(jnp.dot(low(first_norm), up_weight, precision=highest) + ff_bias)
    hidden = low(jax.nn.gelu(inner_pre, approximate=False))
    ffn_out = low_back(jnp.dot(hidden, down_weight, precision=highest) + bias_rows[3])
    live_col = live_rows.reshape(token_count, 1).astype(jnp.float32)
    return normalize(first_norm + ffn_out, norm_gains[1], bias_rows[5]) * live_col

def reference(tokens, qkv_weight, out_weight, up_weight, down_weight, norm_gains, bias_rows, ff_bias, lengths, owners, cotangent):
    device_ids = jnp.arange(N_DP * N_REP, dtype=jnp.int32)
    segment, live_rows = jax.vmap(lambda device: token_segments(lengths, owners, device, TOK_DEV))(device_ids)
    floats = tuple((item.astype(jnp.float32) for item in (tokens, qkv_weight, out_weight, up_weight, down_weight, norm_gains, bias_rows, ff_bias)))

    def forward_fn(*params):
        return layer_forward(*params, segment, live_rows)
    result, pullback = jax.vjp(forward_fn, *floats)
    gradients = pullback(cotangent.astype(jnp.float32))
    return (result.astype(jnp.bfloat16), gradients[0], gradients[1], gradients[2], gradients[3], gradients[4], gradients[5], gradients[6], gradients[7])
```

```python
import functools

import jax
import jax.numpy as jnp
from jax import lax
from jax.experimental import pallas as pl
from jax.experimental.pallas import tpu as pltpu
from jax.sharding import PartitionSpec as P

HEADS = 12
HD = 64
LONG = 512
SHORT = 64
norm_eps = 1e-06
masked_score = -1000000000.0
BF = jnp.bfloat16
F32 = jnp.float32
VMEM_LIMIT = 62 * 1024 * 1024

NN = (((1,), (0,)), ((), ()))
NT = (((1,), (1,)), ((), ()))
TN = (((0,), (0,)), ((), ()))


def dot(a, b, dims=NN):
    return lax.dot_general(a, b, dims, preferred_element_type=F32)


def vm():
    return pl.BlockSpec(memory_space=pltpu.VMEM)


def sm():
    return pl.BlockSpec(memory_space=pltpu.SMEM)


def params(**kw):
    return pltpu.CompilerParams(vmem_limit_bytes=VMEM_LIMIT, **kw)


def place_of():
    dp, rep = lax.axis_index("dp"), lax.axis_index("rep")
    return dp // 2, dp % 2, rep // 2, rep % 2


def peers(z, y, x, c):
    def at(z2, y2, x2, c2):
        return (z2 * 2 + y2, x2 * 2 + c2)

    return (
        [at((z + k) % 4, y, x, c) for k in (1, 2, 3)],
        at(z, 1 - y, x, c),
        at(z, y, 1 - x, c),
        at(z, y, x, 1 - c),
    )


def greet(zs, yp, xp, cp):
    barrier = pltpu.get_barrier_semaphore()
    for peer in (*zs, yp, xp, cp):
        pl.semaphore_signal(barrier, inc=1, device_id=peer, device_id_type=pl.DeviceIdType.MESH)
    pl.semaphore_wait(barrier, 6)


def remote(src, dst, ssem, rsem, peer):
    return pltpu.make_async_remote_copy(
        src_ref=src, dst_ref=dst, send_sem=ssem, recv_sem=rsem,
        device_id=peer, device_id_type=pl.DeviceIdType.MESH,
    )


def wavefront(count, stages):
    for t in range(count + len(stages) - 1):
        for s in range(len(stages) - 1, -1, -1):
            if 0 <= t - s < count:
                stages[s](t - s)


def gather_kernel(n, *refs):
    shards, fulls = refs[:n], refs[n : 2 * n]
    ssem, rsem, lsem = refs[2 * n :]
    z, y, x, c = place_of()
    zs, yp, xp, cp = peers(z, y, x, c)
    greet(zs, yp, xp, cp)
    sent = []

    def go(w, i, src, dst, peer):
        copy = remote(src, dst, ssem.at[w, i], rsem.at[w, i], peer)
        copy.start()
        sent.append(copy)

    def arrive(w, i, ref):
        remote(ref, ref, ssem.at[w, i], rsem.at[w, i], cp).wait_recv()

    def local(w):
        return pltpu.make_async_copy(shards[w], fulls[w].at[z, y], lsem.at[w])

    def near(w):
        local(w).start()
        src = shards[w].at[c, pl.ds(x, 2)]
        dst = fulls[w].at[z, y, c, pl.ds(x, 2)]
        for k in range(3):
            go(w, k, src, dst, zs[k])
        go(w, 3, src, dst, yp)

    def mid(w):
        for k in range(3):
            zk = (z + 3 - k) % 4
            part = fulls[w].at[zk, y, c, pl.ds(x, 2)]
            arrive(w, k, part)
            go(w, 4 + k, part, part, yp)
            q = fulls[w].at[zk, y, c, 2 * x]
            go(w, 7 + k, q, q, xp)

    def far(w):
        for k in range(4):
            zk = (z + 4 - k) % 4
            part = fulls[w].at[zk, 1 - y, c, pl.ds(x, 2)]
            arrive(w, 3 + k, part)
            q = fulls[w].at[zk, 1 - y, c, 2 * x]
            go(w, 10 + k, q, q, xp)

    def across(w):
        for k in range(7):
            zk, yk = ((z + 3 - k) % 4, y) if k < 3 else ((z + 7 - k) % 4, 1 - y)
            arrive(w, 7 + k, fulls[w].at[zk, yk, c, 2 * (1 - x)])
            half = fulls[w].at[zk, yk, c]
            go(w, 14 + k, half, half, cp)

    def last(w):
        for k in range(7):
            zk, yk = ((z + 3 - k) % 4, y) if k < 3 else ((z + 7 - k) % 4, 1 - y)
            arrive(w, 14 + k, fulls[w].at[zk, yk, 1 - c])
        local(w).wait()

    wavefront(n, [near, mid, far, across, last])
    for copy in sent:
        copy.wait_send()


def blocks(shard):
    rows, columns = shard.shape
    return shard.reshape(2, 3, rows // 6, columns)


def gather(shards):
    n = len(shards)
    views = [blocks(s) for s in shards]
    fulls = pl.pallas_call(
        functools.partial(gather_kernel, n),
        out_shape=[jax.ShapeDtypeStruct((4, 2) + v.shape, v.dtype) for v in views],
        in_specs=[vm()] * n,
        out_specs=[pl.BlockSpec(memory_space=pl.ANY)] * n,
        scratch_shapes=[
            pltpu.SemaphoreType.DMA((n, 21)),
            pltpu.SemaphoreType.DMA((n, 21)),
            pltpu.SemaphoreType.DMA((n,)),
        ],
        compiler_params=params(collective_id=0, has_side_effects=True),
        name="gather",
    )(*views)
    return [f.reshape(8 * s.shape[0], s.shape[1]) for f, s in zip(fulls, shards)]


def scatter_kernel(n, *refs):
    grads, outs = refs[:n], refs[n : 2 * n]
    half, rx, rpy, rqy, rpz, rqz, rpx, fin, got = (refs[(2 + i) * n : (3 + i) * n] for i in range(9))
    ssem, rsem = refs[11 * n :]
    z, y, x, c = place_of()
    zs, yp, xp, cp = peers(z, y, x, c)
    greet(zs, yp, xp, cp)
    sent = []

    def go(w, i, src, dst, peer):
        copy = remote(src, dst, ssem.at[w, i], rsem.at[w, i], peer)
        copy.start()
        sent.append(copy)

    def arrive(w, i, ref):
        remote(ref, ref, ssem.at[w, i], rsem.at[w, i], cp).wait_recv()

    def add(*parts):
        total = parts[0].astype(F32)
        for part in parts[1:]:
            total = total + part.astype(F32)
        return total

    def s0(w):
        go(w, 0, grads[w].at[:, :, 1 - c], half[w], cp)

    def s1(w):
        arrive(w, 0, half[w])
        a = half[w]

        @pl.loop(0, 4)
        def _(i):
            for j in range(2):
                for k in range(3):
                    a[i, j, k] = add(grads[w][i, j, c, k], a[i, j, k]).astype(a.dtype)

        go(w, 1, a.at[:, :, 2 * (1 - x)], rx[w], xp)
        go(w, 2, a.at[:, 1 - y, 1], rpy[w], yp)

    def s2(w):
        a = half[w]
        arrive(w, 2, rpy[w])

        @pl.loop(0, 4)
        def _(i):
            a[i, y, 1] = add(a[i, y, 1], rpy[w][i]).astype(a.dtype)

        for k in range(3):
            go(w, 3 + k, a.at[(z + k + 1) % 4, y, 1], rpz[w].at[k], zs[k])
        arrive(w, 1, rx[w])

        @pl.loop(0, 4)
        def _(i):
            for j in range(2):
                a[i, j, 2 * x] = add(a[i, j, 2 * x], rx[w][i, j]).astype(a.dtype)

        go(w, 6, a.at[:, 1 - y, 2 * x], rqy[w], yp)

    def s3(w):
        a = half[w]
        arrive(w, 6, rqy[w])

        @pl.loop(0, 4)
        def _(i):
            a[i, y, 2 * x] = add(a[i, y, 2 * x], rqy[w][i]).astype(a.dtype)

        for k in range(3):
            go(w, 7 + k, a.at[(z + k + 1) % 4, y, 2 * x], rqz[w].at[k], zs[k])
        for k in range(3):
            arrive(w, 3 + k, rpz[w].at[k])
        a[z, y, 1] = add(a[z, y, 1], rpz[w][0], rpz[w][1], rpz[w][2]).astype(a.dtype)
        go(w, 10, a.at[z, y, 1], rpx[w], xp)

    def s4(w):
        a = half[w]
        for k in range(3):
            arrive(w, 7 + k, rqz[w].at[k])
        fin[w][0] = add(a[z, y, 2 * x], rqz[w][0], rqz[w][1], rqz[w][2]).astype(a.dtype)
        go(w, 11, fin[w].at[0], got[w].at[c, 2 * x], xp)
        go(w, 13, fin[w].at[0], got[w].at[c, 2 * x], cp)
        arrive(w, 10, rpx[w])
        fin[w][1] = add(a[z, y, 1], rpx[w][...]).astype(a.dtype)
        go(w, 14, fin[w].at[1], got[w].at[c, 1], cp)

    def s5(w):
        arrive(w, 11, got[w].at[c, 2 * (1 - x)])
        piece = got[w].at[c, 2 * (1 - x)]
        go(w, 12, piece, piece, cp)
        outs[w][c, 2 * x] = fin[w][0].astype(F32)
        outs[w][c, 1] = fin[w][1].astype(F32)
        outs[w][c, 2 * (1 - x)] = got[w][c, 2 * (1 - x)].astype(F32)

    def s6(w):
        arrive(w, 12, got[w].at[1 - c, 2 * (1 - x)])
        arrive(w, 13, got[w].at[1 - c, 2 * x])
        arrive(w, 14, got[w].at[1 - c, 1])
        for k in range(3):
            outs[w][1 - c, k] = got[w][1 - c, k].astype(F32)

    wavefront(n, [s0, s1, s2, s3, s4, s5, s6])
    for copy in sent:
        copy.wait_send()


def scatter(grads):
    n = len(grads)
    views = [g.reshape(4, 2, 2, 3, g.shape[0] // 48, g.shape[1]) for g in grads]
    lead = ((4, 2, 3), (4, 2), (4,), (4,), (3,), (3,), (), (2,), (2, 3))
    scratch = [pltpu.VMEM(s + v.shape[4:], v.dtype) for s in lead for v in views]
    outs = pl.pallas_call(
        functools.partial(scatter_kernel, n),
        out_shape=[jax.ShapeDtypeStruct(v.shape[2:], F32) for v in views],
        in_specs=[vm()] * n,
        out_specs=[vm()] * n,
        scratch_shapes=scratch
        + [pltpu.SemaphoreType.DMA((n, 15)), pltpu.SemaphoreType.DMA((n, 15))],
        compiler_params=params(collective_id=1, has_side_effects=True),
        name="scatter",
    )(*views)
    return [o.reshape(g.shape[0] // 8, g.shape[1]) for o, g in zip(outs, grads)]


def square():
    return lax.axis_size("dp") == 8 and lax.axis_size("rep") == 4


def gather_layer(qkv_weight, out_weight, up_weight, down_weight, norm_gains, bias_rows, ff_bias):
    if not square():
        return (
            lax.all_gather(qkv_weight, "dp", axis=0, tiled=True),
            lax.all_gather(out_weight, "dp", axis=0, tiled=True),
            lax.all_gather(up_weight, "dp", axis=0, tiled=True),
            lax.all_gather(down_weight, "dp", axis=0, tiled=True),
            lax.all_gather(norm_gains, "dp", axis=1, tiled=True),
            lax.all_gather(bias_rows, "dp", axis=1, tiled=True),
            lax.all_gather(ff_bias, "dp", axis=0, tiled=True),
        )
    small = jnp.concatenate([bias_rows.reshape(-1), norm_gains.reshape(-1), ff_bias])
    used = small.shape[0]
    small = jnp.pad(small, (0, 96 * 128 - used)).reshape(96, 128)
    full = gather([small, qkv_weight, out_weight, up_weight, down_weight])
    rows = full[0].reshape(8, 96 * 128)[:, :used]
    nb, ng = bias_rows.size, norm_gains.size
    biases = rows[:, :nb].reshape(8, bias_rows.shape[0], -1).transpose(1, 0, 2)
    gains = rows[:, nb : nb + ng].reshape(8, norm_gains.shape[0], -1).transpose(1, 0, 2)
    return (
        full[1], full[2], full[3], full[4],
        gains.reshape(norm_gains.shape[0], -1),
        biases.reshape(bias_rows.shape[0], -1),
        rows[:, nb + ng :].reshape(-1),
    )


def reduce_layer(d_qkv, d_out, d_up, d_down, d_gains, d_biases, d_up_bias):
    big = [g.astype(BF) for g in (d_down, d_up, d_out, d_qkv)]
    if not square():
        def full(g):
            part = lax.psum_scatter(g, "rep", scatter_dimension=1, tiled=True).astype(F32)
            part = lax.psum_scatter(part, "dp", scatter_dimension=0, tiled=True)
            return lax.all_gather(part.astype(BF), "rep", axis=1, tiled=True).astype(F32)

        down, up, out, qkv = [full(g) for g in big]
        small = lax.psum(
            (
                lax.psum_scatter(d_gains, "dp", scatter_dimension=1, tiled=True),
                lax.psum_scatter(d_biases, "dp", scatter_dimension=1, tiled=True),
                lax.psum_scatter(d_up_bias, "dp", scatter_dimension=0, tiled=True),
            ),
            "rep",
        )
        return (qkv, out, up, down) + small
    def cut(g):
        return g.reshape(g.shape[0], 8, -1).transpose(1, 0, 2).reshape(8, -1)

    parts = [cut(d_gains), cut(d_biases), d_up_bias.reshape(8, -1)]
    small = jnp.concatenate(parts, 1)
    small = jnp.pad(small, ((0, 0), (0, 48 * 128 - small.shape[1]))).reshape(8 * 48, 128)
    down, up, out, qkv, own = scatter(big + [small])
    own = own.reshape(-1)
    n0, n1, n2 = (p.shape[1] for p in parts)
    return (
        qkv, out, up, down,
        own[:n0].reshape(d_gains.shape[0], -1),
        own[n0 : n0 + n1].reshape(d_biases.shape[0], -1),
        own[n0 + n1 : n0 + n1 + n2],
    )


def token_segments(lengths, owners, device, row_count):
    own_mask = owners == device
    own_sizes = jnp.where(own_mask, lengths, 0)
    end_points = jnp.cumsum(own_sizes)
    start_points = jnp.where(own_mask, end_points - own_sizes, row_count)
    start_marks = (
        jnp.zeros((row_count + 1,), jnp.int32).at[start_points].add(jnp.ones_like(start_points))
    )
    segment = jnp.cumsum(start_marks[:row_count])
    live_rows = jnp.arange(row_count, dtype=jnp.int32) < end_points[-1]
    return (segment, live_rows)


def normalize_keep(residual, gain_row, shift_row):
    center = residual - jnp.mean(residual, axis=-1, keepdims=True)
    scale_inv = lax.rsqrt(jnp.mean(center * center, axis=-1, keepdims=True) + norm_eps)
    unit_rows = center * scale_inv
    return (unit_rows * gain_row + shift_row, unit_rows, scale_inv)


def normalize_back(grad_in, unit_rows, scale_inv, gain_row):
    scaled = grad_in * gain_row
    return scale_inv * (
        scaled
        - jnp.mean(scaled, axis=-1, keepdims=True)
        - unit_rows * jnp.mean(scaled * unit_rows, axis=-1, keepdims=True)
    )


def allowed_block(segment, live_rows, row_start, query_block):
    row_count = segment.shape[0]
    stop_row = row_start + query_block
    same_segment = (
        (segment[row_start:stop_row, None] == segment[None, :])
        & live_rows[row_start:stop_row, None]
        & live_rows[None, :]
    )
    self_pair = jnp.arange(query_block)[:, None] + row_start == jnp.arange(row_count)[None, :]
    return (same_segment | self_pair)[None]


def split_pairs(matrix, head_pairs):
    row_count = matrix.shape[0]
    return matrix.reshape(row_count, head_pairs, -1).transpose(1, 0, 2)


def join_pairs(stacked):
    row_count = stacked.shape[1]
    return stacked.transpose(1, 0, 2).reshape(row_count, -1)


def pair_forward(pieces, segment, live_rows, query_block, head_scale):
    queries, keys_pair, values_pair = pieces
    row_count = queries.shape[0]
    head_width = queries.shape[1] // 2
    query_heads = queries.reshape(row_count, 2, head_width)
    key_heads = keys_pair.reshape(row_count, 2, head_width)
    value_heads = values_pair.reshape(row_count, 2, head_width)
    out_blocks = []
    total_blocks = []
    for row_start in range(0, row_count, query_block):
        allowed = allowed_block(segment, live_rows, row_start, query_block)
        scores = (
            jnp.einsum(
                "qhd,khd->hqk",
                query_heads[row_start : row_start + query_block],
                key_heads,
                preferred_element_type=jnp.float32,
            )
            * head_scale
        )
        scores = jnp.where(allowed, scores, masked_score)
        row_max = jnp.max(scores, axis=-1, keepdims=True)
        exp_scores = jnp.exp(scores - row_max)
        row_sum = jnp.sum(exp_scores, axis=-1, keepdims=True)
        attn_probs = (exp_scores / row_sum).astype(jnp.bfloat16)
        attended = jnp.einsum(
            "hqk,khd->qhd", attn_probs, value_heads, preferred_element_type=jnp.float32
        )
        out_blocks.append(attended.reshape(query_block, 2 * head_width))
        total_blocks.append((row_max + jnp.log(row_sum))[:, :, 0])
    return (jnp.concatenate(out_blocks, 0), jnp.concatenate(total_blocks, 1))


def pair_backward(pieces, segment, live_rows, query_block, head_scale):
    queries, keys_pair, values_pair, grad_pair, log_total = pieces
    row_count = queries.shape[0]
    head_width = queries.shape[1] // 2
    query_heads = queries.reshape(row_count, 2, head_width)
    key_heads = keys_pair.reshape(row_count, 2, head_width)
    value_heads = values_pair.reshape(row_count, 2, head_width)
    grad_heads = grad_pair.reshape(row_count, 2, head_width)
    grad_key = jnp.zeros((row_count, 2, head_width), jnp.float32)
    grad_value = jnp.zeros((row_count, 2, head_width), jnp.float32)
    query_grads = []
    for row_start in range(0, row_count, query_block):
        stop_row = row_start + query_block
        query_part = query_heads[row_start:stop_row]
        grad_part = grad_heads[row_start:stop_row]
        allowed = allowed_block(segment, live_rows, row_start, query_block)
        scores = (
            jnp.einsum("qhd,khd->hqk", query_part, key_heads, preferred_element_type=jnp.float32)
            * head_scale
        )
        scores = jnp.where(allowed, scores, masked_score)
        attn_probs = jnp.exp(scores - log_total[:, row_start:stop_row, None])
        grad_probs = jnp.einsum(
            "qhd,khd->hqk", grad_part, value_heads, preferred_element_type=jnp.float32
        )
        grad_scores = (
            attn_probs * (grad_probs - jnp.sum(grad_probs * attn_probs, axis=-1, keepdims=True))
        ).astype(jnp.bfloat16)
        query_grad = (
            jnp.einsum("hqk,khd->qhd", grad_scores, key_heads, preferred_element_type=jnp.float32)
            * head_scale
        )
        query_grads.append(query_grad.reshape(query_block, 2 * head_width))
        grad_key = (
            grad_key
            + jnp.einsum(
                "hqk,qhd->khd", grad_scores, query_part, preferred_element_type=jnp.float32
            )
            * head_scale
        )
        grad_value = grad_value + jnp.einsum(
            "hqk,qhd->khd",
            attn_probs.astype(jnp.bfloat16),
            grad_part,
            preferred_element_type=jnp.float32,
        )
    return (
        jnp.concatenate(query_grads, 0),
        grad_key.reshape(row_count, 2 * head_width),
        grad_value.reshape(row_count, 2 * head_width),
    )


def local(
    tokens,
    qkv_weight,
    out_weight,
    up_weight,
    down_weight,
    norm_gains,
    bias_rows,
    ff_bias,
    lengths,
    owners,
    cotangent,
):
    row_count, model_width = tokens.shape
    device = lax.axis_index("dp") * lax.axis_size("rep") + lax.axis_index("rep")
    segment, live_rows = token_segments(lengths, owners, device, row_count)
    query_block = min(512, row_count)
    head_pairs = HEADS // 2
    head_scale = HD ** (-0.5)
    layer_w = gather_layer(qkv_weight, out_weight, up_weight, down_weight, norm_gains, bias_rows, ff_bias)
    w_qkv, w_out, w_up, w_down, gains_low, biases_low, up_bias_low = layer_w
    gain_rows = gains_low.astype(jnp.float32)
    shift_rows = biases_low.astype(jnp.float32)
    up_bias = up_bias_low.astype(jnp.float32)
    zero_bias = jnp.zeros((model_width,), jnp.float32)
    head_bias = jnp.concatenate([shift_rows[0], zero_bias, shift_rows[1]])
    projected = (jnp.dot(tokens, w_qkv, preferred_element_type=jnp.float32) + head_bias).astype(
        jnp.bfloat16
    )
    queries = split_pairs(projected[:, :model_width], head_pairs)
    keys_all = split_pairs(projected[:, model_width : 2 * model_width], head_pairs)
    values_all = split_pairs(projected[:, 2 * model_width :], head_pairs)

    def attend(pieces):
        return pair_forward(pieces, segment, live_rows, query_block, head_scale)

    mixed_pairs, log_total = lax.map(attend, (queries, keys_all, values_all))
    mixed_rows = join_pairs(mixed_pairs).astype(jnp.bfloat16)
    branch = jnp.dot(mixed_rows, w_out, preferred_element_type=jnp.float32) + shift_rows[2]
    first_norm, unit_one, inv_one = normalize_keep(
        tokens.astype(jnp.float32) + branch, gain_rows[0], shift_rows[4]
    )
    first_low = first_norm.astype(jnp.bfloat16)
    inner_pre = jnp.dot(first_low, w_up, preferred_element_type=jnp.float32) + up_bias
    activated, gelu_pull = jax.vjp(lambda values: jax.nn.gelu(values, approximate=False), inner_pre)
    hidden = activated.astype(jnp.bfloat16)
    ffn_out = jnp.dot(hidden, w_down, preferred_element_type=jnp.float32) + shift_rows[3]
    final_norm, unit_two, inv_two = normalize_keep(
        first_norm + ffn_out, gain_rows[1], shift_rows[5]
    )
    live_col = live_rows.astype(jnp.float32)[:, None]
    output = (final_norm * live_col).astype(jnp.bfloat16)
    grad_out = cotangent.astype(jnp.float32) * live_col
    d_gain_two = jnp.sum(grad_out * unit_two, axis=0)
    d_shift_two = jnp.sum(grad_out, axis=0)
    grad_two = normalize_back(grad_out, unit_two, inv_two, gain_rows[1])
    grad_ffn = grad_two.astype(jnp.bfloat16)
    d_down_bias = jnp.sum(grad_ffn.astype(jnp.float32), axis=0)
    d_down = jnp.einsum("tf,td->fd", hidden, grad_ffn, preferred_element_type=jnp.float32)
    grad_hidden = jnp.einsum("td,fd->tf", grad_ffn, w_down, preferred_element_type=jnp.float32)
    grad_inner = gelu_pull(grad_hidden)[0].astype(jnp.bfloat16)
    d_up_bias = jnp.sum(grad_inner.astype(jnp.float32), axis=0)
    d_up = jnp.einsum("td,tf->df", first_low, grad_inner, preferred_element_type=jnp.float32)
    grad_first = grad_two + jnp.einsum(
        "tf,df->td", grad_inner, w_up, preferred_element_type=jnp.float32
    )
    d_gain_one = jnp.sum(grad_first * unit_one, axis=0)
    d_shift_one = jnp.sum(grad_first, axis=0)
    grad_one = normalize_back(grad_first, unit_one, inv_one, gain_rows[0])
    grad_branch = grad_one.astype(jnp.bfloat16)
    d_out_bias = jnp.sum(grad_branch.astype(jnp.float32), axis=0)
    d_out = jnp.einsum("td,te->de", mixed_rows, grad_branch, preferred_element_type=jnp.float32)
    grad_mixed = jnp.einsum(
        "te,de->td", grad_branch, w_out, preferred_element_type=jnp.float32
    ).astype(jnp.bfloat16)

    def attend_back(pieces):
        return pair_backward(pieces, segment, live_rows, query_block, head_scale)

    grad_query, grad_key, grad_value = lax.map(
        attend_back, (queries, keys_all, values_all, split_pairs(grad_mixed, head_pairs), log_total)
    )
    grad_heads = jnp.concatenate(
        [join_pairs(grad_query), join_pairs(grad_key), join_pairs(grad_value)], 1
    ).astype(jnp.bfloat16)
    d_head_bias = jnp.sum(grad_heads.astype(jnp.float32), axis=0)
    d_qkv = jnp.einsum("td,te->de", tokens, grad_heads, preferred_element_type=jnp.float32)
    grad_tokens = grad_one + jnp.einsum(
        "te,de->td", grad_heads, w_qkv, preferred_element_type=jnp.float32
    )
    d_gains = jnp.stack([d_gain_one, d_gain_two])
    d_biases = jnp.stack(
        [
            d_head_bias[:model_width],
            d_head_bias[2 * model_width :],
            d_out_bias,
            d_down_bias,
            d_shift_one,
            d_shift_two,
        ]
    )
    return (output, grad_tokens) + reduce_layer(d_qkv, d_out, d_up, d_down, d_gains, d_biases, d_up_bias)


def solution(mesh):
    in_specs = (
        P(("dp", "rep"), None),
        P("dp", None),
        P("dp", None),
        P("dp", None),
        P("dp", None),
        P(None, "dp"),
        P(None, "dp"),
        P("dp"),
        P(),
        P(),
        P(("dp", "rep"), None),
    )
    out_specs = (
        P(("dp", "rep"), None),
        P(("dp", "rep"), None),
        P("dp", None),
        P("dp", None),
        P("dp", None),
        P("dp", None),
        P(None, "dp"),
        P(None, "dp"),
        P("dp"),
    )
    return jax.shard_map(local, mesh=mesh, in_specs=in_specs, out_specs=out_specs, check_vma=False)
```

```python
import functools

import jax
import jax.numpy as jnp
from jax import lax
from jax.experimental import pallas as pl
from jax.experimental.pallas import tpu as pltpu
from jax.sharding import PartitionSpec as P

HEADS = 12
HD = 64
LONG = 512
SHORT = 64
norm_eps = 1e-06
masked_score = -1000000000.0
BF = jnp.bfloat16
F32 = jnp.float32
VMEM_LIMIT = 62 * 1024 * 1024

NN = (((1,), (0,)), ((), ()))
NT = (((1,), (1,)), ((), ()))
TN = (((0,), (0,)), ((), ()))


def dot(a, b, dims=NN):
    return lax.dot_general(a, b, dims, preferred_element_type=F32)


def vm():
    return pl.BlockSpec(memory_space=pltpu.VMEM)


def sm():
    return pl.BlockSpec(memory_space=pltpu.SMEM)


def params(**kw):
    return pltpu.CompilerParams(vmem_limit_bytes=VMEM_LIMIT, **kw)


def prep_kernel(per, me_ref, own_ref, len_ref, tok_ref, cot_ref, tok_out, cot_out, tab_ref, wide):
    total = own_ref.shape[0]
    rows = tok_ref.shape[0]
    me = me_ref[0]

    def zero(i, c):
        tab_ref[0, i] = 0
        return c

    lax.fori_loop(0, 128, zero, 0)

    def scan(p, c):
        count, start = c
        hit = own_ref[p] == me
        size = len_ref[p]
        tab_ref[0, count] = start
        tab_ref[0, 16 + count] = size
        return (count + hit.astype(jnp.int32), start + jnp.where(hit, size, 0))

    lax.fori_loop(0, total, scan, (jnp.int32(0), jnp.int32(0)), unroll=8)

    def find(j, c):
        return jnp.where(tab_ref[0, 16 + j] > SHORT, j, c)

    big = lax.fori_loop(0, per, find, jnp.int32(0))

    def place(j, slot):
        is_big = j == big
        tab_ref[0, 32 + j] = jnp.where(is_big, 0, LONG + SHORT * slot)
        tab_ref[0, 48 + j] = jnp.where(is_big, LONG // SHORT, 1)
        at = jnp.where(is_big, 0, slot + 1)
        tab_ref[0, 64 + at] = tab_ref[0, 16 + j]
        return slot + jnp.where(is_big, 0, 1)

    lax.fori_loop(0, per, place, jnp.int32(0))

    for src, dst in ((tok_ref, tok_out), (cot_ref, cot_out)):
        wide[pl.ds(0, rows), :] = src[...].astype(F32)
        wide[pl.ds(rows, LONG + 8), :] = jnp.zeros((LONG + 8, src.shape[1]), F32)

        def passage(j, c):
            start = tab_ref[0, j]
            size = tab_ref[0, 16 + j]
            to = tab_ref[0, 32 + j]

            def chunk(k, c2):
                first = start + k * SHORT
                shift = first % 8
                piece = wide[pl.ds(pl.multiple_of(first - shift, 8), SHORT + 8), :]
                piece = pltpu.roll(piece, (SHORT + 8 - shift) % (SHORT + 8), 0)[:SHORT]
                row = lax.broadcasted_iota(jnp.int32, piece.shape, 0) + k * SHORT
                dst[pl.ds(pl.multiple_of(to + k * SHORT, SHORT), SHORT), :] = jnp.where(
                    row < size, piece, 0.0
                ).astype(BF)
                return c2

            return lax.fori_loop(0, tab_ref[0, 48 + j], chunk, c)

        lax.fori_loop(0, per, passage, 0)


def prep(me, owners, lengths, tokens, cotangent, per):
    rows, width = tokens.shape
    return pl.pallas_call(
        functools.partial(prep_kernel, per),
        out_shape=(
            jax.ShapeDtypeStruct((rows, width), BF),
            jax.ShapeDtypeStruct((rows, width), BF),
            jax.ShapeDtypeStruct((1, 128), jnp.int32),
        ),
        in_specs=[sm(), sm(), sm(), vm(), vm()],
        out_specs=(vm(), vm(), sm()),
        scratch_shapes=[pltpu.VMEM((rows + LONG + 8, width), F32)],
        compiler_params=params(),
        name="prep",
    )(me, owners, lengths, tokens, cotangent)


def unperm_rows(per, tab_ref, src_ref, wide, mask):
    rows = src_ref.shape[0]
    wide[...] = jnp.zeros_like(wide)

    def passage(j, c):
        start = tab_ref[0, j]
        size = tab_ref[0, 16 + j]
        frm = tab_ref[0, 32 + j]

        def chunk(k, c2):
            piece = src_ref[pl.ds(pl.multiple_of(frm + k * SHORT, SHORT), SHORT), :].astype(F32)
            row = lax.broadcasted_iota(jnp.int32, piece.shape, 0) + k * SHORT
            first = start + k * SHORT
            shift = first % 8
            at = pl.ds(pl.multiple_of(first - shift, 8), SHORT + 8)
            piece = jnp.where(row < size, piece, 0.0)
            piece = jnp.concatenate([piece, jnp.zeros((8, piece.shape[1]), F32)], 0)
            piece = pltpu.roll(piece, shift, 0)
            row = lax.broadcasted_iota(jnp.int32, piece.shape, 0)
            wide[at, :] = jnp.where(row >= shift, piece, wide[at, :])
            return c2

        return lax.fori_loop(0, tab_ref[0, 48 + j], chunk, c)

    lax.fori_loop(0, per, passage, 0)


def unperm_kernel(per, tab_ref, src_ref, out_ref, wide):
    unperm_rows(per, tab_ref, src_ref, wide, True)
    out_ref[...] = wide[pl.ds(0, src_ref.shape[0]), :].astype(out_ref.dtype)


def unperm(tab, src, per):
    rows, width = src.shape
    return pl.pallas_call(
        functools.partial(unperm_kernel, per),
        out_shape=jax.ShapeDtypeStruct((rows, width), src.dtype),
        in_specs=[sm(), vm()],
        out_specs=vm(),
        scratch_shapes=[pltpu.VMEM((rows + LONG + 8, width), F32)],
        compiler_params=params(),
        name="unperm",
    )(tab, src)


def place_of():
    dp, rep = lax.axis_index("dp"), lax.axis_index("rep")
    return dp // 2, dp % 2, rep // 2, rep % 2


def peers(z, y, x, c):
    def at(z2, y2, x2, c2):
        return (z2 * 2 + y2, x2 * 2 + c2)

    return (
        [at((z + k) % 4, y, x, c) for k in (1, 2, 3)],
        at(z, 1 - y, x, c),
        at(z, y, 1 - x, c),
        at(z, y, x, 1 - c),
    )


def greet(zs, yp, xp, cp):
    barrier = pltpu.get_barrier_semaphore()
    for peer in (*zs, yp, xp, cp):
        pl.semaphore_signal(barrier, inc=1, device_id=peer, device_id_type=pl.DeviceIdType.MESH)
    pl.semaphore_wait(barrier, 6)


def remote(src, dst, ssem, rsem, peer):
    return pltpu.make_async_remote_copy(
        src_ref=src, dst_ref=dst, send_sem=ssem, recv_sem=rsem,
        device_id=peer, device_id_type=pl.DeviceIdType.MESH,
    )


def wavefront(count, stages):
    for t in range(count + len(stages) - 1):
        for s in range(len(stages) - 1, -1, -1):
            if 0 <= t - s < count:
                stages[s](t - s)


def gather_kernel(n, *refs):
    shards, fulls = refs[:n], refs[n : 2 * n]
    ssem, rsem, lsem = refs[2 * n :]
    z, y, x, c = place_of()
    zs, yp, xp, cp = peers(z, y, x, c)
    greet(zs, yp, xp, cp)
    sent = []

    def go(w, i, src, dst, peer):
        copy = remote(src, dst, ssem.at[w, i], rsem.at[w, i], peer)
        copy.start()
        sent.append(copy)

    def arrive(w, i, ref):
        remote(ref, ref, ssem.at[w, i], rsem.at[w, i], cp).wait_recv()

    def local(w):
        return pltpu.make_async_copy(shards[w], fulls[w].at[z, y], lsem.at[w])

    def near(w):
        local(w).start()
        src = shards[w].at[c, pl.ds(x, 2)]
        dst = fulls[w].at[z, y, c, pl.ds(x, 2)]
        for k in range(3):
            go(w, k, src, dst, zs[k])
        go(w, 3, src, dst, yp)

    def mid(w):
        for k in range(3):
            zk = (z + 3 - k) % 4
            part = fulls[w].at[zk, y, c, pl.ds(x, 2)]
            arrive(w, k, part)
            go(w, 4 + k, part, part, yp)
            q = fulls[w].at[zk, y, c, 2 * x]
            go(w, 7 + k, q, q, xp)

    def far(w):
        for k in range(4):
            zk = (z + 4 - k) % 4
            part = fulls[w].at[zk, 1 - y, c, pl.ds(x, 2)]
            arrive(w, 3 + k, part)
            q = fulls[w].at[zk, 1 - y, c, 2 * x]
            go(w, 10 + k, q, q, xp)

    def across(w):
        for k in range(7):
            zk, yk = ((z + 3 - k) % 4, y) if k < 3 else ((z + 7 - k) % 4, 1 - y)
            arrive(w, 7 + k, fulls[w].at[zk, yk, c, 2 * (1 - x)])
            half = fulls[w].at[zk, yk, c]
            go(w, 14 + k, half, half, cp)

    def last(w):
        for k in range(7):
            zk, yk = ((z + 3 - k) % 4, y) if k < 3 else ((z + 7 - k) % 4, 1 - y)
            arrive(w, 14 + k, fulls[w].at[zk, yk, 1 - c])
        local(w).wait()

    wavefront(n, [near, mid, far, across, last])
    for copy in sent:
        copy.wait_send()


def blocks(shard):
    rows, columns = shard.shape
    return shard.reshape(2, 3, rows // 6, columns)


def gather(shards):
    n = len(shards)
    views = [blocks(s) for s in shards]
    fulls = pl.pallas_call(
        functools.partial(gather_kernel, n),
        out_shape=[jax.ShapeDtypeStruct((4, 2) + v.shape, v.dtype) for v in views],
        in_specs=[vm()] * n,
        out_specs=[pl.BlockSpec(memory_space=pl.ANY)] * n,
        scratch_shapes=[
            pltpu.SemaphoreType.DMA((n, 21)),
            pltpu.SemaphoreType.DMA((n, 21)),
            pltpu.SemaphoreType.DMA((n,)),
        ],
        compiler_params=params(collective_id=0, has_side_effects=True),
        name="gather",
    )(*views)
    return [f.reshape(8 * s.shape[0], s.shape[1]) for f, s in zip(fulls, shards)]


def scatter_kernel(n, *refs):
    grads, outs = refs[:n], refs[n : 2 * n]
    half, rx, rpy, rqy, rpz, rqz, rpx, fin, got = (refs[(2 + i) * n : (3 + i) * n] for i in range(9))
    ssem, rsem = refs[11 * n :]
    z, y, x, c = place_of()
    zs, yp, xp, cp = peers(z, y, x, c)
    greet(zs, yp, xp, cp)
    sent = []

    def go(w, i, src, dst, peer):
        copy = remote(src, dst, ssem.at[w, i], rsem.at[w, i], peer)
        copy.start()
        sent.append(copy)

    def arrive(w, i, ref):
        remote(ref, ref, ssem.at[w, i], rsem.at[w, i], cp).wait_recv()

    def add(*parts):
        total = parts[0].astype(F32)
        for part in parts[1:]:
            total = total + part.astype(F32)
        return total

    def s0(w):
        go(w, 0, grads[w].at[:, :, 1 - c], half[w], cp)

    def s1(w):
        arrive(w, 0, half[w])
        a = half[w]

        @pl.loop(0, 4)
        def _(i):
            for j in range(2):
                for k in range(3):
                    a[i, j, k] = add(grads[w][i, j, c, k], a[i, j, k]).astype(a.dtype)

        go(w, 1, a.at[:, :, 2 * (1 - x)], rx[w], xp)
        go(w, 2, a.at[:, 1 - y, 1], rpy[w], yp)

    def s2(w):
        a = half[w]
        arrive(w, 2, rpy[w])

        @pl.loop(0, 4)
        def _(i):
            a[i, y, 1] = add(a[i, y, 1], rpy[w][i]).astype(a.dtype)

        for k in range(3):
            go(w, 3 + k, a.at[(z + k + 1) % 4, y, 1], rpz[w].at[k], zs[k])
        arrive(w, 1, rx[w])

        @pl.loop(0, 4)
        def _(i):
            for j in range(2):
                a[i, j, 2 * x] = add(a[i, j, 2 * x], rx[w][i, j]).astype(a.dtype)

        go(w, 6, a.at[:, 1 - y, 2 * x], rqy[w], yp)

    def s3(w):
        a = half[w]
        arrive(w, 6, rqy[w])

        @pl.loop(0, 4)
        def _(i):
            a[i, y, 2 * x] = add(a[i, y, 2 * x], rqy[w][i]).astype(a.dtype)

        for k in range(3):
            go(w, 7 + k, a.at[(z + k + 1) % 4, y, 2 * x], rqz[w].at[k], zs[k])
        for k in range(3):
            arrive(w, 3 + k, rpz[w].at[k])
        a[z, y, 1] = add(a[z, y, 1], rpz[w][0], rpz[w][1], rpz[w][2]).astype(a.dtype)
        go(w, 10, a.at[z, y, 1], rpx[w], xp)

    def s4(w):
        a = half[w]
        for k in range(3):
            arrive(w, 7 + k, rqz[w].at[k])
        fin[w][0] = add(a[z, y, 2 * x], rqz[w][0], rqz[w][1], rqz[w][2]).astype(a.dtype)
        go(w, 11, fin[w].at[0], got[w].at[c, 2 * x], xp)
        go(w, 13, fin[w].at[0], got[w].at[c, 2 * x], cp)
        arrive(w, 10, rpx[w])
        fin[w][1] = add(a[z, y, 1], rpx[w][...]).astype(a.dtype)
        go(w, 14, fin[w].at[1], got[w].at[c, 1], cp)

    def s5(w):
        arrive(w, 11, got[w].at[c, 2 * (1 - x)])
        piece = got[w].at[c, 2 * (1 - x)]
        go(w, 12, piece, piece, cp)
        outs[w][c, 2 * x] = fin[w][0].astype(F32)
        outs[w][c, 1] = fin[w][1].astype(F32)
        outs[w][c, 2 * (1 - x)] = got[w][c, 2 * (1 - x)].astype(F32)

    def s6(w):
        arrive(w, 12, got[w].at[1 - c, 2 * (1 - x)])
        arrive(w, 13, got[w].at[1 - c, 2 * x])
        arrive(w, 14, got[w].at[1 - c, 1])
        for k in range(3):
            outs[w][1 - c, k] = got[w][1 - c, k].astype(F32)

    wavefront(n, [s0, s1, s2, s3, s4, s5, s6])
    for copy in sent:
        copy.wait_send()


def scatter(grads):
    n = len(grads)
    views = [g.reshape(4, 2, 2, 3, g.shape[0] // 48, g.shape[1]) for g in grads]
    lead = ((4, 2, 3), (4, 2), (4,), (4,), (3,), (3,), (), (2,), (2, 3))
    scratch = [pltpu.VMEM(s + v.shape[4:], v.dtype) for s in lead for v in views]
    outs = pl.pallas_call(
        functools.partial(scatter_kernel, n),
        out_shape=[jax.ShapeDtypeStruct(v.shape[2:], F32) for v in views],
        in_specs=[vm()] * n,
        out_specs=[vm()] * n,
        scratch_shapes=scratch
        + [pltpu.SemaphoreType.DMA((n, 15)), pltpu.SemaphoreType.DMA((n, 15))],
        compiler_params=params(collective_id=1, has_side_effects=True),
        name="scatter",
    )(*views)
    return [o.reshape(g.shape[0] // 8, g.shape[1]) for o, g in zip(outs, grads)]


def head_lanes(block, head):
    lane = lax.broadcasted_iota(jnp.int32, (1, block.shape[1]), 1)
    keep = jnp.where(lane >= HD, float(head), 1.0 - head)
    return block * keep.astype(BF)


def softmax_keys(scores, valid):
    scores = jnp.where(valid, scores, masked_score)
    weights = jnp.exp(scores - jnp.max(scores, axis=0, keepdims=True))
    return weights * (1.0 / jnp.sum(weights, axis=0, keepdims=True))


def short_valid(tab_ref, pair, size):
    key = lax.broadcasted_iota(jnp.int32, (size, size), 0)
    query = lax.broadcasted_iota(jnp.int32, (size, size), 1)
    low, high = tab_ref[0, 65 + 2 * pair], tab_ref[0, 66 + 2 * pair]
    bound = jnp.where(key >= SHORT, SHORT + high, low)
    return (key < bound) & (key // SHORT == query // SHORT)


def attend_kernel(scale, tab_ref, q_ref, k_ref, v_ref, out_ref, long_ref, short_ref):
    two = 2 * SHORT
    key = lax.broadcasted_iota(jnp.int32, (LONG, LONG), 0)
    valid = key < tab_ref[0, 64]
    shorts = (q_ref.shape[0] - LONG) // two
    keeps = [short_valid(tab_ref, b, two) for b in range(shorts)]
    total = None
    tails = [None] * shorts
    for h in range(2):
        scores = dot(head_lanes(k_ref[0:LONG], h), q_ref[0:LONG], NT) * scale
        probs = softmax_keys(scores, valid).astype(BF)
        long_ref[h] = probs
        part = dot(probs, head_lanes(v_ref[0:LONG], h), TN)
        total = part if total is None else total + part
        for b in range(shorts):
            rows = slice(LONG + b * two, LONG + (b + 1) * two)
            scores = dot(head_lanes(k_ref[rows], h), q_ref[rows], NT) * scale
            probs = softmax_keys(scores, keeps[b]).astype(BF)
            short_ref[h, b * two : (b + 1) * two] = probs
            part = dot(probs, head_lanes(v_ref[rows], h), TN)
            tails[b] = part if tails[b] is None else tails[b] + part
    out_ref[0:LONG] = total.astype(BF)
    for b in range(shorts):
        out_ref[LONG + b * two : LONG + (b + 1) * two] = tails[b].astype(BF)


def attend(tab, projected):
    rows, wide = projected.shape
    width = wide // 3
    pairs = width // (2 * HD)
    column = lambda off: pl.BlockSpec((rows, 2 * HD), lambda i, off=off: (0, off + i))
    return pl.pallas_call(
        functools.partial(attend_kernel, HD ** (-0.5)),
        grid=(pairs,),
        out_shape=(
            jax.ShapeDtypeStruct((rows, width), BF),
            jax.ShapeDtypeStruct((2 * pairs, LONG, LONG), BF),
            jax.ShapeDtypeStruct((2 * pairs, rows - LONG, 2 * SHORT), BF),
        ),
        in_specs=[sm(), column(0), column(pairs), column(2 * pairs)],
        out_specs=(
            column(0),
            pl.BlockSpec((2, LONG, LONG), lambda i: (i, 0, 0)),
            pl.BlockSpec((2, rows - LONG, 2 * SHORT), lambda i: (i, 0, 0)),
        ),
        compiler_params=params(),
        name="attend",
    )(tab, projected, projected, projected)


def attend_back_kernel(scale, q_ref, k_ref, v_ref, g_ref, long_ref, short_ref, out_ref):
    two = 2 * SHORT
    shorts = (q_ref.shape[0] - LONG) // two
    spans = [(slice(0, LONG), None)]
    spans += [(slice(LONG + b * two, LONG + (b + 1) * two), b) for b in range(shorts)]
    for rows, b in spans:
        sums = None
        for h in range(2):
            probs = long_ref[h] if b is None else short_ref[h, b * two : (b + 1) * two]
            grad = head_lanes(g_ref[rows], h)
            wide = probs.astype(F32)
            grad_probs = dot(v_ref[rows], grad, NT)
            mean = jnp.sum(grad_probs * wide, axis=0, keepdims=True)
            grad_scores = (wide * (grad_probs - mean)).astype(BF)
            parts = (
                dot(grad_scores, head_lanes(k_ref[rows], h), TN),
                dot(grad_scores, head_lanes(q_ref[rows], h)),
                dot(probs, grad),
            )
            sums = parts if sums is None else tuple(a + p for a, p in zip(sums, parts))
        out_ref[0, rows] = (sums[0] * scale).astype(BF)
        out_ref[1, rows] = (sums[1] * scale).astype(BF)
        out_ref[2, rows] = sums[2].astype(BF)


def attend_back(projected, grad_mixed, long_probs, short_probs):
    rows, wide = projected.shape
    width = wide // 3
    pairs = width // (2 * HD)
    column = lambda off: pl.BlockSpec((rows, 2 * HD), lambda i, off=off: (0, off + i))
    return pl.pallas_call(
        functools.partial(attend_back_kernel, HD ** (-0.5)),
        grid=(pairs,),
        out_shape=jax.ShapeDtypeStruct((3, rows, width), BF),
        in_specs=[
            column(0), column(pairs), column(2 * pairs), column(0),
            pl.BlockSpec((2, LONG, LONG), lambda i: (i, 0, 0)),
            pl.BlockSpec((2, rows - LONG, 2 * SHORT), lambda i: (i, 0, 0)),
        ],
        out_specs=pl.BlockSpec((3, rows, 2 * HD), lambda i: (0, 0, i)),
        compiler_params=params(),
        name="attend_back",
    )(projected, projected, projected, grad_mixed, long_probs, short_probs)


def square():
    return lax.axis_size("dp") == 8 and lax.axis_size("rep") == 4


def gather_layer(qkv_weight, out_weight, up_weight, down_weight, norm_gains, bias_rows, ff_bias):
    if not square():
        return (
            lax.all_gather(qkv_weight, "dp", axis=0, tiled=True),
            lax.all_gather(out_weight, "dp", axis=0, tiled=True),
            lax.all_gather(up_weight, "dp", axis=0, tiled=True),
            lax.all_gather(down_weight, "dp", axis=0, tiled=True),
            lax.all_gather(norm_gains, "dp", axis=1, tiled=True),
            lax.all_gather(bias_rows, "dp", axis=1, tiled=True),
            lax.all_gather(ff_bias, "dp", axis=0, tiled=True),
        )
    small = jnp.concatenate([bias_rows.reshape(-1), norm_gains.reshape(-1), ff_bias])
    used = small.shape[0]
    small = jnp.pad(small, (0, 96 * 128 - used)).reshape(96, 128)
    full = gather([small, qkv_weight, out_weight, up_weight, down_weight])
    rows = full[0].reshape(8, 96 * 128)[:, :used]
    nb, ng = bias_rows.size, norm_gains.size
    biases = rows[:, :nb].reshape(8, bias_rows.shape[0], -1).transpose(1, 0, 2)
    gains = rows[:, nb : nb + ng].reshape(8, norm_gains.shape[0], -1).transpose(1, 0, 2)
    return (
        full[1], full[2], full[3], full[4],
        gains.reshape(norm_gains.shape[0], -1),
        biases.reshape(bias_rows.shape[0], -1),
        rows[:, nb + ng :].reshape(-1),
    )


def reduce_layer(d_qkv, d_out, d_up, d_down, d_gains, d_biases, d_up_bias):
    big = [g.astype(BF) for g in (d_down, d_up, d_out, d_qkv)]
    if not square():
        def full(g):
            part = lax.psum_scatter(g, "rep", scatter_dimension=1, tiled=True).astype(F32)
            part = lax.psum_scatter(part, "dp", scatter_dimension=0, tiled=True)
            return lax.all_gather(part.astype(BF), "rep", axis=1, tiled=True).astype(F32)

        down, up, out, qkv = [full(g) for g in big]
        small = lax.psum(
            (
                lax.psum_scatter(d_gains, "dp", scatter_dimension=1, tiled=True),
                lax.psum_scatter(d_biases, "dp", scatter_dimension=1, tiled=True),
                lax.psum_scatter(d_up_bias, "dp", scatter_dimension=0, tiled=True),
            ),
            "rep",
        )
        return (qkv, out, up, down) + small
    def cut(g):
        return g.reshape(g.shape[0], 8, -1).transpose(1, 0, 2).reshape(8, -1)

    parts = [cut(d_gains), cut(d_biases), d_up_bias.reshape(8, -1)]
    small = jnp.concatenate(parts, 1)
    small = jnp.pad(small, ((0, 0), (0, 48 * 128 - small.shape[1]))).reshape(8 * 48, 128)
    down, up, out, qkv, own = scatter(big + [small])
    own = own.reshape(-1)
    n0, n1, n2 = (p.shape[1] for p in parts)
    return (
        qkv, out, up, down,
        own[:n0].reshape(d_gains.shape[0], -1),
        own[n0 : n0 + n1].reshape(d_biases.shape[0], -1),
        own[n0 + n1 : n0 + n1 + n2],
    )


def normalize_keep(residual, gain_row, shift_row):
    center = residual - jnp.mean(residual, axis=-1, keepdims=True)
    scale_inv = lax.rsqrt(jnp.mean(center * center, axis=-1, keepdims=True) + norm_eps)
    unit_rows = center * scale_inv
    return (unit_rows * gain_row + shift_row, unit_rows, scale_inv)


def normalize_back(grad_in, unit_rows, scale_inv, gain_row):
    scaled = grad_in * gain_row
    return scale_inv * (
        scaled
        - jnp.mean(scaled, axis=-1, keepdims=True)
        - unit_rows * jnp.mean(scaled * unit_rows, axis=-1, keepdims=True)
    )


def local(
    tokens,
    qkv_weight,
    out_weight,
    up_weight,
    down_weight,
    norm_gains,
    bias_rows,
    ff_bias,
    lengths,
    owners,
    cotangent,
):
    row_count, model_width = tokens.shape
    device = lax.axis_index("dp") * lax.axis_size("rep") + lax.axis_index("rep")
    devices = lax.axis_size("dp") * lax.axis_size("rep")
    per = lengths.shape[0] // devices
    assert row_count == LONG + SHORT * (per - 1)
    me = device.astype(jnp.int32).reshape(1)
    tokens, cotangent, tab = prep(me, owners, lengths, tokens, cotangent, per)
    layer_w = gather_layer(qkv_weight, out_weight, up_weight, down_weight, norm_gains, bias_rows, ff_bias)
    w_qkv, w_out, w_up, w_down, gains_low, biases_low, up_bias_low = layer_w
    gain_rows = gains_low.astype(jnp.float32)
    shift_rows = biases_low.astype(jnp.float32)
    up_bias = up_bias_low.astype(jnp.float32)
    zero_bias = jnp.zeros((model_width,), jnp.float32)
    head_bias = jnp.concatenate([shift_rows[0], zero_bias, shift_rows[1]])
    projected = (jnp.dot(tokens, w_qkv, preferred_element_type=jnp.float32) + head_bias).astype(
        jnp.bfloat16
    )
    mixed_rows, long_probs, short_probs = attend(tab, projected)
    branch = jnp.dot(mixed_rows, w_out, preferred_element_type=jnp.float32) + shift_rows[2]
    first_norm, unit_one, inv_one = normalize_keep(
        tokens.astype(jnp.float32) + branch, gain_rows[0], shift_rows[4]
    )
    first_low = first_norm.astype(jnp.bfloat16)
    inner_pre = jnp.dot(first_low, w_up, preferred_element_type=jnp.float32) + up_bias
    activated, gelu_pull = jax.vjp(lambda values: jax.nn.gelu(values, approximate=False), inner_pre)
    hidden = activated.astype(jnp.bfloat16)
    ffn_out = jnp.dot(hidden, w_down, preferred_element_type=jnp.float32) + shift_rows[3]
    final_norm, unit_two, inv_two = normalize_keep(
        first_norm + ffn_out, gain_rows[1], shift_rows[5]
    )
    output = unperm(tab, final_norm.astype(BF), per)
    grad_out = cotangent.astype(jnp.float32)
    d_gain_two = jnp.sum(grad_out * unit_two, axis=0)
    d_shift_two = jnp.sum(grad_out, axis=0)
    grad_two = normalize_back(grad_out, unit_two, inv_two, gain_rows[1])
    grad_ffn = grad_two.astype(jnp.bfloat16)
    d_down_bias = jnp.sum(grad_ffn.astype(jnp.float32), axis=0)
    d_down = jnp.einsum("tf,td->fd", hidden, grad_ffn, preferred_element_type=jnp.float32)
    grad_hidden = jnp.einsum("td,fd->tf", grad_ffn, w_down, preferred_element_type=jnp.float32)
    grad_inner = gelu_pull(grad_hidden)[0].astype(jnp.bfloat16)
    d_up_bias = jnp.sum(grad_inner.astype(jnp.float32), axis=0)
    d_up = jnp.einsum("td,tf->df", first_low, grad_inner, preferred_element_type=jnp.float32)
    grad_first = grad_two + jnp.einsum(
        "tf,df->td", grad_inner, w_up, preferred_element_type=jnp.float32
    )
    d_gain_one = jnp.sum(grad_first * unit_one, axis=0)
    d_shift_one = jnp.sum(grad_first, axis=0)
    grad_one = normalize_back(grad_first, unit_one, inv_one, gain_rows[0])
    grad_branch = grad_one.astype(jnp.bfloat16)
    d_out_bias = jnp.sum(grad_branch.astype(jnp.float32), axis=0)
    d_out = jnp.einsum("td,te->de", mixed_rows, grad_branch, preferred_element_type=jnp.float32)
    grad_mixed = jnp.einsum(
        "te,de->td", grad_branch, w_out, preferred_element_type=jnp.float32
    ).astype(jnp.bfloat16)

    parts = attend_back(projected, grad_mixed, long_probs, short_probs)
    grad_heads = jnp.concatenate([parts[0], parts[1], parts[2]], 1)
    d_head_bias = jnp.sum(grad_heads.astype(jnp.float32), axis=0)
    d_qkv = jnp.einsum("td,te->de", tokens, grad_heads, preferred_element_type=jnp.float32)
    grad_tokens = grad_one + jnp.einsum(
        "te,de->td", grad_heads, w_qkv, preferred_element_type=jnp.float32
    )
    grad_tokens = unperm(tab, grad_tokens, per)
    d_gains = jnp.stack([d_gain_one, d_gain_two])
    d_biases = jnp.stack(
        [
            d_head_bias[:model_width],
            d_head_bias[2 * model_width :],
            d_out_bias,
            d_down_bias,
            d_shift_one,
            d_shift_two,
        ]
    )
    return (output, grad_tokens) + reduce_layer(d_qkv, d_out, d_up, d_down, d_gains, d_biases, d_up_bias)


def solution(mesh):
    in_specs = (
        P(("dp", "rep"), None),
        P("dp", None),
        P("dp", None),
        P("dp", None),
        P("dp", None),
        P(None, "dp"),
        P(None, "dp"),
        P("dp"),
        P(),
        P(),
        P(("dp", "rep"), None),
    )
    out_specs = (
        P(("dp", "rep"), None),
        P(("dp", "rep"), None),
        P("dp", None),
        P("dp", None),
        P("dp", None),
        P("dp", None),
        P(None, "dp"),
        P(None, "dp"),
        P("dp"),
    )
    return jax.shard_map(local, mesh=mesh, in_specs=in_specs, out_specs=out_specs, check_vma=False)
```

```python
import functools

import jax
import jax.numpy as jnp
from jax import lax
from jax.experimental import pallas as pl
from jax.experimental.pallas import tpu as pltpu
from jax.sharding import PartitionSpec as P

HEADS = 12
HD = 64
LONG = 512
SHORT = 64
norm_eps = 1e-06
masked_score = -1000000000.0
BF = jnp.bfloat16
F32 = jnp.float32
VMEM_LIMIT = 62 * 1024 * 1024

NN = (((1,), (0,)), ((), ()))
NT = (((1,), (1,)), ((), ()))
TN = (((0,), (0,)), ((), ()))


def dot(a, b, dims=NN):
    return lax.dot_general(a, b, dims, preferred_element_type=F32)


def vm():
    return pl.BlockSpec(memory_space=pltpu.VMEM)


def sm():
    return pl.BlockSpec(memory_space=pltpu.SMEM)


def params(**kw):
    return pltpu.CompilerParams(vmem_limit_bytes=VMEM_LIMIT, **kw)


def prep_kernel(per, me_ref, own_ref, len_ref, tok_ref, cot_ref, tok_out, cot_out, tab_ref, wide):
    total = own_ref.shape[0]
    rows = tok_ref.shape[0]
    me = me_ref[0]

    def zero(i, c):
        tab_ref[0, i] = 0
        return c

    lax.fori_loop(0, 128, zero, 0)

    def scan(p, c):
        count, start = c
        hit = own_ref[p] == me
        size = len_ref[p]
        tab_ref[0, count] = start
        tab_ref[0, 16 + count] = size
        return (count + hit.astype(jnp.int32), start + jnp.where(hit, size, 0))

    lax.fori_loop(0, total, scan, (jnp.int32(0), jnp.int32(0)), unroll=8)

    def find(j, c):
        return jnp.where(tab_ref[0, 16 + j] > SHORT, j, c)

    big = lax.fori_loop(0, per, find, jnp.int32(0))

    def place(j, slot):
        is_big = j == big
        tab_ref[0, 32 + j] = jnp.where(is_big, 0, LONG + SHORT * slot)
        tab_ref[0, 48 + j] = jnp.where(is_big, LONG // SHORT, 1)
        at = jnp.where(is_big, 0, slot + 1)
        tab_ref[0, 64 + at] = tab_ref[0, 16 + j]
        return slot + jnp.where(is_big, 0, 1)

    lax.fori_loop(0, per, place, jnp.int32(0))

    for src, dst in ((tok_ref, tok_out), (cot_ref, cot_out)):
        wide[pl.ds(0, rows), :] = src[...].astype(F32)
        wide[pl.ds(rows, LONG + 8), :] = jnp.zeros((LONG + 8, src.shape[1]), F32)

        def passage(j, c):
            start = tab_ref[0, j]
            size = tab_ref[0, 16 + j]
            to = tab_ref[0, 32 + j]

            def chunk(k, c2):
                first = start + k * SHORT
                shift = first % 8
                piece = wide[pl.ds(pl.multiple_of(first - shift, 8), SHORT + 8), :]
                piece = pltpu.roll(piece, (SHORT + 8 - shift) % (SHORT + 8), 0)[:SHORT]
                row = lax.broadcasted_iota(jnp.int32, piece.shape, 0) + k * SHORT
                dst[pl.ds(pl.multiple_of(to + k * SHORT, SHORT), SHORT), :] = jnp.where(
                    row < size, piece, 0.0
                ).astype(BF)
                return c2

            return lax.fori_loop(0, tab_ref[0, 48 + j], chunk, c)

        lax.fori_loop(0, per, passage, 0)


def prep(me, owners, lengths, tokens, cotangent, per):
    rows, width = tokens.shape
    return pl.pallas_call(
        functools.partial(prep_kernel, per),
        out_shape=(
            jax.ShapeDtypeStruct((rows, width), BF),
            jax.ShapeDtypeStruct((rows, width), BF),
            jax.ShapeDtypeStruct((1, 128), jnp.int32),
        ),
        in_specs=[sm(), sm(), sm(), vm(), vm()],
        out_specs=(vm(), vm(), sm()),
        scratch_shapes=[pltpu.VMEM((rows + LONG + 8, width), F32)],
        compiler_params=params(),
        name="prep",
    )(me, owners, lengths, tokens, cotangent)


def unperm_rows(per, tab_ref, src_ref, wide, mask):
    rows = src_ref.shape[0]
    wide[...] = jnp.zeros_like(wide)

    def passage(j, c):
        start = tab_ref[0, j]
        size = tab_ref[0, 16 + j]
        frm = tab_ref[0, 32 + j]

        def chunk(k, c2):
            piece = src_ref[pl.ds(pl.multiple_of(frm + k * SHORT, SHORT), SHORT), :].astype(F32)
            row = lax.broadcasted_iota(jnp.int32, piece.shape, 0) + k * SHORT
            first = start + k * SHORT
            shift = first % 8
            at = pl.ds(pl.multiple_of(first - shift, 8), SHORT + 8)
            piece = jnp.where(row < size, piece, 0.0)
            piece = jnp.concatenate([piece, jnp.zeros((8, piece.shape[1]), F32)], 0)
            piece = pltpu.roll(piece, shift, 0)
            row = lax.broadcasted_iota(jnp.int32, piece.shape, 0)
            wide[at, :] = jnp.where(row >= shift, piece, wide[at, :])
            return c2

        return lax.fori_loop(0, tab_ref[0, 48 + j], chunk, c)

    lax.fori_loop(0, per, passage, 0)


def unperm_kernel(per, tab_ref, src_ref, out_ref, wide):
    unperm_rows(per, tab_ref, src_ref, wide, True)
    out_ref[...] = wide[pl.ds(0, src_ref.shape[0]), :].astype(out_ref.dtype)


def unperm(tab, src, per):
    rows, width = src.shape
    return pl.pallas_call(
        functools.partial(unperm_kernel, per),
        out_shape=jax.ShapeDtypeStruct((rows, width), src.dtype),
        in_specs=[sm(), vm()],
        out_specs=vm(),
        scratch_shapes=[pltpu.VMEM((rows + LONG + 8, width), F32)],
        compiler_params=params(),
        name="unperm",
    )(tab, src)


def place_of():
    dp, rep = lax.axis_index("dp"), lax.axis_index("rep")
    return dp // 2, dp % 2, rep // 2, rep % 2


def peers(z, y, x, c):
    def at(z2, y2, x2, c2):
        return (z2 * 2 + y2, x2 * 2 + c2)

    return (
        [at((z + k) % 4, y, x, c) for k in (1, 2, 3)],
        at(z, 1 - y, x, c),
        at(z, y, 1 - x, c),
        at(z, y, x, 1 - c),
    )


def greet(zs, yp, xp, cp):
    barrier = pltpu.get_barrier_semaphore()
    for peer in (*zs, yp, xp, cp):
        pl.semaphore_signal(barrier, inc=1, device_id=peer, device_id_type=pl.DeviceIdType.MESH)
    pl.semaphore_wait(barrier, 6)


def remote(src, dst, ssem, rsem, peer):
    return pltpu.make_async_remote_copy(
        src_ref=src, dst_ref=dst, send_sem=ssem, recv_sem=rsem,
        device_id=peer, device_id_type=pl.DeviceIdType.MESH,
    )


def wavefront(count, stages):
    for t in range(count + len(stages) - 1):
        for s in range(len(stages) - 1, -1, -1):
            if 0 <= t - s < count:
                stages[s](t - s)


def gather_kernel(n, *refs):
    shards, fulls = refs[:n], refs[n : 2 * n]
    ssem, rsem, lsem = refs[2 * n :]
    z, y, x, c = place_of()
    zs, yp, xp, cp = peers(z, y, x, c)
    greet(zs, yp, xp, cp)
    sent = []

    def go(w, i, src, dst, peer):
        copy = remote(src, dst, ssem.at[w, i], rsem.at[w, i], peer)
        copy.start()
        sent.append(copy)

    def arrive(w, i, ref):
        remote(ref, ref, ssem.at[w, i], rsem.at[w, i], cp).wait_recv()

    def local(w):
        return pltpu.make_async_copy(shards[w], fulls[w].at[z, y], lsem.at[w])

    def near(w):
        local(w).start()
        src = shards[w].at[c, pl.ds(x, 2)]
        dst = fulls[w].at[z, y, c, pl.ds(x, 2)]
        for k in range(3):
            go(w, k, src, dst, zs[k])
        go(w, 3, src, dst, yp)

    def mid(w):
        for k in range(3):
            zk = (z + 3 - k) % 4
            part = fulls[w].at[zk, y, c, pl.ds(x, 2)]
            arrive(w, k, part)
            go(w, 4 + k, part, part, yp)
            q = fulls[w].at[zk, y, c, 2 * x]
            go(w, 7 + k, q, q, xp)

    def far(w):
        for k in range(4):
            zk = (z + 4 - k) % 4
            part = fulls[w].at[zk, 1 - y, c, pl.ds(x, 2)]
            arrive(w, 3 + k, part)
            q = fulls[w].at[zk, 1 - y, c, 2 * x]
            go(w, 10 + k, q, q, xp)

    def across(w):
        for k in range(7):
            zk, yk = ((z + 3 - k) % 4, y) if k < 3 else ((z + 7 - k) % 4, 1 - y)
            arrive(w, 7 + k, fulls[w].at[zk, yk, c, 2 * (1 - x)])
            half = fulls[w].at[zk, yk, c]
            go(w, 14 + k, half, half, cp)

    def last(w):
        for k in range(7):
            zk, yk = ((z + 3 - k) % 4, y) if k < 3 else ((z + 7 - k) % 4, 1 - y)
            arrive(w, 14 + k, fulls[w].at[zk, yk, 1 - c])
        local(w).wait()

    wavefront(n, [near, mid, far, across, last])
    for copy in sent:
        copy.wait_send()


def blocks(shard):
    rows, columns = shard.shape
    return shard.reshape(2, 3, rows // 6, columns)


def gather(shards):
    n = len(shards)
    views = [blocks(s) for s in shards]
    fulls = pl.pallas_call(
        functools.partial(gather_kernel, n),
        out_shape=[jax.ShapeDtypeStruct((4, 2) + v.shape, v.dtype) for v in views],
        in_specs=[vm()] * n,
        out_specs=[pl.BlockSpec(memory_space=pl.ANY)] * n,
        scratch_shapes=[
            pltpu.SemaphoreType.DMA((n, 21)),
            pltpu.SemaphoreType.DMA((n, 21)),
            pltpu.SemaphoreType.DMA((n,)),
        ],
        compiler_params=params(collective_id=0, has_side_effects=True),
        name="gather",
    )(*views)
    return [f.reshape(8 * s.shape[0], s.shape[1]) for f, s in zip(fulls, shards)]


def scatter_kernel(n, *refs):
    grads, outs = refs[:n], refs[n : 2 * n]
    half, rx, rpy, rqy, rpz, rqz, rpx, fin, got = (refs[(2 + i) * n : (3 + i) * n] for i in range(9))
    ssem, rsem = refs[11 * n :]
    z, y, x, c = place_of()
    zs, yp, xp, cp = peers(z, y, x, c)
    greet(zs, yp, xp, cp)
    sent = []

    def go(w, i, src, dst, peer):
        copy = remote(src, dst, ssem.at[w, i], rsem.at[w, i], peer)
        copy.start()
        sent.append(copy)

    def arrive(w, i, ref):
        remote(ref, ref, ssem.at[w, i], rsem.at[w, i], cp).wait_recv()

    def add(*parts):
        total = parts[0].astype(F32)
        for part in parts[1:]:
            total = total + part.astype(F32)
        return total

    def s0(w):
        go(w, 0, grads[w].at[:, :, 1 - c], half[w], cp)

    def s1(w):
        arrive(w, 0, half[w])
        a = half[w]

        @pl.loop(0, 4)
        def _(i):
            for j in range(2):
                for k in range(3):
                    a[i, j, k] = add(grads[w][i, j, c, k], a[i, j, k]).astype(a.dtype)

        go(w, 1, a.at[:, :, 2 * (1 - x)], rx[w], xp)
        go(w, 2, a.at[:, 1 - y, 1], rpy[w], yp)

    def s2(w):
        a = half[w]
        arrive(w, 2, rpy[w])

        @pl.loop(0, 4)
        def _(i):
            a[i, y, 1] = add(a[i, y, 1], rpy[w][i]).astype(a.dtype)

        for k in range(3):
            go(w, 3 + k, a.at[(z + k + 1) % 4, y, 1], rpz[w].at[k], zs[k])
        arrive(w, 1, rx[w])

        @pl.loop(0, 4)
        def _(i):
            for j in range(2):
                a[i, j, 2 * x] = add(a[i, j, 2 * x], rx[w][i, j]).astype(a.dtype)

        go(w, 6, a.at[:, 1 - y, 2 * x], rqy[w], yp)

    def s3(w):
        a = half[w]
        arrive(w, 6, rqy[w])

        @pl.loop(0, 4)
        def _(i):
            a[i, y, 2 * x] = add(a[i, y, 2 * x], rqy[w][i]).astype(a.dtype)

        for k in range(3):
            go(w, 7 + k, a.at[(z + k + 1) % 4, y, 2 * x], rqz[w].at[k], zs[k])
        for k in range(3):
            arrive(w, 3 + k, rpz[w].at[k])
        a[z, y, 1] = add(a[z, y, 1], rpz[w][0], rpz[w][1], rpz[w][2]).astype(a.dtype)
        go(w, 10, a.at[z, y, 1], rpx[w], xp)

    def s4(w):
        a = half[w]
        for k in range(3):
            arrive(w, 7 + k, rqz[w].at[k])
        fin[w][0] = add(a[z, y, 2 * x], rqz[w][0], rqz[w][1], rqz[w][2]).astype(a.dtype)
        go(w, 11, fin[w].at[0], got[w].at[c, 2 * x], xp)
        go(w, 13, fin[w].at[0], got[w].at[c, 2 * x], cp)
        arrive(w, 10, rpx[w])
        fin[w][1] = add(a[z, y, 1], rpx[w][...]).astype(a.dtype)
        go(w, 14, fin[w].at[1], got[w].at[c, 1], cp)

    def s5(w):
        arrive(w, 11, got[w].at[c, 2 * (1 - x)])
        piece = got[w].at[c, 2 * (1 - x)]
        go(w, 12, piece, piece, cp)
        outs[w][c, 2 * x] = fin[w][0].astype(F32)
        outs[w][c, 1] = fin[w][1].astype(F32)
        outs[w][c, 2 * (1 - x)] = got[w][c, 2 * (1 - x)].astype(F32)

    def s6(w):
        arrive(w, 12, got[w].at[1 - c, 2 * (1 - x)])
        arrive(w, 13, got[w].at[1 - c, 2 * x])
        arrive(w, 14, got[w].at[1 - c, 1])
        for k in range(3):
            outs[w][1 - c, k] = got[w][1 - c, k].astype(F32)

    wavefront(n, [s0, s1, s2, s3, s4, s5, s6])
    for copy in sent:
        copy.wait_send()


def scatter(grads):
    n = len(grads)
    views = [g.reshape(4, 2, 2, 3, g.shape[0] // 48, g.shape[1]) for g in grads]
    lead = ((4, 2, 3), (4, 2), (4,), (4,), (3,), (3,), (), (2,), (2, 3))
    scratch = [pltpu.VMEM(s + v.shape[4:], v.dtype) for s in lead for v in views]
    outs = pl.pallas_call(
        functools.partial(scatter_kernel, n),
        out_shape=[jax.ShapeDtypeStruct(v.shape[2:], F32) for v in views],
        in_specs=[vm()] * n,
        out_specs=[vm()] * n,
        scratch_shapes=scratch
        + [pltpu.SemaphoreType.DMA((n, 15)), pltpu.SemaphoreType.DMA((n, 15))],
        compiler_params=params(collective_id=1, has_side_effects=True),
        name="scatter",
    )(*views)
    return [o.reshape(g.shape[0] // 8, g.shape[1]) for o, g in zip(outs, grads)]


def head_lanes(block, head):
    lane = lax.broadcasted_iota(jnp.int32, (1, block.shape[1]), 1)
    keep = jnp.where(lane >= HD, float(head), 1.0 - head)
    return block * keep.astype(BF)


def softmax_keys(scores, valid):
    scores = jnp.where(valid, scores, masked_score)
    weights = jnp.exp(scores - jnp.max(scores, axis=0, keepdims=True))
    return weights * (1.0 / jnp.sum(weights, axis=0, keepdims=True))


def short_valid(tab_ref, pair, size):
    key = lax.broadcasted_iota(jnp.int32, (size, size), 0)
    query = lax.broadcasted_iota(jnp.int32, (size, size), 1)
    low, high = tab_ref[0, 65 + 2 * pair], tab_ref[0, 66 + 2 * pair]
    bound = jnp.where(key >= SHORT, SHORT + high, low)
    return (key < bound) & (key // SHORT == query // SHORT)


def attend_kernel(scale, tab_ref, q_ref, k_ref, v_ref, out_ref, long_ref, short_ref):
    two = 2 * SHORT
    key = lax.broadcasted_iota(jnp.int32, (LONG, LONG), 0)
    valid = key < tab_ref[0, 64]
    shorts = (q_ref.shape[0] - LONG) // two
    keeps = [short_valid(tab_ref, b, two) for b in range(shorts)]
    total = None
    tails = [None] * shorts
    for h in range(2):
        scores = dot(head_lanes(k_ref[0:LONG], h), q_ref[0:LONG], NT) * scale
        probs = softmax_keys(scores, valid).astype(BF)
        long_ref[h] = probs
        part = dot(probs, head_lanes(v_ref[0:LONG], h), TN)
        total = part if total is None else total + part
        for b in range(shorts):
            rows = slice(LONG + b * two, LONG + (b + 1) * two)
            scores = dot(head_lanes(k_ref[rows], h), q_ref[rows], NT) * scale
            probs = softmax_keys(scores, keeps[b]).astype(BF)
            short_ref[h, b * two : (b + 1) * two] = probs
            part = dot(probs, head_lanes(v_ref[rows], h), TN)
            tails[b] = part if tails[b] is None else tails[b] + part
    out_ref[0:LONG] = total.astype(BF)
    for b in range(shorts):
        out_ref[LONG + b * two : LONG + (b + 1) * two] = tails[b].astype(BF)


def attend(tab, projected):
    rows, wide = projected.shape
    width = wide // 3
    pairs = width // (2 * HD)
    column = lambda off: pl.BlockSpec((rows, 2 * HD), lambda i, off=off: (0, off + i))
    return pl.pallas_call(
        functools.partial(attend_kernel, HD ** (-0.5)),
        grid=(pairs,),
        out_shape=(
            jax.ShapeDtypeStruct((rows, width), BF),
            jax.ShapeDtypeStruct((2 * pairs, LONG, LONG), BF),
            jax.ShapeDtypeStruct((2 * pairs, rows - LONG, 2 * SHORT), BF),
        ),
        in_specs=[sm(), column(0), column(pairs), column(2 * pairs)],
        out_specs=(
            column(0),
            pl.BlockSpec((2, LONG, LONG), lambda i: (i, 0, 0)),
            pl.BlockSpec((2, rows - LONG, 2 * SHORT), lambda i: (i, 0, 0)),
        ),
        compiler_params=params(),
        name="attend",
    )(tab, projected, projected, projected)


def attend_back_kernel(scale, q_ref, k_ref, v_ref, g_ref, long_ref, short_ref, out_ref):
    two = 2 * SHORT
    shorts = (q_ref.shape[0] - LONG) // two
    spans = [(slice(0, LONG), None)]
    spans += [(slice(LONG + b * two, LONG + (b + 1) * two), b) for b in range(shorts)]
    for rows, b in spans:
        sums = None
        for h in range(2):
            probs = long_ref[h] if b is None else short_ref[h, b * two : (b + 1) * two]
            grad = head_lanes(g_ref[rows], h)
            wide = probs.astype(F32)
            grad_probs = dot(v_ref[rows], grad, NT)
            mean = jnp.sum(grad_probs * wide, axis=0, keepdims=True)
            grad_scores = (wide * (grad_probs - mean)).astype(BF)
            parts = (
                dot(grad_scores, head_lanes(k_ref[rows], h), TN),
                dot(grad_scores, head_lanes(q_ref[rows], h)),
                dot(probs, grad),
            )
            sums = parts if sums is None else tuple(a + p for a, p in zip(sums, parts))
        out_ref[0, rows] = (sums[0] * scale).astype(BF)
        out_ref[1, rows] = (sums[1] * scale).astype(BF)
        out_ref[2, rows] = sums[2].astype(BF)


def attend_back(projected, grad_mixed, long_probs, short_probs):
    rows, wide = projected.shape
    width = wide // 3
    pairs = width // (2 * HD)
    column = lambda off: pl.BlockSpec((rows, 2 * HD), lambda i, off=off: (0, off + i))
    return pl.pallas_call(
        functools.partial(attend_back_kernel, HD ** (-0.5)),
        grid=(pairs,),
        out_shape=jax.ShapeDtypeStruct((3, rows, width), BF),
        in_specs=[
            column(0), column(pairs), column(2 * pairs), column(0),
            pl.BlockSpec((2, LONG, LONG), lambda i: (i, 0, 0)),
            pl.BlockSpec((2, rows - LONG, 2 * SHORT), lambda i: (i, 0, 0)),
        ],
        out_specs=pl.BlockSpec((3, rows, 2 * HD), lambda i: (0, 0, i)),
        compiler_params=params(),
        name="attend_back",
    )(projected, projected, projected, grad_mixed, long_probs, short_probs)


def gelu_pair(value):
    size = jnp.abs(value)
    bell = jnp.exp(-0.5 * value * value)
    t = 1.0 / (1.0 + 0.23164189 * size)
    tail = t * (0.127414796 + t * (-0.142248368 + t * (0.7107068705 + t * (-0.7265760135 + t * 0.5307027145))))
    tail = tail * bell
    whole = jnp.where(value >= 0.0, 1.0 - tail, tail)
    return (value * whole, whole + value * bell * 0.3989422804)


def middle_kernel(
    step, span, mixed, tokens, cot, w_out, w_up, w_down, gains, biases, ff_bias,
    out, acc, g_mixed, d_out, d_up, d_down, sums, d_ffb, unit, low, low2, hidden, slope, inv
):
    rows = mixed.shape[0]
    parts = w_up.shape[1] // span
    sums[...] = jnp.zeros_like(sums)

    def rows_at(i):
        return pl.ds(pl.multiple_of(i * step, step), step)

    def columns_at(j):
        return pl.ds(pl.multiple_of(j * span, span), span)

    def mean(a):
        return jnp.mean(a, axis=-1, keepdims=True)

    def tally(i, a):
        sums[i : i + 1, :] += jnp.sum(a, axis=0, keepdims=True)

    def norm(r):
        center = r - mean(r)
        scale = lax.rsqrt(mean(center * center) + norm_eps)
        return center * scale, scale

    def back(s, u, scale):
        return scale * (s - mean(s) - u * mean(s * u))

    @pl.loop(0, rows // step)
    def _(i):
        at = rows_at(i)
        branch = dot(mixed[at, :], w_out[...]) + biases[2:3, :]
        u, scale = norm(tokens[at, :].astype(F32) + branch)
        unit[at, :] = u
        inv[at, :] = scale
        low[at, :] = (u * gains[0:1, :] + biases[4:5, :]).astype(BF)
        acc[at, :] = jnp.zeros((step, acc.shape[1]), F32)

    @pl.loop(0, parts)
    def _(j):
        cols = columns_at(j)
        for i in range(rows // step):
            at = slice(i * step, (i + 1) * step)
            inner = dot(low[at, :], w_up[:, cols]) + ff_bias[:, cols]
            act, der = gelu_pair(inner)
            act = act.astype(BF)
            hidden[at, cols] = act
            slope[at, cols] = der.astype(BF)
            acc[at, :] += dot(act, w_down[cols, :])

    @pl.loop(0, rows // step)
    def _(i):
        at = rows_at(i)
        first = unit[at, :] * gains[0:1, :] + biases[4:5, :]
        u, scale = norm(first + acc[at, :] + biases[3:4, :])
        out[at, :] = (u * gains[1:2, :] + biases[5:6, :]).astype(BF)
        g = cot[at, :].astype(F32)
        tally(1, g * u)
        tally(5, g)
        g = back(g * gains[1:2, :], u, scale)
        acc[at, :] = g
        g = g.astype(BF)
        low2[at, :] = g
        tally(3, g.astype(F32))

    @pl.loop(0, parts)
    def _(j):
        cols = columns_at(j)
        total = None
        for i in range(rows // step):
            at = slice(i * step, (i + 1) * step)
            g = dot(low2[at, :], w_down[cols, :], NT) * slope[at, cols].astype(F32)
            g = g.astype(BF)
            slope[at, cols] = g
            part = jnp.sum(g.astype(F32), axis=0, keepdims=True)
            total = part if total is None else total + part
            acc[at, :] += dot(g, w_up[:, cols], NT)
        d_ffb[:, cols] = total
        d_down[cols, :] = dot(hidden[:, cols], low2[...], TN).astype(BF)
        d_up[:, cols] = dot(low[...], slope[:, cols], TN).astype(BF)

    @pl.loop(0, rows // step)
    def _(i):
        at = rows_at(i)
        g, u = acc[at, :], unit[at, :]
        tally(0, g * u)
        tally(4, g)
        g = back(g * gains[0:1, :], u, inv[at, :])
        acc[at, :] = g
        g = g.astype(BF)
        low2[at, :] = g
        tally(2, g.astype(F32))
        g_mixed[at, :] = dot(g, w_out[...], NT).astype(BF)

    d_out[...] = dot(mixed[...], low2[...], TN).astype(BF)


def middle(mixed, tokens, cot, w_out, w_up, w_down, gains, biases, ff_bias):
    rows, width = mixed.shape
    ff = w_up.shape[1]
    shape = jax.ShapeDtypeStruct
    return pl.pallas_call(
        functools.partial(middle_kernel, 256, 512),
        out_shape=(
            shape((rows, width), BF), shape((rows, width), F32), shape((rows, width), BF),
            shape((width, width), BF), shape((width, ff), BF), shape((ff, width), BF),
            shape((8, width), F32), shape((1, ff), F32),
        ),
        in_specs=[vm()] * 9,
        out_specs=(vm(),) * 8,
        scratch_shapes=[
            pltpu.VMEM((rows, width), F32), pltpu.VMEM((rows, width), BF),
            pltpu.VMEM((rows, width), BF), pltpu.VMEM((rows, ff), BF),
            pltpu.VMEM((rows, ff), BF), pltpu.VMEM((rows, 1), F32),
        ],
        compiler_params=params(),
        name="middle",
    )(mixed, tokens, cot, w_out, w_up, w_down, gains, biases, ff_bias)


def square():
    return lax.axis_size("dp") == 8 and lax.axis_size("rep") == 4


def gather_layer(qkv_weight, out_weight, up_weight, down_weight, norm_gains, bias_rows, ff_bias):
    if not square():
        return (
            lax.all_gather(qkv_weight, "dp", axis=0, tiled=True),
            lax.all_gather(out_weight, "dp", axis=0, tiled=True),
            lax.all_gather(up_weight, "dp", axis=0, tiled=True),
            lax.all_gather(down_weight, "dp", axis=0, tiled=True),
            lax.all_gather(norm_gains, "dp", axis=1, tiled=True),
            lax.all_gather(bias_rows, "dp", axis=1, tiled=True),
            lax.all_gather(ff_bias, "dp", axis=0, tiled=True),
        )
    small = jnp.concatenate([bias_rows.reshape(-1), norm_gains.reshape(-1), ff_bias])
    used = small.shape[0]
    small = jnp.pad(small, (0, 96 * 128 - used)).reshape(96, 128)
    full = gather([small, qkv_weight, out_weight, up_weight, down_weight])
    rows = full[0].reshape(8, 96 * 128)[:, :used]
    nb, ng = bias_rows.size, norm_gains.size
    biases = rows[:, :nb].reshape(8, bias_rows.shape[0], -1).transpose(1, 0, 2)
    gains = rows[:, nb : nb + ng].reshape(8, norm_gains.shape[0], -1).transpose(1, 0, 2)
    return (
        full[1], full[2], full[3], full[4],
        gains.reshape(norm_gains.shape[0], -1),
        biases.reshape(bias_rows.shape[0], -1),
        rows[:, nb + ng :].reshape(-1),
    )


def reduce_layer(d_qkv, d_out, d_up, d_down, d_gains, d_biases, d_up_bias):
    big = [g.astype(BF) for g in (d_down, d_up, d_out, d_qkv)]
    if not square():
        def full(g):
            part = lax.psum_scatter(g, "rep", scatter_dimension=1, tiled=True).astype(F32)
            part = lax.psum_scatter(part, "dp", scatter_dimension=0, tiled=True)
            return lax.all_gather(part.astype(BF), "rep", axis=1, tiled=True).astype(F32)

        down, up, out, qkv = [full(g) for g in big]
        small = lax.psum(
            (
                lax.psum_scatter(d_gains, "dp", scatter_dimension=1, tiled=True),
                lax.psum_scatter(d_biases, "dp", scatter_dimension=1, tiled=True),
                lax.psum_scatter(d_up_bias, "dp", scatter_dimension=0, tiled=True),
            ),
            "rep",
        )
        return (qkv, out, up, down) + small
    def cut(g):
        return g.reshape(g.shape[0], 8, -1).transpose(1, 0, 2).reshape(8, -1)

    parts = [cut(d_gains), cut(d_biases), d_up_bias.reshape(8, -1)]
    small = jnp.concatenate(parts, 1)
    small = jnp.pad(small, ((0, 0), (0, 48 * 128 - small.shape[1]))).reshape(8 * 48, 128)
    down, up, out, qkv, own = scatter(big + [small])
    own = own.reshape(-1)
    n0, n1, n2 = (p.shape[1] for p in parts)
    return (
        qkv, out, up, down,
        own[:n0].reshape(d_gains.shape[0], -1),
        own[n0 : n0 + n1].reshape(d_biases.shape[0], -1),
        own[n0 + n1 : n0 + n1 + n2],
    )


def local(
    tokens,
    qkv_weight,
    out_weight,
    up_weight,
    down_weight,
    norm_gains,
    bias_rows,
    ff_bias,
    lengths,
    owners,
    cotangent,
):
    row_count, model_width = tokens.shape
    device = lax.axis_index("dp") * lax.axis_size("rep") + lax.axis_index("rep")
    devices = lax.axis_size("dp") * lax.axis_size("rep")
    per = lengths.shape[0] // devices
    assert row_count == LONG + SHORT * (per - 1)
    me = device.astype(jnp.int32).reshape(1)
    tokens, cotangent, tab = prep(me, owners, lengths, tokens, cotangent, per)
    layer_w = gather_layer(qkv_weight, out_weight, up_weight, down_weight, norm_gains, bias_rows, ff_bias)
    w_qkv, w_out, w_up, w_down, gains_low, biases_low, up_bias_low = layer_w
    gain_rows = gains_low.astype(jnp.float32)
    shift_rows = biases_low.astype(jnp.float32)
    up_bias = up_bias_low.astype(jnp.float32)
    zero_bias = jnp.zeros((model_width,), jnp.float32)
    head_bias = jnp.concatenate([shift_rows[0], zero_bias, shift_rows[1]])
    projected = (jnp.dot(tokens, w_qkv, preferred_element_type=jnp.float32) + head_bias).astype(
        jnp.bfloat16
    )
    mixed_rows, long_probs, short_probs = attend(tab, projected)
    final, grad_one, grad_mixed, d_out, d_up, d_down, sums, d_up_bias = middle(
        mixed_rows, tokens, cotangent, w_out, w_up, w_down, gain_rows, shift_rows, up_bias[None]
    )
    d_up_bias = d_up_bias[0]
    output = unperm(tab, final, per)
    parts = attend_back(projected, grad_mixed, long_probs, short_probs)
    grad_heads = jnp.concatenate([parts[0], parts[1], parts[2]], 1)
    d_head_bias = jnp.sum(grad_heads.astype(jnp.float32), axis=0)
    d_qkv = jnp.einsum("td,te->de", tokens, grad_heads, preferred_element_type=jnp.float32)
    grad_tokens = grad_one + jnp.einsum(
        "te,de->td", grad_heads, w_qkv, preferred_element_type=jnp.float32
    )
    grad_tokens = unperm(tab, grad_tokens, per)
    d_gains = sums[0:2]
    d_biases = jnp.concatenate(
        [d_head_bias[None, :model_width], d_head_bias[None, 2 * model_width :], sums[2:6]]
    )
    return (output, grad_tokens) + reduce_layer(d_qkv, d_out, d_up, d_down, d_gains, d_biases, d_up_bias)


def solution(mesh):
    in_specs = (
        P(("dp", "rep"), None),
        P("dp", None),
        P("dp", None),
        P("dp", None),
        P("dp", None),
        P(None, "dp"),
        P(None, "dp"),
        P("dp"),
        P(),
        P(),
        P(("dp", "rep"), None),
    )
    out_specs = (
        P(("dp", "rep"), None),
        P(("dp", "rep"), None),
        P("dp", None),
        P("dp", None),
        P("dp", None),
        P("dp", None),
        P(None, "dp"),
        P(None, "dp"),
        P("dp"),
    )
    return jax.shard_map(local, mesh=mesh, in_specs=in_specs, out_specs=out_specs, check_vma=False)
```

```python
import functools

import jax
import jax.numpy as jnp
from jax import lax
from jax.experimental import pallas as pl
from jax.experimental.pallas import tpu as pltpu
from jax.sharding import PartitionSpec as P

HEADS = 12
HD = 64
LONG = 512
SHORT = 64
norm_eps = 1e-06
masked_score = -1000000000.0
BF = jnp.bfloat16
F32 = jnp.float32
VMEM_LIMIT = 62 * 1024 * 1024

NN = (((1,), (0,)), ((), ()))
NT = (((1,), (1,)), ((), ()))
TN = (((0,), (0,)), ((), ()))


def dot(a, b, dims=NN):
    return lax.dot_general(a, b, dims, preferred_element_type=F32)


def vm():
    return pl.BlockSpec(memory_space=pltpu.VMEM)


def sm():
    return pl.BlockSpec(memory_space=pltpu.SMEM)


def params(**kw):
    return pltpu.CompilerParams(vmem_limit_bytes=VMEM_LIMIT, **kw)


def prep_kernel(per, me_ref, own_ref, len_ref, tok_ref, cot_ref, tok_out, cot_out, tab_ref, wide):
    total = own_ref.shape[0]
    rows = tok_ref.shape[0]
    me = me_ref[0]

    def zero(i, c):
        tab_ref[0, i] = 0
        return c

    lax.fori_loop(0, 128, zero, 0)

    def scan(p, c):
        count, start = c
        hit = own_ref[p] == me
        size = len_ref[p]
        tab_ref[0, count] = start
        tab_ref[0, 16 + count] = size
        return (count + hit.astype(jnp.int32), start + jnp.where(hit, size, 0))

    lax.fori_loop(0, total, scan, (jnp.int32(0), jnp.int32(0)), unroll=8)

    def find(j, c):
        return jnp.where(tab_ref[0, 16 + j] > SHORT, j, c)

    big = lax.fori_loop(0, per, find, jnp.int32(0))

    def place(j, slot):
        is_big = j == big
        tab_ref[0, 32 + j] = jnp.where(is_big, 0, LONG + SHORT * slot)
        tab_ref[0, 48 + j] = jnp.where(is_big, LONG // SHORT, 1)
        at = jnp.where(is_big, 0, slot + 1)
        tab_ref[0, 64 + at] = tab_ref[0, 16 + j]
        return slot + jnp.where(is_big, 0, 1)

    lax.fori_loop(0, per, place, jnp.int32(0))

    for src, dst in ((tok_ref, tok_out), (cot_ref, cot_out)):
        wide[pl.ds(0, rows), :] = src[...].astype(F32)
        wide[pl.ds(rows, LONG + 8), :] = jnp.zeros((LONG + 8, src.shape[1]), F32)

        def passage(j, c):
            start = tab_ref[0, j]
            size = tab_ref[0, 16 + j]
            to = tab_ref[0, 32 + j]

            def chunk(k, c2):
                first = start + k * SHORT
                shift = first % 8
                piece = wide[pl.ds(pl.multiple_of(first - shift, 8), SHORT + 8), :]
                piece = pltpu.roll(piece, (SHORT + 8 - shift) % (SHORT + 8), 0)[:SHORT]
                row = lax.broadcasted_iota(jnp.int32, piece.shape, 0) + k * SHORT
                dst[pl.ds(pl.multiple_of(to + k * SHORT, SHORT), SHORT), :] = jnp.where(
                    row < size, piece, 0.0
                ).astype(BF)
                return c2

            return lax.fori_loop(0, tab_ref[0, 48 + j], chunk, c)

        lax.fori_loop(0, per, passage, 0)


def prep(me, owners, lengths, tokens, cotangent, per):
    rows, width = tokens.shape
    return pl.pallas_call(
        functools.partial(prep_kernel, per),
        out_shape=(
            jax.ShapeDtypeStruct((rows, width), BF),
            jax.ShapeDtypeStruct((rows, width), BF),
            jax.ShapeDtypeStruct((1, 128), jnp.int32),
        ),
        in_specs=[sm(), sm(), sm(), vm(), vm()],
        out_specs=(vm(), vm(), sm()),
        scratch_shapes=[pltpu.VMEM((rows + LONG + 8, width), F32)],
        compiler_params=params(),
        name="prep",
    )(me, owners, lengths, tokens, cotangent)


def unperm_rows(per, tab_ref, src_ref, wide, mask):
    rows = src_ref.shape[0]
    wide[...] = jnp.zeros_like(wide)

    def passage(j, c):
        start = tab_ref[0, j]
        size = tab_ref[0, 16 + j]
        frm = tab_ref[0, 32 + j]

        def chunk(k, c2):
            piece = src_ref[pl.ds(pl.multiple_of(frm + k * SHORT, SHORT), SHORT), :].astype(F32)
            row = lax.broadcasted_iota(jnp.int32, piece.shape, 0) + k * SHORT
            first = start + k * SHORT
            shift = first % 8
            at = pl.ds(pl.multiple_of(first - shift, 8), SHORT + 8)
            piece = jnp.where(row < size, piece, 0.0)
            piece = jnp.concatenate([piece, jnp.zeros((8, piece.shape[1]), F32)], 0)
            piece = pltpu.roll(piece, shift, 0)
            row = lax.broadcasted_iota(jnp.int32, piece.shape, 0)
            wide[at, :] = jnp.where(row >= shift, piece, wide[at, :])
            return c2

        return lax.fori_loop(0, tab_ref[0, 48 + j], chunk, c)

    lax.fori_loop(0, per, passage, 0)


def unperm_kernel(per, tab_ref, src_ref, out_ref, wide):
    unperm_rows(per, tab_ref, src_ref, wide, True)
    out_ref[...] = wide[pl.ds(0, src_ref.shape[0]), :].astype(out_ref.dtype)


def unperm(tab, src, per):
    rows, width = src.shape
    return pl.pallas_call(
        functools.partial(unperm_kernel, per),
        out_shape=jax.ShapeDtypeStruct((rows, width), src.dtype),
        in_specs=[sm(), vm()],
        out_specs=vm(),
        scratch_shapes=[pltpu.VMEM((rows + LONG + 8, width), F32)],
        compiler_params=params(),
        name="unperm",
    )(tab, src)


def place_of():
    dp, rep = lax.axis_index("dp"), lax.axis_index("rep")
    return dp // 2, dp % 2, rep // 2, rep % 2


def peers(z, y, x, c):
    def at(z2, y2, x2, c2):
        return (z2 * 2 + y2, x2 * 2 + c2)

    return (
        [at((z + k) % 4, y, x, c) for k in (1, 2, 3)],
        at(z, 1 - y, x, c),
        at(z, y, 1 - x, c),
        at(z, y, x, 1 - c),
    )


def greet(zs, yp, xp, cp):
    barrier = pltpu.get_barrier_semaphore()
    for peer in (*zs, yp, xp, cp):
        pl.semaphore_signal(barrier, inc=1, device_id=peer, device_id_type=pl.DeviceIdType.MESH)
    pl.semaphore_wait(barrier, 6)


def remote(src, dst, ssem, rsem, peer):
    return pltpu.make_async_remote_copy(
        src_ref=src, dst_ref=dst, send_sem=ssem, recv_sem=rsem,
        device_id=peer, device_id_type=pl.DeviceIdType.MESH,
    )


def wavefront(count, stages):
    for t in range(count + len(stages) - 1):
        for s in range(len(stages) - 1, -1, -1):
            if 0 <= t - s < count:
                stages[s](t - s)


def gather_kernel(n, *refs):
    shards, fulls = refs[:n], refs[n : 2 * n]
    ssem, rsem, lsem = refs[2 * n :]
    z, y, x, c = place_of()
    zs, yp, xp, cp = peers(z, y, x, c)
    greet(zs, yp, xp, cp)
    sent = []

    def go(w, i, src, dst, peer):
        copy = remote(src, dst, ssem.at[w, i], rsem.at[w, i], peer)
        copy.start()
        sent.append(copy)

    def arrive(w, i, ref):
        remote(ref, ref, ssem.at[w, i], rsem.at[w, i], cp).wait_recv()

    def local(w):
        return pltpu.make_async_copy(shards[w], fulls[w].at[z, y], lsem.at[w])

    def near(w):
        local(w).start()
        src = shards[w].at[c, pl.ds(x, 2)]
        dst = fulls[w].at[z, y, c, pl.ds(x, 2)]
        for k in range(3):
            go(w, k, src, dst, zs[k])
        go(w, 3, src, dst, yp)

    def mid(w):
        for k in range(3):
            zk = (z + 3 - k) % 4
            part = fulls[w].at[zk, y, c, pl.ds(x, 2)]
            arrive(w, k, part)
            go(w, 4 + k, part, part, yp)
            q = fulls[w].at[zk, y, c, 2 * x]
            go(w, 7 + k, q, q, xp)

    def far(w):
        for k in range(4):
            zk = (z + 4 - k) % 4
            part = fulls[w].at[zk, 1 - y, c, pl.ds(x, 2)]
            arrive(w, 3 + k, part)
            q = fulls[w].at[zk, 1 - y, c, 2 * x]
            go(w, 10 + k, q, q, xp)

    def across(w):
        for k in range(7):
            zk, yk = ((z + 3 - k) % 4, y) if k < 3 else ((z + 7 - k) % 4, 1 - y)
            arrive(w, 7 + k, fulls[w].at[zk, yk, c, 2 * (1 - x)])
            half = fulls[w].at[zk, yk, c]
            go(w, 14 + k, half, half, cp)

    def last(w):
        for k in range(7):
            zk, yk = ((z + 3 - k) % 4, y) if k < 3 else ((z + 7 - k) % 4, 1 - y)
            arrive(w, 14 + k, fulls[w].at[zk, yk, 1 - c])
        local(w).wait()

    wavefront(n, [near, mid, far, across, last])
    for copy in sent:
        copy.wait_send()


def blocks(shard):
    rows, columns = shard.shape
    return shard.reshape(2, 3, rows // 6, columns)


def gather(shards):
    n = len(shards)
    views = [blocks(s) for s in shards]
    fulls = pl.pallas_call(
        functools.partial(gather_kernel, n),
        out_shape=[jax.ShapeDtypeStruct((4, 2) + v.shape, v.dtype) for v in views],
        in_specs=[vm()] * n,
        out_specs=[pl.BlockSpec(memory_space=pl.ANY)] * n,
        scratch_shapes=[
            pltpu.SemaphoreType.DMA((n, 21)),
            pltpu.SemaphoreType.DMA((n, 21)),
            pltpu.SemaphoreType.DMA((n,)),
        ],
        compiler_params=params(collective_id=0, has_side_effects=True),
        name="gather",
    )(*views)
    return [f.reshape(8 * s.shape[0], s.shape[1]) for f, s in zip(fulls, shards)]


def head_lanes(block, head):
    lane = lax.broadcasted_iota(jnp.int32, (1, block.shape[1]), 1)
    keep = jnp.where(lane >= HD, float(head), 1.0 - head)
    return block * keep.astype(BF)


def softmax_keys(scores, valid):
    scores = jnp.where(valid, scores, masked_score)
    weights = jnp.exp(scores - jnp.max(scores, axis=0, keepdims=True))
    return weights * (1.0 / jnp.sum(weights, axis=0, keepdims=True))


def short_valid(tab_ref, pair, size):
    key = lax.broadcasted_iota(jnp.int32, (size, size), 0)
    query = lax.broadcasted_iota(jnp.int32, (size, size), 1)
    low, high = tab_ref[0, 65 + 2 * pair], tab_ref[0, 66 + 2 * pair]
    bound = jnp.where(key >= SHORT, SHORT + high, low)
    return (key < bound) & (key // SHORT == query // SHORT)


def attend_kernel(scale, tab_ref, q_ref, k_ref, v_ref, out_ref, long_ref, short_ref):
    two = 2 * SHORT
    key = lax.broadcasted_iota(jnp.int32, (LONG, LONG), 0)
    valid = key < tab_ref[0, 64]
    shorts = (q_ref.shape[0] - LONG) // two
    keeps = [short_valid(tab_ref, b, two) for b in range(shorts)]
    total = None
    tails = [None] * shorts
    for h in range(2):
        scores = dot(head_lanes(k_ref[0:LONG], h), q_ref[0:LONG], NT) * scale
        probs = softmax_keys(scores, valid).astype(BF)
        long_ref[h] = probs
        part = dot(probs, head_lanes(v_ref[0:LONG], h), TN)
        total = part if total is None else total + part
        for b in range(shorts):
            rows = slice(LONG + b * two, LONG + (b + 1) * two)
            scores = dot(head_lanes(k_ref[rows], h), q_ref[rows], NT) * scale
            probs = softmax_keys(scores, keeps[b]).astype(BF)
            short_ref[h, b * two : (b + 1) * two] = probs
            part = dot(probs, head_lanes(v_ref[rows], h), TN)
            tails[b] = part if tails[b] is None else tails[b] + part
    out_ref[0:LONG] = total.astype(BF)
    for b in range(shorts):
        out_ref[LONG + b * two : LONG + (b + 1) * two] = tails[b].astype(BF)


def attend(tab, projected):
    rows, wide = projected.shape
    width = wide // 3
    pairs = width // (2 * HD)
    column = lambda off: pl.BlockSpec((rows, 2 * HD), lambda i, off=off: (0, off + i))
    return pl.pallas_call(
        functools.partial(attend_kernel, HD ** (-0.5)),
        grid=(pairs,),
        out_shape=(
            jax.ShapeDtypeStruct((rows, width), BF),
            jax.ShapeDtypeStruct((2 * pairs, LONG, LONG), BF),
            jax.ShapeDtypeStruct((2 * pairs, rows - LONG, 2 * SHORT), BF),
        ),
        in_specs=[sm(), column(0), column(pairs), column(2 * pairs)],
        out_specs=(
            column(0),
            pl.BlockSpec((2, LONG, LONG), lambda i: (i, 0, 0)),
            pl.BlockSpec((2, rows - LONG, 2 * SHORT), lambda i: (i, 0, 0)),
        ),
        compiler_params=params(),
        name="attend",
    )(tab, projected, projected, projected)


def attend_back_kernel(scale, q_ref, k_ref, v_ref, g_ref, long_ref, short_ref, out_ref):
    two = 2 * SHORT
    shorts = (q_ref.shape[0] - LONG) // two
    spans = [(slice(0, LONG), None)]
    spans += [(slice(LONG + b * two, LONG + (b + 1) * two), b) for b in range(shorts)]
    for rows, b in spans:
        sums = None
        for h in range(2):
            probs = long_ref[h] if b is None else short_ref[h, b * two : (b + 1) * two]
            grad = head_lanes(g_ref[rows], h)
            wide = probs.astype(F32)
            grad_probs = dot(v_ref[rows], grad, NT)
            mean = jnp.sum(grad_probs * wide, axis=0, keepdims=True)
            grad_scores = (wide * (grad_probs - mean)).astype(BF)
            parts = (
                dot(grad_scores, head_lanes(k_ref[rows], h), TN),
                dot(grad_scores, head_lanes(q_ref[rows], h)),
                dot(probs, grad),
            )
            sums = parts if sums is None else tuple(a + p for a, p in zip(sums, parts))
        out_ref[0, rows] = (sums[0] * scale).astype(BF)
        out_ref[1, rows] = (sums[1] * scale).astype(BF)
        out_ref[2, rows] = sums[2].astype(BF)


def attend_back(projected, grad_mixed, long_probs, short_probs):
    rows, wide = projected.shape
    width = wide // 3
    pairs = width // (2 * HD)
    column = lambda off: pl.BlockSpec((rows, 2 * HD), lambda i, off=off: (0, off + i))
    return pl.pallas_call(
        functools.partial(attend_back_kernel, HD ** (-0.5)),
        grid=(pairs,),
        out_shape=jax.ShapeDtypeStruct((3, rows, width), BF),
        in_specs=[
            column(0), column(pairs), column(2 * pairs), column(0),
            pl.BlockSpec((2, LONG, LONG), lambda i: (i, 0, 0)),
            pl.BlockSpec((2, rows - LONG, 2 * SHORT), lambda i: (i, 0, 0)),
        ],
        out_specs=pl.BlockSpec((3, rows, 2 * HD), lambda i: (0, 0, i)),
        compiler_params=params(),
        name="attend_back",
    )(projected, projected, projected, grad_mixed, long_probs, short_probs)


def gelu_pair(value):
    size = jnp.abs(value)
    bell = jnp.exp(-0.5 * value * value)
    t = 1.0 / (1.0 + 0.23164189 * size)
    tail = t * (0.127414796 + t * (-0.142248368 + t * (0.7107068705 + t * (-0.7265760135 + t * 0.5307027145))))
    tail = tail * bell
    whole = jnp.where(value >= 0.0, 1.0 - tail, tail)
    return (value * whole, whole + value * bell * 0.3989422804)


def middle_kernel(
    step, span, mixed, tokens, cot, w_out, w_up, w_down, gains, biases, ff_bias,
    out, acc, g_mixed, d_out, d_up, d_down, sums, d_ffb, unit, low, low2, hidden, slope, inv
):
    rows = mixed.shape[0]
    parts = w_up.shape[1] // span
    sums[...] = jnp.zeros_like(sums)

    def rows_at(i):
        return pl.ds(pl.multiple_of(i * step, step), step)

    def columns_at(j):
        return pl.ds(pl.multiple_of(j * span, span), span)

    def mean(a):
        return jnp.mean(a, axis=-1, keepdims=True)

    def tally(i, a):
        sums[i : i + 1, :] += jnp.sum(a, axis=0, keepdims=True)

    def norm(r):
        center = r - mean(r)
        scale = lax.rsqrt(mean(center * center) + norm_eps)
        return center * scale, scale

    def back(s, u, scale):
        return scale * (s - mean(s) - u * mean(s * u))

    @pl.loop(0, rows // step)
    def _(i):
        at = rows_at(i)
        branch = dot(mixed[at, :], w_out[...]) + biases[2:3, :]
        u, scale = norm(tokens[at, :].astype(F32) + branch)
        unit[at, :] = u
        inv[at, :] = scale
        low[at, :] = (u * gains[0:1, :] + biases[4:5, :]).astype(BF)
        acc[at, :] = jnp.zeros((step, acc.shape[1]), F32)

    @pl.loop(0, parts)
    def _(j):
        cols = columns_at(j)
        for i in range(rows // step):
            at = slice(i * step, (i + 1) * step)
            inner = dot(low[at, :], w_up[:, cols]) + ff_bias[:, cols]
            act, der = gelu_pair(inner)
            act = act.astype(BF)
            hidden[at, cols] = act
            slope[at, cols] = der.astype(BF)
            acc[at, :] += dot(act, w_down[cols, :])

    @pl.loop(0, rows // step)
    def _(i):
        at = rows_at(i)
        first = unit[at, :] * gains[0:1, :] + biases[4:5, :]
        u, scale = norm(first + acc[at, :] + biases[3:4, :])
        out[at, :] = (u * gains[1:2, :] + biases[5:6, :]).astype(BF)
        g = cot[at, :].astype(F32)
        tally(1, g * u)
        tally(5, g)
        g = back(g * gains[1:2, :], u, scale)
        acc[at, :] = g
        g = g.astype(BF)
        low2[at, :] = g
        tally(3, g.astype(F32))

    @pl.loop(0, parts)
    def _(j):
        cols = columns_at(j)
        total = None
        for i in range(rows // step):
            at = slice(i * step, (i + 1) * step)
            g = dot(low2[at, :], w_down[cols, :], NT) * slope[at, cols].astype(F32)
            g = g.astype(BF)
            slope[at, cols] = g
            part = jnp.sum(g.astype(F32), axis=0, keepdims=True)
            total = part if total is None else total + part
            acc[at, :] += dot(g, w_up[:, cols], NT)
        d_ffb[:, cols] = total
        d_down[cols, :] = dot(hidden[:, cols], low2[...], TN).astype(BF)
        d_up[:, cols] = dot(low[...], slope[:, cols], TN).astype(BF)

    @pl.loop(0, rows // step)
    def _(i):
        at = rows_at(i)
        g, u = acc[at, :], unit[at, :]
        tally(0, g * u)
        tally(4, g)
        g = back(g * gains[0:1, :], u, inv[at, :])
        acc[at, :] = g
        g = g.astype(BF)
        low2[at, :] = g
        tally(2, g.astype(F32))
        g_mixed[at, :] = dot(g, w_out[...], NT).astype(BF)

    d_out[...] = dot(mixed[...], low2[...], TN).astype(BF)


def middle(mixed, tokens, cot, w_out, w_up, w_down, gains, biases, ff_bias):
    rows, width = mixed.shape
    ff = w_up.shape[1]
    shape = jax.ShapeDtypeStruct
    return pl.pallas_call(
        functools.partial(middle_kernel, 256, 512),
        out_shape=(
            shape((rows, width), BF), shape((rows, width), F32), shape((rows, width), BF),
            shape((width, width), BF), shape((width, ff), BF), shape((ff, width), BF),
            shape((8, width), F32), shape((1, ff), F32),
        ),
        in_specs=[vm()] * 9,
        out_specs=(vm(),) * 8,
        scratch_shapes=[
            pltpu.VMEM((rows, width), F32), pltpu.VMEM((rows, width), BF),
            pltpu.VMEM((rows, width), BF), pltpu.VMEM((rows, ff), BF),
            pltpu.VMEM((rows, ff), BF), pltpu.VMEM((rows, 1), F32),
        ],
        compiler_params=params(),
        name="middle",
    )(mixed, tokens, cot, w_out, w_up, w_down, gains, biases, ff_bias)


def tail_kernel(scale, pairs, *refs):
    d_down, d_up, d_out, small_in, projected, g_mixed, tokens, grad_one, long_hbm, short_hbm, w_hbm = refs[:11]
    outs, grad_tokens = refs[11:16], refs[16]
    own = refs[17:]
    n = 5
    half, rx, rpy, rqy, rpz, rqz, rpx, fin, got = (own[i * n : (i + 1) * n] for i in range(9))
    ssem, rsem, lsem, d_qkv, small, heads, long_buf, short_buf, w_qkv = own[9 * n :]
    grads = [d_down, d_up, d_out, d_qkv, small]
    z, y, x, c = place_of()
    zs, yp, xp, cp = peers(z, y, x, c)
    width = tokens.shape[1]
    two = 2 * HD
    sent = []

    def fetch(i):
        return (
            pltpu.make_async_copy(long_hbm.at[2 * i : 2 * i + 2], long_buf.at[i % 2], lsem.at[i % 2]),
            pltpu.make_async_copy(short_hbm.at[2 * i : 2 * i + 2], short_buf.at[i % 2], lsem.at[2 + i % 2]),
        )

    weights = pltpu.make_async_copy(w_hbm, w_qkv, lsem.at[4])
    weights.start()
    for copy in fetch(0):
        copy.start()
    small[...] = small_in[...]
    greet(zs, yp, xp, cp)

    def go(w, i, src, dst, peer):
        copy = remote(src, dst, ssem.at[w, i], rsem.at[w, i], peer)
        copy.start()
        sent.append(copy)

    def arrive(w, i, ref):
        remote(ref, ref, ssem.at[w, i], rsem.at[w, i], cp).wait_recv()

    def add(*parts):
        total = parts[0].astype(F32)
        for part in parts[1:]:
            total = total + part.astype(F32)
        return total

    def s0(w):
        go(w, 0, grads[w].at[:, :, 1 - c], half[w], cp)

    def s1(w):
        arrive(w, 0, half[w])
        a = half[w]

        @pl.loop(0, 4)
        def _(i):
            for j in range(2):
                for k in range(3):
                    a[i, j, k] = add(grads[w][i, j, c, k], a[i, j, k]).astype(a.dtype)

        go(w, 1, a.at[:, :, 2 * (1 - x)], rx[w], xp)
        go(w, 2, a.at[:, 1 - y, 1], rpy[w], yp)

    def s2p(w):
        a = half[w]
        arrive(w, 2, rpy[w])

        @pl.loop(0, 4)
        def _(i):
            a[i, y, 1] = add(a[i, y, 1], rpy[w][i]).astype(a.dtype)

        for k in range(3):
            go(w, 3 + k, a.at[(z + k + 1) % 4, y, 1], rpz[w].at[k], zs[k])

    def s2q(w):
        a = half[w]
        arrive(w, 1, rx[w])

        @pl.loop(0, 4)
        def _(i):
            for j in range(2):
                a[i, j, 2 * x] = add(a[i, j, 2 * x], rx[w][i, j]).astype(a.dtype)

        go(w, 6, a.at[:, 1 - y, 2 * x], rqy[w], yp)

    def s3p(w):
        a = half[w]
        for k in range(3):
            arrive(w, 3 + k, rpz[w].at[k])
        a[z, y, 1] = add(a[z, y, 1], rpz[w][0], rpz[w][1], rpz[w][2]).astype(a.dtype)
        go(w, 10, a.at[z, y, 1], rpx[w], xp)

    def s3q(w):
        a = half[w]
        arrive(w, 6, rqy[w])

        @pl.loop(0, 4)
        def _(i):
            a[i, y, 2 * x] = add(a[i, y, 2 * x], rqy[w][i]).astype(a.dtype)

        for k in range(3):
            go(w, 7 + k, a.at[(z + k + 1) % 4, y, 2 * x], rqz[w].at[k], zs[k])

    def s4p(w):
        a = half[w]
        arrive(w, 10, rpx[w])
        fin[w][1] = add(a[z, y, 1], rpx[w][...]).astype(a.dtype)
        go(w, 14, fin[w].at[1], got[w].at[c, 1], cp)

    def s4q(w):
        a = half[w]
        for k in range(3):
            arrive(w, 7 + k, rqz[w].at[k])
        fin[w][0] = add(a[z, y, 2 * x], rqz[w][0], rqz[w][1], rqz[w][2]).astype(a.dtype)
        go(w, 11, fin[w].at[0], got[w].at[c, 2 * x], xp)
        go(w, 13, fin[w].at[0], got[w].at[c, 2 * x], cp)

    def s5(w):
        arrive(w, 11, got[w].at[c, 2 * (1 - x)])
        piece = got[w].at[c, 2 * (1 - x)]
        go(w, 12, piece, piece, cp)
        outs[w][c, 2 * x] = fin[w][0].astype(F32)
        outs[w][c, 1] = fin[w][1].astype(F32)
        outs[w][c, 2 * (1 - x)] = got[w][c, 2 * (1 - x)].astype(F32)

    def s6(w):
        arrive(w, 12, got[w].at[1 - c, 2 * (1 - x)])
        arrive(w, 13, got[w].at[1 - c, 2 * x])
        arrive(w, 14, got[w].at[1 - c, 1])
        for k in range(3):
            outs[w][1 - c, k] = got[w][1 - c, k].astype(F32)

    def back(i):
        if i + 1 < pairs:
            for copy in fetch(i + 1):
                copy.start()
        for copy in fetch(i):
            copy.wait()
        at = pl.ds(i * two, two)
        attend_back_kernel(
            scale,
            projected.at[:, at],
            projected.at[:, pl.ds(width + i * two, two)],
            projected.at[:, pl.ds(2 * width + i * two, two)],
            g_mixed.at[:, at],
            long_buf.at[i % 2], short_buf.at[i % 2],
            heads.at[:, :, at],
        )

    def weight(k):
        part = 256
        for j in range(width // part):
            at = slice(j * part, (j + 1) * part)
            value = dot(tokens[...], heads[k, :, at], TN).astype(BF)
            d_qkv[:, :, :, :, :, k * width + j * part : k * width + (j + 1) * part] = value.reshape(
                d_qkv.shape[:5] + (part,)
            )
        if k != 1:
            total = jnp.sum(heads[k].astype(F32), axis=0, keepdims=True)
            cut = width // 8
            for i in range(8):
                row = k // 2
                small[i // 2, i % 2, 0, 0, row : row + 1, 0:cut] = total[:, i * cut : (i + 1) * cut]

    def rows_back(i):
        step = tokens.shape[0] // 4
        at = slice(i * step, (i + 1) * step)
        total = grad_one[at, :]
        for k in range(3):
            total = total + dot(heads[k, at, :], w_qkv[:, k * width : (k + 1) * width], NT)
        grad_tokens[at, :] = total

    def run(*steps):
        for f, *which in steps:
            for w in which:
                f(w)

    run(
        (s0, 0, 1, 2), (back, 0, 1), (s1, 0), (back, 2), (s1, 1), (back, 3), (s1, 2), (back, 4),
        (s2p, 0), (back, 5), (s2p, 1), (weight, 0), (s2p, 2), (s2q, 0), (weight, 1, 2),
        (s0, 3, 4), (s3p, 0, 1, 2), (s3q, 0), (s1, 3, 4), (s2q, 1),
        (s2p, 3, 4), (s2q, 2), (s4p, 0, 1, 2), (s4q, 0),
    )
    weights.wait()
    run(
        (s3q, 1, 2), (s5, 0), (rows_back, 0), (s3p, 3, 4), (rows_back, 1), (s2q, 3, 4), (s4q, 1, 2), (rows_back, 2),
        (s3q, 3, 4), (s5, 1, 2), (s4p, 3, 4), (rows_back, 3), (s4q, 3, 4), (s6, 0, 1, 2), (s5, 3, 4),
        (s6, 3, 4),
    )
    for copy in sent:
        copy.wait_send()


def tail(d_down, d_up, d_out, small, projected, g_mixed, tokens, grad_one, long_probs, short_probs, w_qkv):
    rows, wide = projected.shape
    width = wide // 3
    pairs = width // (2 * HD)

    def view(shape):
        return (4, 2, 2, 3, shape[0] // 48, shape[1])

    views = [g.reshape(view(g.shape)) for g in (d_down, d_up, d_out)] + [small.reshape(view(small.shape))]
    qkv_view = view(w_qkv.shape)
    kinds = [(v.shape, v.dtype) for v in views[:3]] + [(qkv_view, BF), (views[3].shape, F32)]
    lead = ((4, 2, 3), (4, 2), (4,), (4,), (3,), (3,), (), (2,), (2, 3))
    scratch = [pltpu.VMEM(s + v[4:], t) for s in lead for v, t in kinds]
    anywhere = pl.BlockSpec(memory_space=pl.ANY)
    results = pl.pallas_call(
        functools.partial(tail_kernel, HD ** (-0.5), pairs),
        out_shape=[jax.ShapeDtypeStruct(v[2:], F32) for v, _ in kinds]
        + [jax.ShapeDtypeStruct((rows, width), F32)],
        in_specs=[vm()] * 8 + [anywhere] * 3,
        out_specs=[vm()] * 6,
        scratch_shapes=scratch
        + [
            pltpu.SemaphoreType.DMA((5, 15)), pltpu.SemaphoreType.DMA((5, 15)),
            pltpu.SemaphoreType.DMA((5,)),
            pltpu.VMEM(qkv_view, BF), pltpu.VMEM(views[3].shape, F32),
            pltpu.VMEM((3, rows, width), BF),
            pltpu.VMEM((2, 2) + long_probs.shape[1:], BF),
            pltpu.VMEM((2, 2) + short_probs.shape[1:], BF),
            pltpu.VMEM(w_qkv.shape, BF),
        ],
        compiler_params=params(collective_id=1, has_side_effects=True),
        name="tail",
    )(*views, projected, g_mixed, tokens, grad_one, long_probs, short_probs, w_qkv)
    flat = [o.reshape(-1, o.shape[-1]) for o in results[:5]]
    return flat, results[5]


def square():
    return lax.axis_size("dp") == 8 and lax.axis_size("rep") == 4


def gather_layer(qkv_weight, out_weight, up_weight, down_weight, norm_gains, bias_rows, ff_bias):
    if not square():
        return (
            lax.all_gather(qkv_weight, "dp", axis=0, tiled=True),
            lax.all_gather(out_weight, "dp", axis=0, tiled=True),
            lax.all_gather(up_weight, "dp", axis=0, tiled=True),
            lax.all_gather(down_weight, "dp", axis=0, tiled=True),
            lax.all_gather(norm_gains, "dp", axis=1, tiled=True),
            lax.all_gather(bias_rows, "dp", axis=1, tiled=True),
            lax.all_gather(ff_bias, "dp", axis=0, tiled=True),
        )
    small = jnp.concatenate([bias_rows.reshape(-1), norm_gains.reshape(-1), ff_bias])
    used = small.shape[0]
    small = jnp.pad(small, (0, 96 * 128 - used)).reshape(96, 128)
    full = gather([small, qkv_weight, out_weight, up_weight, down_weight])
    rows = full[0].reshape(8, 96 * 128)[:, :used]
    nb, ng = bias_rows.size, norm_gains.size
    biases = rows[:, :nb].reshape(8, bias_rows.shape[0], -1).transpose(1, 0, 2)
    gains = rows[:, nb : nb + ng].reshape(8, norm_gains.shape[0], -1).transpose(1, 0, 2)
    return (
        full[1], full[2], full[3], full[4],
        gains.reshape(norm_gains.shape[0], -1),
        biases.reshape(bias_rows.shape[0], -1),
        rows[:, nb + ng :].reshape(-1),
    )


def reduce_layer(d_qkv, d_out, d_up, d_down, d_gains, d_biases, d_up_bias):
    def full(g):
        part = lax.psum_scatter(g, "rep", scatter_dimension=1, tiled=True).astype(F32)
        part = lax.psum_scatter(part, "dp", scatter_dimension=0, tiled=True)
        return lax.all_gather(part.astype(BF), "rep", axis=1, tiled=True).astype(F32)

    small = lax.psum(
        (
            lax.psum_scatter(d_gains, "dp", scatter_dimension=1, tiled=True),
            lax.psum_scatter(d_biases, "dp", scatter_dimension=1, tiled=True),
            lax.psum_scatter(d_up_bias, "dp", scatter_dimension=0, tiled=True),
        ),
        "rep",
    )
    return tuple(full(g.astype(BF)) for g in (d_qkv, d_out, d_up, d_down)) + small


def back_layer(projected, grad_mixed, probs, tokens, grad_one, w_qkv, d_out, d_up, d_down, sums, d_up_bias):
    width = tokens.shape[1]
    if not square():
        parts = attend_back(projected, grad_mixed, *probs)
        grad_heads = jnp.concatenate([parts[0], parts[1], parts[2]], 1)
        d_head = jnp.sum(grad_heads.astype(F32), axis=0)[None]
        d_qkv = dot(tokens, grad_heads, TN)
        grad_tokens = grad_one + dot(grad_heads, w_qkv, NT)
        d_biases = jnp.concatenate([d_head[:, :width], d_head[:, 2 * width :], sums[2:6]])
        return (grad_tokens,) + reduce_layer(d_qkv, d_out, d_up, d_down, sums[0:2], d_biases, d_up_bias)

    def cut(g):
        return g.reshape(g.shape[0], 8, -1).transpose(1, 0, 2).reshape(8, -1)

    rest = jnp.concatenate([cut(sums[0:6]), d_up_bias.reshape(8, -1)], 1)
    n0, n1 = 6 * (width // 8), rest.shape[1]
    small = jnp.pad(rest, ((0, 0), (1024, 5 * 1024 - n1))).reshape(8 * 48, 128)
    (down, up, out, qkv, own), grad_tokens = tail(
        d_down, d_up, d_out, small, projected, grad_mixed, tokens, grad_one, *probs, w_qkv
    )
    own_rest = own[8:].reshape(-1)
    rows = own_rest[:n0].reshape(6, -1)
    biases = jnp.concatenate([own[0:2, : width // 8], rows[2:6]])
    return (grad_tokens, qkv, out, up, down, rows[0:2], biases, own_rest[n0:n1])


def local(
    tokens,
    qkv_weight,
    out_weight,
    up_weight,
    down_weight,
    norm_gains,
    bias_rows,
    ff_bias,
    lengths,
    owners,
    cotangent,
):
    row_count, model_width = tokens.shape
    device = lax.axis_index("dp") * lax.axis_size("rep") + lax.axis_index("rep")
    devices = lax.axis_size("dp") * lax.axis_size("rep")
    per = lengths.shape[0] // devices
    assert row_count == LONG + SHORT * (per - 1)
    me = device.astype(jnp.int32).reshape(1)
    tokens, cotangent, tab = prep(me, owners, lengths, tokens, cotangent, per)
    layer_w = gather_layer(qkv_weight, out_weight, up_weight, down_weight, norm_gains, bias_rows, ff_bias)
    w_qkv, w_out, w_up, w_down, gains_low, biases_low, up_bias_low = layer_w
    gain_rows = gains_low.astype(jnp.float32)
    shift_rows = biases_low.astype(jnp.float32)
    up_bias = up_bias_low.astype(jnp.float32)
    zero_bias = jnp.zeros((model_width,), jnp.float32)
    head_bias = jnp.concatenate([shift_rows[0], zero_bias, shift_rows[1]])
    projected = (jnp.dot(tokens, w_qkv, preferred_element_type=jnp.float32) + head_bias).astype(
        jnp.bfloat16
    )
    mixed_rows, long_probs, short_probs = attend(tab, projected)
    final, grad_one, grad_mixed, d_out, d_up, d_down, sums, d_up_bias = middle(
        mixed_rows, tokens, cotangent, w_out, w_up, w_down, gain_rows, shift_rows, up_bias[None]
    )
    d_up_bias = d_up_bias[0]
    output = unperm(tab, final, per)
    grad_tokens, *rest = back_layer(
        projected, grad_mixed, (long_probs, short_probs), tokens, grad_one, w_qkv,
        d_out, d_up, d_down, sums, d_up_bias,
    )
    return (output, unperm(tab, grad_tokens, per)) + tuple(rest)


def solution(mesh):
    in_specs = (
        P(("dp", "rep"), None),
        P("dp", None),
        P("dp", None),
        P("dp", None),
        P("dp", None),
        P(None, "dp"),
        P(None, "dp"),
        P("dp"),
        P(),
        P(),
        P(("dp", "rep"), None),
    )
    out_specs = (
        P(("dp", "rep"), None),
        P(("dp", "rep"), None),
        P("dp", None),
        P("dp", None),
        P("dp", None),
        P("dp", None),
        P(None, "dp"),
        P(None, "dp"),
        P("dp"),
    )
    return jax.shard_map(local, mesh=mesh, in_specs=in_specs, out_specs=out_specs, check_vma=False)
```

```python
import functools

import jax
import jax.numpy as jnp
from jax import lax
from jax.experimental import pallas as pl
from jax.experimental.pallas import tpu as pltpu
from jax.sharding import PartitionSpec as P

HEADS = 12
HD = 64
LONG = 512
SHORT = 64
norm_eps = 1e-06
masked_score = -1000000000.0
BF = jnp.bfloat16
F32 = jnp.float32
VMEM_LIMIT = 62 * 1024 * 1024

NN = (((1,), (0,)), ((), ()))
NT = (((1,), (1,)), ((), ()))
TN = (((0,), (0,)), ((), ()))


def dot(a, b, dims=NN):
    return lax.dot_general(a, b, dims, preferred_element_type=F32)


def vm():
    return pl.BlockSpec(memory_space=pltpu.VMEM)


def sm():
    return pl.BlockSpec(memory_space=pltpu.SMEM)


def params(**kw):
    return pltpu.CompilerParams(vmem_limit_bytes=VMEM_LIMIT, **kw)


def prep_kernel(per, me_ref, own_ref, len_ref, tok_ref, cot_ref, tok_out, cot_out, tab_ref, wide):
    total = own_ref.shape[0]
    rows = tok_ref.shape[0]
    me = me_ref[0]

    def zero(i, c):
        tab_ref[0, i] = 0
        return c

    lax.fori_loop(0, 128, zero, 0)

    def scan(p, c):
        count, start = c
        hit = own_ref[p] == me
        size = len_ref[p]
        tab_ref[0, count] = start
        tab_ref[0, 16 + count] = size
        return (count + hit.astype(jnp.int32), start + jnp.where(hit, size, 0))

    lax.fori_loop(0, total, scan, (jnp.int32(0), jnp.int32(0)), unroll=8)

    def find(j, c):
        return jnp.where(tab_ref[0, 16 + j] > SHORT, j, c)

    big = lax.fori_loop(0, per, find, jnp.int32(0))

    def place(j, slot):
        is_big = j == big
        tab_ref[0, 32 + j] = jnp.where(is_big, 0, LONG + SHORT * slot)
        tab_ref[0, 48 + j] = jnp.where(is_big, LONG // SHORT, 1)
        at = jnp.where(is_big, 0, slot + 1)
        tab_ref[0, 64 + at] = tab_ref[0, 16 + j]
        return slot + jnp.where(is_big, 0, 1)

    lax.fori_loop(0, per, place, jnp.int32(0))

    for src, dst in ((tok_ref, tok_out), (cot_ref, cot_out)):
        wide[pl.ds(0, rows), :] = src[...].astype(F32)
        wide[pl.ds(rows, LONG + 8), :] = jnp.zeros((LONG + 8, src.shape[1]), F32)

        def passage(j, c):
            start = tab_ref[0, j]
            size = tab_ref[0, 16 + j]
            to = tab_ref[0, 32 + j]

            def chunk(k, c2):
                first = start + k * SHORT
                shift = first % 8
                piece = wide[pl.ds(pl.multiple_of(first - shift, 8), SHORT + 8), :]
                piece = pltpu.roll(piece, (SHORT + 8 - shift) % (SHORT + 8), 0)[:SHORT]
                row = lax.broadcasted_iota(jnp.int32, piece.shape, 0) + k * SHORT
                dst[pl.ds(pl.multiple_of(to + k * SHORT, SHORT), SHORT), :] = jnp.where(
                    row < size, piece, 0.0
                ).astype(BF)
                return c2

            return lax.fori_loop(0, tab_ref[0, 48 + j], chunk, c)

        lax.fori_loop(0, per, passage, 0)


def prep(me, owners, lengths, tokens, cotangent, per):
    rows, width = tokens.shape
    return pl.pallas_call(
        functools.partial(prep_kernel, per),
        out_shape=(
            jax.ShapeDtypeStruct((rows, width), BF),
            jax.ShapeDtypeStruct((rows, width), BF),
            jax.ShapeDtypeStruct((1, 128), jnp.int32),
        ),
        in_specs=[sm(), sm(), sm(), vm(), vm()],
        out_specs=(vm(), vm(), sm()),
        scratch_shapes=[pltpu.VMEM((rows + LONG + 8, width), F32)],
        compiler_params=params(),
        name="prep",
    )(me, owners, lengths, tokens, cotangent)


def unperm_rows(per, tab_ref, src_ref, wide, mask):
    rows = src_ref.shape[0]
    wide[...] = jnp.zeros_like(wide)

    def passage(j, c):
        start = tab_ref[0, j]
        size = tab_ref[0, 16 + j]
        frm = tab_ref[0, 32 + j]

        def chunk(k, c2):
            piece = src_ref[pl.ds(pl.multiple_of(frm + k * SHORT, SHORT), SHORT), :].astype(F32)
            row = lax.broadcasted_iota(jnp.int32, piece.shape, 0) + k * SHORT
            first = start + k * SHORT
            shift = first % 8
            at = pl.ds(pl.multiple_of(first - shift, 8), SHORT + 8)
            piece = jnp.where(row < size, piece, 0.0)
            piece = jnp.concatenate([piece, jnp.zeros((8, piece.shape[1]), F32)], 0)
            piece = pltpu.roll(piece, shift, 0)
            row = lax.broadcasted_iota(jnp.int32, piece.shape, 0)
            wide[at, :] = jnp.where(row >= shift, piece, wide[at, :])
            return c2

        return lax.fori_loop(0, tab_ref[0, 48 + j], chunk, c)

    lax.fori_loop(0, per, passage, 0)


def unperm_kernel(per, tab_ref, src_ref, out_ref, wide):
    unperm_rows(per, tab_ref, src_ref, wide, True)
    out_ref[...] = wide[pl.ds(0, src_ref.shape[0]), :].astype(out_ref.dtype)


def unperm(tab, src, per):
    rows, width = src.shape
    return pl.pallas_call(
        functools.partial(unperm_kernel, per),
        out_shape=jax.ShapeDtypeStruct((rows, width), src.dtype),
        in_specs=[sm(), vm()],
        out_specs=vm(),
        scratch_shapes=[pltpu.VMEM((rows + LONG + 8, width), F32)],
        compiler_params=params(),
        name="unperm",
    )(tab, src)


def place_of():
    dp, rep = lax.axis_index("dp"), lax.axis_index("rep")
    return dp // 2, dp % 2, rep // 2, rep % 2


def peers(z, y, x, c):
    def at(z2, y2, x2, c2):
        return (z2 * 2 + y2, x2 * 2 + c2)

    return (
        [at((z + k) % 4, y, x, c) for k in (1, 2, 3)],
        at(z, 1 - y, x, c),
        at(z, y, 1 - x, c),
        at(z, y, x, 1 - c),
    )


def greet(zs, yp, xp, cp):
    barrier = pltpu.get_barrier_semaphore()
    for peer in (*zs, yp, xp, cp):
        pl.semaphore_signal(barrier, inc=1, device_id=peer, device_id_type=pl.DeviceIdType.MESH)
    pl.semaphore_wait(barrier, 6)


def remote(src, dst, ssem, rsem, peer):
    return pltpu.make_async_remote_copy(
        src_ref=src, dst_ref=dst, send_sem=ssem, recv_sem=rsem,
        device_id=peer, device_id_type=pl.DeviceIdType.MESH,
    )


def blocks(shard):
    rows, columns = shard.shape
    return shard.reshape(2, 3, rows // 6, columns)


def head_lanes(block, head):
    lane = lax.broadcasted_iota(jnp.int32, (1, block.shape[1]), 1)
    keep = jnp.where(lane >= HD, float(head), 1.0 - head)
    return block * keep.astype(BF)


def softmax_keys(scores, valid):
    scores = jnp.where(valid, scores, masked_score)
    weights = jnp.exp(scores - jnp.max(scores, axis=0, keepdims=True))
    return weights * (1.0 / jnp.sum(weights, axis=0, keepdims=True))


def short_valid(tab_ref, pair, size):
    key = lax.broadcasted_iota(jnp.int32, (size, size), 0)
    query = lax.broadcasted_iota(jnp.int32, (size, size), 1)
    low, high = tab_ref[0, 65 + 2 * pair], tab_ref[0, 66 + 2 * pair]
    bound = jnp.where(key >= SHORT, SHORT + high, low)
    return (key < bound) & (key // SHORT == query // SHORT)


def attend_kernel(scale, tab_ref, q_ref, k_ref, v_ref, out_ref, long_ref, short_ref):
    two = 2 * SHORT
    key = lax.broadcasted_iota(jnp.int32, (LONG, LONG), 0)
    valid = key < tab_ref[0, 64]
    shorts = (q_ref.shape[0] - LONG) // two
    keeps = [short_valid(tab_ref, b, two) for b in range(shorts)]
    total = None
    tails = [None] * shorts
    for h in range(2):
        scores = dot(head_lanes(k_ref[0:LONG], h), q_ref[0:LONG], NT) * scale
        probs = softmax_keys(scores, valid).astype(BF)
        long_ref[h] = probs
        part = dot(probs, head_lanes(v_ref[0:LONG], h), TN)
        total = part if total is None else total + part
        for b in range(shorts):
            rows = slice(LONG + b * two, LONG + (b + 1) * two)
            scores = dot(head_lanes(k_ref[rows], h), q_ref[rows], NT) * scale
            probs = softmax_keys(scores, keeps[b]).astype(BF)
            short_ref[h, b * two : (b + 1) * two] = probs
            part = dot(probs, head_lanes(v_ref[rows], h), TN)
            tails[b] = part if tails[b] is None else tails[b] + part
    out_ref[0:LONG] = total.astype(BF)
    for b in range(shorts):
        out_ref[LONG + b * two : LONG + (b + 1) * two] = tails[b].astype(BF)


def attend(tab, projected):
    rows, wide = projected.shape
    width = wide // 3
    pairs = width // (2 * HD)
    column = lambda off: pl.BlockSpec((rows, 2 * HD), lambda i, off=off: (0, off + i))
    return pl.pallas_call(
        functools.partial(attend_kernel, HD ** (-0.5)),
        grid=(pairs,),
        out_shape=(
            jax.ShapeDtypeStruct((rows, width), BF),
            jax.ShapeDtypeStruct((2 * pairs, LONG, LONG), BF),
            jax.ShapeDtypeStruct((2 * pairs, rows - LONG, 2 * SHORT), BF),
        ),
        in_specs=[sm(), column(0), column(pairs), column(2 * pairs)],
        out_specs=(
            column(0),
            pl.BlockSpec((2, LONG, LONG), lambda i: (i, 0, 0)),
            pl.BlockSpec((2, rows - LONG, 2 * SHORT), lambda i: (i, 0, 0)),
        ),
        compiler_params=params(),
        name="attend",
    )(tab, projected, projected, projected)


def attend_back_kernel(scale, q_ref, k_ref, v_ref, g_ref, long_ref, short_ref, out_ref):
    two = 2 * SHORT
    shorts = (q_ref.shape[0] - LONG) // two
    spans = [(slice(0, LONG), None)]
    spans += [(slice(LONG + b * two, LONG + (b + 1) * two), b) for b in range(shorts)]
    for rows, b in spans:
        sums = None
        for h in range(2):
            probs = long_ref[h] if b is None else short_ref[h, b * two : (b + 1) * two]
            grad = head_lanes(g_ref[rows], h)
            wide = probs.astype(F32)
            grad_probs = dot(v_ref[rows], grad, NT)
            mean = jnp.sum(grad_probs * wide, axis=0, keepdims=True)
            grad_scores = (wide * (grad_probs - mean)).astype(BF)
            parts = (
                dot(grad_scores, head_lanes(k_ref[rows], h), TN),
                dot(grad_scores, head_lanes(q_ref[rows], h)),
                dot(probs, grad),
            )
            sums = parts if sums is None else tuple(a + p for a, p in zip(sums, parts))
        out_ref[0, rows] = (sums[0] * scale).astype(BF)
        out_ref[1, rows] = (sums[1] * scale).astype(BF)
        out_ref[2, rows] = sums[2].astype(BF)


def attend_back(projected, grad_mixed, long_probs, short_probs):
    rows, wide = projected.shape
    width = wide // 3
    pairs = width // (2 * HD)
    column = lambda off: pl.BlockSpec((rows, 2 * HD), lambda i, off=off: (0, off + i))
    return pl.pallas_call(
        functools.partial(attend_back_kernel, HD ** (-0.5)),
        grid=(pairs,),
        out_shape=jax.ShapeDtypeStruct((3, rows, width), BF),
        in_specs=[
            column(0), column(pairs), column(2 * pairs), column(0),
            pl.BlockSpec((2, LONG, LONG), lambda i: (i, 0, 0)),
            pl.BlockSpec((2, rows - LONG, 2 * SHORT), lambda i: (i, 0, 0)),
        ],
        out_specs=pl.BlockSpec((3, rows, 2 * HD), lambda i: (0, 0, i)),
        compiler_params=params(),
        name="attend_back",
    )(projected, projected, projected, grad_mixed, long_probs, short_probs)


def gelu_pair(value):
    size = jnp.abs(value)
    bell = jnp.exp(-0.5 * value * value)
    t = 1.0 / (1.0 + 0.23164189 * size)
    tail = t * (0.127414796 + t * (-0.142248368 + t * (0.7107068705 + t * (-0.7265760135 + t * 0.5307027145))))
    tail = tail * bell
    whole = jnp.where(value >= 0.0, 1.0 - tail, tail)
    return (value * whole, whole + value * bell * 0.3989422804)


def middle_kernel(
    step, span, mixed, tokens, cot, w_out, w_up, w_down, gains, biases, ff_bias,
    out, acc, g_mixed, d_out, d_up, d_down, sums, d_ffb, unit, low, low2, hidden, slope, inv
):
    rows = mixed.shape[0]
    parts = w_up.shape[1] // span
    sums[...] = jnp.zeros_like(sums)

    def rows_at(i):
        return pl.ds(pl.multiple_of(i * step, step), step)

    def columns_at(j):
        return pl.ds(pl.multiple_of(j * span, span), span)

    def mean(a):
        return jnp.mean(a, axis=-1, keepdims=True)

    def tally(i, a):
        sums[i : i + 1, :] += jnp.sum(a, axis=0, keepdims=True)

    def norm(r):
        center = r - mean(r)
        scale = lax.rsqrt(mean(center * center) + norm_eps)
        return center * scale, scale

    def back(s, u, scale):
        return scale * (s - mean(s) - u * mean(s * u))

    @pl.loop(0, rows // step)
    def _(i):
        at = rows_at(i)
        branch = dot(mixed[at, :], w_out[...]) + biases[2:3, :]
        u, scale = norm(tokens[at, :].astype(F32) + branch)
        unit[at, :] = u
        inv[at, :] = scale
        low[at, :] = (u * gains[0:1, :] + biases[4:5, :]).astype(BF)
        acc[at, :] = jnp.zeros((step, acc.shape[1]), F32)

    @pl.loop(0, parts)
    def _(j):
        cols = columns_at(j)
        for i in range(rows // step):
            at = slice(i * step, (i + 1) * step)
            inner = dot(low[at, :], w_up[:, cols]) + ff_bias[:, cols]
            act, der = gelu_pair(inner)
            act = act.astype(BF)
            hidden[at, cols] = act
            slope[at, cols] = der.astype(BF)
            acc[at, :] += dot(act, w_down[cols, :])

    @pl.loop(0, rows // step)
    def _(i):
        at = rows_at(i)
        first = unit[at, :] * gains[0:1, :] + biases[4:5, :]
        u, scale = norm(first + acc[at, :] + biases[3:4, :])
        out[at, :] = (u * gains[1:2, :] + biases[5:6, :]).astype(BF)
        g = cot[at, :].astype(F32)
        tally(1, g * u)
        tally(5, g)
        g = back(g * gains[1:2, :], u, scale)
        acc[at, :] = g
        g = g.astype(BF)
        low2[at, :] = g
        tally(3, g.astype(F32))

    @pl.loop(0, parts)
    def _(j):
        cols = columns_at(j)
        total = None
        for i in range(rows // step):
            at = slice(i * step, (i + 1) * step)
            g = dot(low2[at, :], w_down[cols, :], NT) * slope[at, cols].astype(F32)
            g = g.astype(BF)
            slope[at, cols] = g
            part = jnp.sum(g.astype(F32), axis=0, keepdims=True)
            total = part if total is None else total + part
            acc[at, :] += dot(g, w_up[:, cols], NT)
        d_ffb[:, cols] = total
        d_down[cols, :] = dot(hidden[:, cols], low2[...], TN).astype(BF)
        d_up[:, cols] = dot(low[...], slope[:, cols], TN).astype(BF)

    @pl.loop(0, rows // step)
    def _(i):
        at = rows_at(i)
        g, u = acc[at, :], unit[at, :]
        tally(0, g * u)
        tally(4, g)
        g = back(g * gains[0:1, :], u, inv[at, :])
        acc[at, :] = g
        g = g.astype(BF)
        low2[at, :] = g
        tally(2, g.astype(F32))
        g_mixed[at, :] = dot(g, w_out[...], NT).astype(BF)

    d_out[...] = dot(mixed[...], low2[...], TN).astype(BF)


def middle(mixed, tokens, cot, w_out, w_up, w_down, gains, biases, ff_bias):
    rows, width = mixed.shape
    ff = w_up.shape[1]
    shape = jax.ShapeDtypeStruct
    return pl.pallas_call(
        functools.partial(middle_kernel, 256, 512),
        out_shape=(
            shape((rows, width), BF), shape((rows, width), F32), shape((rows, width), BF),
            shape((width, width), BF), shape((width, ff), BF), shape((ff, width), BF),
            shape((8, width), F32), shape((1, ff), F32),
        ),
        in_specs=[vm()] * 9,
        out_specs=(vm(),) * 8,
        scratch_shapes=[
            pltpu.VMEM((rows, width), F32), pltpu.VMEM((rows, width), BF),
            pltpu.VMEM((rows, width), BF), pltpu.VMEM((rows, ff), BF),
            pltpu.VMEM((rows, ff), BF), pltpu.VMEM((rows, 1), F32),
        ],
        compiler_params=params(),
        name="middle",
    )(mixed, tokens, cot, w_out, w_up, w_down, gains, biases, ff_bias)


def head_kernel(scale, pairs, tab, *refs):
    n = 5
    shards, tokens = refs[:n], refs[n]
    fulls = refs[n + 1 : 2 * n + 1]
    projected, mixed, long_hbm, short_hbm = refs[2 * n + 1 : 2 * n + 5]
    ssem, rsem, lsem, osem, bias, long_buf, short_buf = refs[2 * n + 5 :]
    z, y, x, c = place_of()
    zs, yp, xp, cp = peers(z, y, x, c)
    greet(zs, yp, xp, cp)
    width = tokens.shape[1]
    two = 2 * HD
    sent = []

    def go(w, i, src, dst, peer):
        copy = remote(src, dst, ssem.at[w, i], rsem.at[w, i], peer)
        copy.start()
        sent.append(copy)

    def arrive(w, i, ref):
        remote(ref, ref, ssem.at[w, i], rsem.at[w, i], cp).wait_recv()

    def local(w):
        return pltpu.make_async_copy(shards[w], fulls[w].at[z, y], lsem.at[w])

    def near(w):
        local(w).start()
        src = shards[w].at[c, pl.ds(x, 2)]
        dst = fulls[w].at[z, y, c, pl.ds(x, 2)]
        for k in range(3):
            go(w, k, src, dst, zs[k])
        go(w, 3, src, dst, yp)

    def mid_at(w, k):
        zk = (z + 3 - k) % 4
        part = fulls[w].at[zk, y, c, pl.ds(x, 2)]
        arrive(w, k, part)
        go(w, 4 + k, part, part, yp)
        q = fulls[w].at[zk, y, c, 2 * x]
        go(w, 7 + k, q, q, xp)

    def far_at(w, k):
        zk = (z + 4 - k) % 4
        part = fulls[w].at[zk, 1 - y, c, pl.ds(x, 2)]
        arrive(w, 3 + k, part)
        q = fulls[w].at[zk, 1 - y, c, 2 * x]
        go(w, 10 + k, q, q, xp)

    def mid(w):
        for k in range(3):
            mid_at(w, k)

    def far(w):
        for k in range(4):
            far_at(w, k)

    def across(w):
        for k in range(7):
            zk, yk = ((z + 3 - k) % 4, y) if k < 3 else ((z + 7 - k) % 4, 1 - y)
            arrive(w, 7 + k, fulls[w].at[zk, yk, c, 2 * (1 - x)])
            part = fulls[w].at[zk, yk, c]
            go(w, 14 + k, part, part, cp)

    def last(w):
        for k in range(7):
            zk, yk = ((z + 3 - k) % 4, y) if k < 3 else ((z + 7 - k) % 4, 1 - y)
            arrive(w, 14 + k, fulls[w].at[zk, yk, 1 - c])
        local(w).wait()

    def project():
        cut = width // 8
        rows = [fulls[0][i // 2, i % 2, 0, 0].astype(F32) for i in range(8)]
        bias[...] = jnp.zeros_like(bias)
        bias[:, 0:width] = jnp.concatenate([r[0:1, 0:cut] for r in rows], 1)
        bias[:, 2 * width :] = jnp.concatenate([r[1:2, 0:cut] for r in rows], 1)
        span = width // 2

        @pl.loop(0, 6)
        def _(j):
            cols = pl.ds(pl.multiple_of(j * span, span), span)
            part = fulls[1][:, :, :, :, :, cols].reshape(width, span)
            projected[:, cols] = (dot(tokens[...], part) + bias[:, cols]).astype(BF)

    def store(i):
        return (
            pltpu.make_async_copy(long_buf.at[i % 2], long_hbm.at[2 * i : 2 * i + 2], osem.at[i % 2]),
            pltpu.make_async_copy(short_buf.at[i % 2], short_hbm.at[2 * i : 2 * i + 2], osem.at[2 + i % 2]),
        )

    def attend_at(i):
        if i >= 2:
            for copy in store(i - 2):
                copy.wait()
        at = pl.ds(i * two, two)
        attend_kernel(
            scale, tab,
            projected.at[:, at],
            projected.at[:, pl.ds(width + i * two, two)],
            projected.at[:, pl.ds(2 * width + i * two, two)],
            mixed.at[:, at], long_buf.at[i % 2], short_buf.at[i % 2],
        )
        for copy in store(i):
            copy.start()

    for w in range(n):
        near(w)
    mid(0)
    mid(1)
    far(0)
    far(1)
    across(0)
    across(1)
    mid(2)
    last(0)
    last(1)
    far(2)
    project()
    across(2)
    attend_at(0)
    mid_at(3, 0)
    attend_at(1)
    mid_at(3, 1)
    attend_at(2)
    far_at(3, 0)
    mid_at(3, 2)
    attend_at(3)
    far_at(3, 1)
    attend_at(4)
    far_at(3, 2)
    mid_at(4, 0)
    attend_at(5)
    far_at(3, 3)
    last(2)
    mid_at(4, 1)
    far_at(4, 0)
    across(3)
    mid_at(4, 2)
    far_at(4, 1)
    far_at(4, 2)
    far_at(4, 3)
    last(3)
    across(4)
    last(4)
    for i in (pairs - 2, pairs - 1):
        for copy in store(i):
            copy.wait()
    for copy in sent:
        copy.wait_send()


def head(tab, shards, tokens):
    n = len(shards)
    views = [blocks(s) for s in shards]
    rows, width = tokens.shape
    pairs = width // (2 * HD)
    shape = jax.ShapeDtypeStruct
    anywhere = pl.BlockSpec(memory_space=pl.ANY)
    results = pl.pallas_call(
        functools.partial(head_kernel, HD ** (-0.5), pairs),
        out_shape=[shape((4, 2) + v.shape, v.dtype) for v in views]
        + [
            shape((rows, 3 * width), BF), shape((rows, width), BF),
            shape((2 * pairs, LONG, LONG), BF), shape((2 * pairs, rows - LONG, 2 * SHORT), BF),
        ],
        in_specs=[sm()] + [vm()] * (n + 1),
        out_specs=[vm()] * 2 + [anywhere] * 3 + [vm()] * 2 + [anywhere] * 2,
        scratch_shapes=[
            pltpu.SemaphoreType.DMA((n, 21)), pltpu.SemaphoreType.DMA((n, 21)),
            pltpu.SemaphoreType.DMA((n,)), pltpu.SemaphoreType.DMA((4,)),
            pltpu.VMEM((1, 3 * width), F32),
            pltpu.VMEM((2, 2, LONG, LONG), BF), pltpu.VMEM((2, 2, rows - LONG, 2 * SHORT), BF),
        ],
        compiler_params=params(collective_id=0, has_side_effects=True),
        name="head",
    )(tab, *views, tokens)
    return [f.reshape(8 * s.shape[0], s.shape[1]) for f, s in zip(results, shards)], results[n:]


def tail_kernel(scale, pairs, *refs):
    d_down, d_up, d_out, small_in, projected, g_mixed, tokens, grad_one, long_hbm, short_hbm, w_hbm = refs[:11]
    outs, grad_tokens = refs[11:16], refs[16]
    own = refs[17:]
    n = 5
    half, rx, rpy, rqy, rpz, rqz, rpx, fin, got = (own[i * n : (i + 1) * n] for i in range(9))
    ssem, rsem, lsem, d_qkv, small, heads, long_buf, short_buf, w_qkv = own[9 * n :]
    grads = [d_down, d_up, d_out, d_qkv, small]
    z, y, x, c = place_of()
    zs, yp, xp, cp = peers(z, y, x, c)
    width = tokens.shape[1]
    two = 2 * HD
    sent = []

    def fetch(i):
        return (
            pltpu.make_async_copy(long_hbm.at[2 * i : 2 * i + 2], long_buf.at[i % 2], lsem.at[i % 2]),
            pltpu.make_async_copy(short_hbm.at[2 * i : 2 * i + 2], short_buf.at[i % 2], lsem.at[2 + i % 2]),
        )

    weights = pltpu.make_async_copy(w_hbm, w_qkv, lsem.at[4])
    weights.start()
    for copy in fetch(0):
        copy.start()
    small[...] = small_in[...]
    greet(zs, yp, xp, cp)

    def go(w, i, src, dst, peer):
        copy = remote(src, dst, ssem.at[w, i], rsem.at[w, i], peer)
        copy.start()
        sent.append(copy)

    def arrive(w, i, ref):
        remote(ref, ref, ssem.at[w, i], rsem.at[w, i], cp).wait_recv()

    def add(*parts):
        total = parts[0].astype(F32)
        for part in parts[1:]:
            total = total + part.astype(F32)
        return total

    def s0(w):
        go(w, 0, grads[w].at[:, :, 1 - c], half[w], cp)

    def s1(w):
        arrive(w, 0, half[w])
        a = half[w]

        @pl.loop(0, 4)
        def _(i):
            for j in range(2):
                for k in range(3):
                    a[i, j, k] = add(grads[w][i, j, c, k], a[i, j, k]).astype(a.dtype)

        go(w, 1, a.at[:, :, 2 * (1 - x)], rx[w], xp)
        go(w, 2, a.at[:, 1 - y, 1], rpy[w], yp)

    def s2p(w):
        a = half[w]
        arrive(w, 2, rpy[w])

        @pl.loop(0, 4)
        def _(i):
            a[i, y, 1] = add(a[i, y, 1], rpy[w][i]).astype(a.dtype)

        for k in range(3):
            go(w, 3 + k, a.at[(z + k + 1) % 4, y, 1], rpz[w].at[k], zs[k])

    def s2q(w):
        a = half[w]
        arrive(w, 1, rx[w])

        @pl.loop(0, 4)
        def _(i):
            for j in range(2):
                a[i, j, 2 * x] = add(a[i, j, 2 * x], rx[w][i, j]).astype(a.dtype)

        go(w, 6, a.at[:, 1 - y, 2 * x], rqy[w], yp)

    def s3p(w):
        a = half[w]
        for k in range(3):
            arrive(w, 3 + k, rpz[w].at[k])
        a[z, y, 1] = add(a[z, y, 1], rpz[w][0], rpz[w][1], rpz[w][2]).astype(a.dtype)
        go(w, 10, a.at[z, y, 1], rpx[w], xp)

    def s3q(w):
        a = half[w]
        arrive(w, 6, rqy[w])

        @pl.loop(0, 4)
        def _(i):
            a[i, y, 2 * x] = add(a[i, y, 2 * x], rqy[w][i]).astype(a.dtype)

        for k in range(3):
            go(w, 7 + k, a.at[(z + k + 1) % 4, y, 2 * x], rqz[w].at[k], zs[k])

    def s4p(w):
        a = half[w]
        arrive(w, 10, rpx[w])
        fin[w][1] = add(a[z, y, 1], rpx[w][...]).astype(a.dtype)
        go(w, 14, fin[w].at[1], got[w].at[c, 1], cp)

    def s4q(w):
        a = half[w]
        for k in range(3):
            arrive(w, 7 + k, rqz[w].at[k])
        fin[w][0] = add(a[z, y, 2 * x], rqz[w][0], rqz[w][1], rqz[w][2]).astype(a.dtype)
        go(w, 11, fin[w].at[0], got[w].at[c, 2 * x], xp)
        go(w, 13, fin[w].at[0], got[w].at[c, 2 * x], cp)

    def s5(w):
        arrive(w, 11, got[w].at[c, 2 * (1 - x)])
        piece = got[w].at[c, 2 * (1 - x)]
        go(w, 12, piece, piece, cp)
        outs[w][c, 2 * x] = fin[w][0].astype(F32)
        outs[w][c, 1] = fin[w][1].astype(F32)
        outs[w][c, 2 * (1 - x)] = got[w][c, 2 * (1 - x)].astype(F32)

    def s6(w):
        arrive(w, 12, got[w].at[1 - c, 2 * (1 - x)])
        arrive(w, 13, got[w].at[1 - c, 2 * x])
        arrive(w, 14, got[w].at[1 - c, 1])
        for k in range(3):
            outs[w][1 - c, k] = got[w][1 - c, k].astype(F32)

    def back(i):
        if i + 1 < pairs:
            for copy in fetch(i + 1):
                copy.start()
        for copy in fetch(i):
            copy.wait()
        at = pl.ds(i * two, two)
        attend_back_kernel(
            scale,
            projected.at[:, at],
            projected.at[:, pl.ds(width + i * two, two)],
            projected.at[:, pl.ds(2 * width + i * two, two)],
            g_mixed.at[:, at],
            long_buf.at[i % 2], short_buf.at[i % 2],
            heads.at[:, :, at],
        )

    def weight(k):
        part = 256
        for j in range(width // part):
            at = slice(j * part, (j + 1) * part)
            value = dot(tokens[...], heads[k, :, at], TN).astype(BF)
            d_qkv[:, :, :, :, :, k * width + j * part : k * width + (j + 1) * part] = value.reshape(
                d_qkv.shape[:5] + (part,)
            )
        if k != 1:
            total = jnp.sum(heads[k].astype(F32), axis=0, keepdims=True)
            cut = width // 8
            for i in range(8):
                row = k // 2
                small[i // 2, i % 2, 0, 0, row : row + 1, 0:cut] = total[:, i * cut : (i + 1) * cut]

    def rows_back(i):
        step = tokens.shape[0] // 4
        at = slice(i * step, (i + 1) * step)
        total = grad_one[at, :]
        for k in range(3):
            total = total + dot(heads[k, at, :], w_qkv[:, k * width : (k + 1) * width], NT)
        grad_tokens[at, :] = total

    def run(*steps):
        for f, *which in steps:
            for w in which:
                f(w)

    run(
        (s0, 0, 1, 2), (back, 0, 1), (s1, 0), (back, 2), (s1, 1), (back, 3), (s1, 2), (back, 4),
        (s2p, 0), (back, 5), (s2p, 1), (weight, 0), (s2p, 2), (s2q, 0), (weight, 1, 2),
        (s0, 3, 4), (s3p, 0, 1, 2), (s3q, 0), (s1, 3, 4), (s2q, 1),
        (s2p, 3, 4), (s2q, 2), (s4p, 0, 1, 2), (s4q, 0),
    )
    weights.wait()
    run(
        (s3q, 1, 2), (s5, 0), (rows_back, 0), (s3p, 3, 4), (rows_back, 1), (s2q, 3, 4), (s4q, 1, 2), (rows_back, 2),
        (s3q, 3, 4), (s5, 1, 2), (s4p, 3, 4), (rows_back, 3), (s4q, 3, 4), (s6, 0, 1, 2), (s5, 3, 4),
        (s6, 3, 4),
    )
    for copy in sent:
        copy.wait_send()


def tail(d_down, d_up, d_out, small, projected, g_mixed, tokens, grad_one, long_probs, short_probs, w_qkv):
    rows, wide = projected.shape
    width = wide // 3
    pairs = width // (2 * HD)

    def view(shape):
        return (4, 2, 2, 3, shape[0] // 48, shape[1])

    views = [g.reshape(view(g.shape)) for g in (d_down, d_up, d_out)] + [small.reshape(view(small.shape))]
    qkv_view = view(w_qkv.shape)
    kinds = [(v.shape, v.dtype) for v in views[:3]] + [(qkv_view, BF), (views[3].shape, F32)]
    lead = ((4, 2, 3), (4, 2), (4,), (4,), (3,), (3,), (), (2,), (2, 3))
    scratch = [pltpu.VMEM(s + v[4:], t) for s in lead for v, t in kinds]
    anywhere = pl.BlockSpec(memory_space=pl.ANY)
    results = pl.pallas_call(
        functools.partial(tail_kernel, HD ** (-0.5), pairs),
        out_shape=[jax.ShapeDtypeStruct(v[2:], F32) for v, _ in kinds]
        + [jax.ShapeDtypeStruct((rows, width), F32)],
        in_specs=[vm()] * 8 + [anywhere] * 3,
        out_specs=[vm()] * 6,
        scratch_shapes=scratch
        + [
            pltpu.SemaphoreType.DMA((5, 15)), pltpu.SemaphoreType.DMA((5, 15)),
            pltpu.SemaphoreType.DMA((5,)),
            pltpu.VMEM(qkv_view, BF), pltpu.VMEM(views[3].shape, F32),
            pltpu.VMEM((3, rows, width), BF),
            pltpu.VMEM((2, 2) + long_probs.shape[1:], BF),
            pltpu.VMEM((2, 2) + short_probs.shape[1:], BF),
            pltpu.VMEM(w_qkv.shape, BF),
        ],
        compiler_params=params(collective_id=1, has_side_effects=True),
        name="tail",
    )(*views, projected, g_mixed, tokens, grad_one, long_probs, short_probs, w_qkv)
    flat = [o.reshape(-1, o.shape[-1]) for o in results[:5]]
    return flat, results[5]


def square():
    return lax.axis_size("dp") == 8 and lax.axis_size("rep") == 4


def front_layer(tab, tokens, qkv_weight, out_weight, up_weight, down_weight, norm_gains, bias_rows, ff_bias):
    width = tokens.shape[1]
    if not square():
        w_qkv, w_out, w_up, w_down = (
            lax.all_gather(w, "dp", axis=0, tiled=True)
            for w in (qkv_weight, out_weight, up_weight, down_weight)
        )
        gains = lax.all_gather(norm_gains, "dp", axis=1, tiled=True)
        biases = lax.all_gather(bias_rows, "dp", axis=1, tiled=True)
        up_bias = lax.all_gather(ff_bias, "dp", axis=0, tiled=True)
        wide = biases.astype(F32)
        bias = jnp.concatenate([wide[0], jnp.zeros((width,), F32), wide[1]])
        projected = (dot(tokens, w_qkv) + bias).astype(BF)
        mixed, *probs = attend(tab, projected)
        return (w_qkv, w_out, w_up, w_down, gains, biases, up_bias, projected, mixed, tuple(probs))

    cut = width // 8
    kept = bias_rows.shape[0] - 2
    rest = jnp.concatenate([bias_rows[2:].reshape(-1), norm_gains.reshape(-1), ff_bias])
    used = rest.shape[0]
    first = jnp.pad(bias_rows[:2], ((0, 14), (0, 128 - cut)))
    rest = jnp.pad(rest, (0, 80 * 128 - used)).reshape(80, 128)
    small = jnp.concatenate([first, rest])
    full, (projected, mixed, *probs) = head(
        tab, [small, qkv_weight, out_weight, up_weight, down_weight], tokens
    )
    rows = full[0].reshape(8, 96, 128)
    lead = rows[:, :2, :cut]
    rows = rows[:, 16:].reshape(8, -1)[:, :used]
    nb, ng = kept * cut, norm_gains.shape[0] * cut
    biases = jnp.concatenate([lead, rows[:, :nb].reshape(8, kept, cut)], 1).transpose(1, 0, 2)
    gains = rows[:, nb : nb + ng].reshape(8, -1, cut).transpose(1, 0, 2)
    return (
        full[1], full[2], full[3], full[4],
        gains.reshape(-1, width), biases.reshape(-1, width), rows[:, nb + ng :].reshape(-1),
        projected, mixed, tuple(probs),
    )


def reduce_layer(d_qkv, d_out, d_up, d_down, d_gains, d_biases, d_up_bias):
    def full(g):
        part = lax.psum_scatter(g, "rep", scatter_dimension=1, tiled=True).astype(F32)
        part = lax.psum_scatter(part, "dp", scatter_dimension=0, tiled=True)
        return lax.all_gather(part.astype(BF), "rep", axis=1, tiled=True).astype(F32)

    small = lax.psum(
        (
            lax.psum_scatter(d_gains, "dp", scatter_dimension=1, tiled=True),
            lax.psum_scatter(d_biases, "dp", scatter_dimension=1, tiled=True),
            lax.psum_scatter(d_up_bias, "dp", scatter_dimension=0, tiled=True),
        ),
        "rep",
    )
    return tuple(full(g.astype(BF)) for g in (d_qkv, d_out, d_up, d_down)) + small


def back_layer(projected, grad_mixed, probs, tokens, grad_one, w_qkv, d_out, d_up, d_down, sums, d_up_bias):
    width = tokens.shape[1]
    if not square():
        parts = attend_back(projected, grad_mixed, *probs)
        grad_heads = jnp.concatenate([parts[0], parts[1], parts[2]], 1)
        d_head = jnp.sum(grad_heads.astype(F32), axis=0)[None]
        d_qkv = dot(tokens, grad_heads, TN)
        grad_tokens = grad_one + dot(grad_heads, w_qkv, NT)
        d_biases = jnp.concatenate([d_head[:, :width], d_head[:, 2 * width :], sums[2:6]])
        return (grad_tokens,) + reduce_layer(d_qkv, d_out, d_up, d_down, sums[0:2], d_biases, d_up_bias)

    def cut(g):
        return g.reshape(g.shape[0], 8, -1).transpose(1, 0, 2).reshape(8, -1)

    rest = jnp.concatenate([cut(sums[0:6]), d_up_bias.reshape(8, -1)], 1)
    n0, n1 = 6 * (width // 8), rest.shape[1]
    small = jnp.pad(rest, ((0, 0), (1024, 5 * 1024 - n1))).reshape(8 * 48, 128)
    (down, up, out, qkv, own), grad_tokens = tail(
        d_down, d_up, d_out, small, projected, grad_mixed, tokens, grad_one, *probs, w_qkv
    )
    own_rest = own[8:].reshape(-1)
    rows = own_rest[:n0].reshape(6, -1)
    biases = jnp.concatenate([own[0:2, : width // 8], rows[2:6]])
    return (grad_tokens, qkv, out, up, down, rows[0:2], biases, own_rest[n0:n1])


def local(
    tokens,
    qkv_weight,
    out_weight,
    up_weight,
    down_weight,
    norm_gains,
    bias_rows,
    ff_bias,
    lengths,
    owners,
    cotangent,
):
    row_count = tokens.shape[0]
    device = lax.axis_index("dp") * lax.axis_size("rep") + lax.axis_index("rep")
    devices = lax.axis_size("dp") * lax.axis_size("rep")
    per = lengths.shape[0] // devices
    assert row_count == LONG + SHORT * (per - 1)
    me = device.astype(jnp.int32).reshape(1)
    tokens, cotangent, tab = prep(me, owners, lengths, tokens, cotangent, per)
    w_qkv, w_out, w_up, w_down, gains, biases, up_bias, projected, mixed_rows, probs = front_layer(
        tab, tokens, qkv_weight, out_weight, up_weight, down_weight, norm_gains, bias_rows, ff_bias
    )
    gain_rows = gains.astype(F32)
    shift_rows = biases.astype(F32)
    up_bias = up_bias.astype(F32)
    final, grad_one, grad_mixed, d_out, d_up, d_down, sums, d_up_bias = middle(
        mixed_rows, tokens, cotangent, w_out, w_up, w_down, gain_rows, shift_rows, up_bias[None]
    )
    d_up_bias = d_up_bias[0]
    output = unperm(tab, final, per)
    grad_tokens, *rest = back_layer(
        projected, grad_mixed, probs, tokens, grad_one, w_qkv,
        d_out, d_up, d_down, sums, d_up_bias,
    )
    return (output, unperm(tab, grad_tokens, per)) + tuple(rest)


def solution(mesh):
    in_specs = (
        P(("dp", "rep"), None),
        P("dp", None),
        P("dp", None),
        P("dp", None),
        P("dp", None),
        P(None, "dp"),
        P(None, "dp"),
        P("dp"),
        P(),
        P(),
        P(("dp", "rep"), None),
    )
    out_specs = (
        P(("dp", "rep"), None),
        P(("dp", "rep"), None),
        P("dp", None),
        P("dp", None),
        P("dp", None),
        P("dp", None),
        P(None, "dp"),
        P(None, "dp"),
        P("dp"),
    )
    return jax.shard_map(local, mesh=mesh, in_specs=in_specs, out_specs=out_specs, check_vma=False)
```

```python
import functools

import jax
import jax.numpy as jnp
from jax import lax
from jax.experimental import pallas as pl
from jax.experimental.pallas import tpu as pltpu
from jax.sharding import PartitionSpec as P

HEADS = 12
HD = 64
LONG = 512
SHORT = 64
norm_eps = 1e-06
masked_score = -1000000000.0
BF = jnp.bfloat16
F32 = jnp.float32
VMEM_LIMIT = 62 * 1024 * 1024

NN = (((1,), (0,)), ((), ()))
NT = (((1,), (1,)), ((), ()))
TN = (((0,), (0,)), ((), ()))


def dot(a, b, dims=NN):
    return lax.dot_general(a, b, dims, preferred_element_type=F32)


def vm():
    return pl.BlockSpec(memory_space=pltpu.VMEM)


def sm():
    return pl.BlockSpec(memory_space=pltpu.SMEM)


def params(**kw):
    return pltpu.CompilerParams(vmem_limit_bytes=VMEM_LIMIT, **kw)


def prep_kernel(per, me_ref, own_ref, len_ref, tok_ref, cot_ref, tok_out, cot_out, tab_ref, wide):
    total = own_ref.shape[0]
    rows = tok_ref.shape[0]
    me = me_ref[0]

    def zero(i, c):
        tab_ref[0, i] = 0
        return c

    lax.fori_loop(0, 128, zero, 0)

    def scan(p, c):
        count, start = c
        hit = own_ref[p] == me
        size = len_ref[p]
        tab_ref[0, count] = start
        tab_ref[0, 16 + count] = size
        return (count + hit.astype(jnp.int32), start + jnp.where(hit, size, 0))

    lax.fori_loop(0, total, scan, (jnp.int32(0), jnp.int32(0)), unroll=8)

    def find(j, c):
        return jnp.where(tab_ref[0, 16 + j] > SHORT, j, c)

    big = lax.fori_loop(0, per, find, jnp.int32(0))

    def place(j, slot):
        is_big = j == big
        tab_ref[0, 32 + j] = jnp.where(is_big, 0, LONG + SHORT * slot)
        tab_ref[0, 48 + j] = jnp.where(is_big, LONG // SHORT, 1)
        at = jnp.where(is_big, 0, slot + 1)
        tab_ref[0, 64 + at] = tab_ref[0, 16 + j]
        return slot + jnp.where(is_big, 0, 1)

    lax.fori_loop(0, per, place, jnp.int32(0))

    for src, dst in ((tok_ref, tok_out), (cot_ref, cot_out)):
        wide[pl.ds(0, rows), :] = src[...].astype(F32)
        wide[pl.ds(rows, LONG + 8), :] = jnp.zeros((LONG + 8, src.shape[1]), F32)

        def passage(j, c):
            start = tab_ref[0, j]
            size = tab_ref[0, 16 + j]
            to = tab_ref[0, 32 + j]

            def chunk(k, c2):
                first = start + k * SHORT
                shift = first % 8
                piece = wide[pl.ds(pl.multiple_of(first - shift, 8), SHORT + 8), :]
                piece = pltpu.roll(piece, (SHORT + 8 - shift) % (SHORT + 8), 0)[:SHORT]
                row = lax.broadcasted_iota(jnp.int32, piece.shape, 0) + k * SHORT
                dst[pl.ds(pl.multiple_of(to + k * SHORT, SHORT), SHORT), :] = jnp.where(
                    row < size, piece, 0.0
                ).astype(BF)
                return c2

            return lax.fori_loop(0, tab_ref[0, 48 + j], chunk, c)

        lax.fori_loop(0, per, passage, 0)


def prep(me, owners, lengths, tokens, cotangent, per):
    rows, width = tokens.shape
    return pl.pallas_call(
        functools.partial(prep_kernel, per),
        out_shape=(
            jax.ShapeDtypeStruct((rows, width), BF),
            jax.ShapeDtypeStruct((rows, width), BF),
            jax.ShapeDtypeStruct((1, 128), jnp.int32),
        ),
        in_specs=[sm(), sm(), sm(), vm(), vm()],
        out_specs=(vm(), vm(), sm()),
        scratch_shapes=[pltpu.VMEM((rows + LONG + 8, width), F32)],
        compiler_params=params(),
        name="prep",
    )(me, owners, lengths, tokens, cotangent)


def unperm_rows(per, tab_ref, src_ref, wide, mask):
    rows = src_ref.shape[0]
    wide[...] = jnp.zeros_like(wide)

    def passage(j, c):
        start = tab_ref[0, j]
        size = tab_ref[0, 16 + j]
        frm = tab_ref[0, 32 + j]

        def chunk(k, c2):
            piece = src_ref[pl.ds(pl.multiple_of(frm + k * SHORT, SHORT), SHORT), :].astype(F32)
            row = lax.broadcasted_iota(jnp.int32, piece.shape, 0) + k * SHORT
            first = start + k * SHORT
            shift = first % 8
            at = pl.ds(pl.multiple_of(first - shift, 8), SHORT + 8)
            piece = jnp.where(row < size, piece, 0.0)
            piece = jnp.concatenate([piece, jnp.zeros((8, piece.shape[1]), F32)], 0)
            piece = pltpu.roll(piece, shift, 0)
            row = lax.broadcasted_iota(jnp.int32, piece.shape, 0)
            wide[at, :] = jnp.where(row >= shift, piece, wide[at, :])
            return c2

        return lax.fori_loop(0, tab_ref[0, 48 + j], chunk, c)

    lax.fori_loop(0, per, passage, 0)


def unperm_kernel(per, tab_ref, src_ref, out_ref, wide):
    unperm_rows(per, tab_ref, src_ref, wide, True)
    out_ref[...] = wide[pl.ds(0, src_ref.shape[0]), :].astype(out_ref.dtype)


def unperm(tab, src, per):
    rows, width = src.shape
    return pl.pallas_call(
        functools.partial(unperm_kernel, per),
        out_shape=jax.ShapeDtypeStruct((rows, width), src.dtype),
        in_specs=[sm(), vm()],
        out_specs=vm(),
        scratch_shapes=[pltpu.VMEM((rows + LONG + 8, width), F32)],
        compiler_params=params(),
        name="unperm",
    )(tab, src)


def place_of():
    dp, rep = lax.axis_index("dp"), lax.axis_index("rep")
    return dp // 2, dp % 2, rep // 2, rep % 2


def peers(z, y, x, c):
    def at(z2, y2, x2, c2):
        return (z2 * 2 + y2, x2 * 2 + c2)

    return (
        [at((z + k) % 4, y, x, c) for k in (1, 2, 3)],
        at(z, 1 - y, x, c),
        at(z, y, 1 - x, c),
        at(z, y, x, 1 - c),
    )


def greet(zs, yp, xp, cp):
    barrier = pltpu.get_barrier_semaphore()
    for peer in (*zs, yp, xp, cp):
        pl.semaphore_signal(barrier, inc=1, device_id=peer, device_id_type=pl.DeviceIdType.MESH)
    pl.semaphore_wait(barrier, 6)


def remote(src, dst, ssem, rsem, peer):
    return pltpu.make_async_remote_copy(
        src_ref=src, dst_ref=dst, send_sem=ssem, recv_sem=rsem,
        device_id=peer, device_id_type=pl.DeviceIdType.MESH,
    )


def blocks(shard):
    rows, columns = shard.shape
    return shard.reshape(2, 3, rows // 6, columns)


def head_lanes(block, head):
    lane = lax.broadcasted_iota(jnp.int32, (1, block.shape[1]), 1)
    keep = jnp.where(lane >= HD, float(head), 1.0 - head)
    return block * keep.astype(BF)


def softmax_keys(scores, valid):
    scores = jnp.where(valid, scores, masked_score)
    weights = jnp.exp(scores - jnp.max(scores, axis=0, keepdims=True))
    return weights * (1.0 / jnp.sum(weights, axis=0, keepdims=True))


def short_valid(tab_ref, pair, size):
    key = lax.broadcasted_iota(jnp.int32, (size, size), 0)
    query = lax.broadcasted_iota(jnp.int32, (size, size), 1)
    low, high = tab_ref[0, 65 + 2 * pair], tab_ref[0, 66 + 2 * pair]
    bound = jnp.where(key >= SHORT, SHORT + high, low)
    return (key < bound) & (key // SHORT == query // SHORT)


def attend_kernel(scale, tab_ref, q_ref, k_ref, v_ref, out_ref, long_ref, short_ref):
    two = 2 * SHORT
    key = lax.broadcasted_iota(jnp.int32, (LONG, LONG), 0)
    valid = key < tab_ref[0, 64]
    shorts = (q_ref.shape[0] - LONG) // two
    keeps = [short_valid(tab_ref, b, two) for b in range(shorts)]
    total = None
    tails = [None] * shorts
    for h in range(2):
        scores = dot(head_lanes(k_ref[0:LONG], h), q_ref[0:LONG], NT) * scale
        probs = softmax_keys(scores, valid).astype(BF)
        long_ref[h] = probs
        part = dot(probs, head_lanes(v_ref[0:LONG], h), TN)
        total = part if total is None else total + part
        for b in range(shorts):
            rows = slice(LONG + b * two, LONG + (b + 1) * two)
            scores = dot(head_lanes(k_ref[rows], h), q_ref[rows], NT) * scale
            probs = softmax_keys(scores, keeps[b]).astype(BF)
            short_ref[h, b * two : (b + 1) * two] = probs
            part = dot(probs, head_lanes(v_ref[rows], h), TN)
            tails[b] = part if tails[b] is None else tails[b] + part
    out_ref[0:LONG] = total.astype(BF)
    for b in range(shorts):
        out_ref[LONG + b * two : LONG + (b + 1) * two] = tails[b].astype(BF)


def attend(tab, projected):
    rows, wide = projected.shape
    width = wide // 3
    pairs = width // (2 * HD)
    column = lambda off: pl.BlockSpec((rows, 2 * HD), lambda i, off=off: (0, off + i))
    return pl.pallas_call(
        functools.partial(attend_kernel, HD ** (-0.5)),
        grid=(pairs,),
        out_shape=(
            jax.ShapeDtypeStruct((rows, width), BF),
            jax.ShapeDtypeStruct((2 * pairs, LONG, LONG), BF),
            jax.ShapeDtypeStruct((2 * pairs, rows - LONG, 2 * SHORT), BF),
        ),
        in_specs=[sm(), column(0), column(pairs), column(2 * pairs)],
        out_specs=(
            column(0),
            pl.BlockSpec((2, LONG, LONG), lambda i: (i, 0, 0)),
            pl.BlockSpec((2, rows - LONG, 2 * SHORT), lambda i: (i, 0, 0)),
        ),
        compiler_params=params(),
        name="attend",
    )(tab, projected, projected, projected)


def attend_back_kernel(scale, q_ref, k_ref, v_ref, g_ref, long_ref, short_ref, out_ref):
    two = 2 * SHORT
    shorts = (q_ref.shape[0] - LONG) // two
    spans = [(slice(0, LONG), None)]
    spans += [(slice(LONG + b * two, LONG + (b + 1) * two), b) for b in range(shorts)]
    for rows, b in spans:
        sums = None
        for h in range(2):
            probs = long_ref[h] if b is None else short_ref[h, b * two : (b + 1) * two]
            grad = head_lanes(g_ref[rows], h)
            wide = probs.astype(F32)
            grad_probs = dot(v_ref[rows], grad, NT)
            mean = jnp.sum(grad_probs * wide, axis=0, keepdims=True)
            grad_scores = (wide * (grad_probs - mean)).astype(BF)
            parts = (
                dot(grad_scores, head_lanes(k_ref[rows], h), TN),
                dot(grad_scores, head_lanes(q_ref[rows], h)),
                dot(probs, grad),
            )
            sums = parts if sums is None else tuple(a + p for a, p in zip(sums, parts))
        out_ref[0, rows] = (sums[0] * scale).astype(BF)
        out_ref[1, rows] = (sums[1] * scale).astype(BF)
        out_ref[2, rows] = sums[2].astype(BF)


def attend_back(projected, grad_mixed, long_probs, short_probs):
    rows, wide = projected.shape
    width = wide // 3
    pairs = width // (2 * HD)
    column = lambda off: pl.BlockSpec((rows, 2 * HD), lambda i, off=off: (0, off + i))
    return pl.pallas_call(
        functools.partial(attend_back_kernel, HD ** (-0.5)),
        grid=(pairs,),
        out_shape=jax.ShapeDtypeStruct((3, rows, width), BF),
        in_specs=[
            column(0), column(pairs), column(2 * pairs), column(0),
            pl.BlockSpec((2, LONG, LONG), lambda i: (i, 0, 0)),
            pl.BlockSpec((2, rows - LONG, 2 * SHORT), lambda i: (i, 0, 0)),
        ],
        out_specs=pl.BlockSpec((3, rows, 2 * HD), lambda i: (0, 0, i)),
        compiler_params=params(),
        name="attend_back",
    )(projected, projected, projected, grad_mixed, long_probs, short_probs)


def gelu_pair(value):
    size = jnp.abs(value)
    bell = jnp.exp(-0.5 * value * value)
    t = 1.0 / (1.0 + 0.23164189 * size)
    tail = t * (0.127414796 + t * (-0.142248368 + t * (0.7107068705 + t * (-0.7265760135 + t * 0.5307027145))))
    tail = tail * bell
    whole = jnp.where(value >= 0.0, 1.0 - tail, tail)
    return (value * whole, whole + value * bell * 0.3989422804)


def middle_kernel(
    step, span, mixed, tokens, cot, w_out, w_up, w_down, gains, biases, ff_bias,
    out, acc, g_mixed, d_out, d_up, d_down, sums, d_ffb, unit, low, low2, hidden, slope, inv
):
    rows = mixed.shape[0]
    parts = w_up.shape[1] // span
    sums[...] = jnp.zeros_like(sums)

    def rows_at(i):
        return pl.ds(pl.multiple_of(i * step, step), step)

    def columns_at(j):
        return pl.ds(pl.multiple_of(j * span, span), span)

    def mean(a):
        return jnp.mean(a, axis=-1, keepdims=True)

    def tally(i, a):
        sums[i : i + 1, :] += jnp.sum(a, axis=0, keepdims=True)

    def norm(r):
        center = r - mean(r)
        scale = lax.rsqrt(mean(center * center) + norm_eps)
        return center * scale, scale

    def back(s, u, scale):
        return scale * (s - mean(s) - u * mean(s * u))

    @pl.loop(0, rows // step)
    def _(i):
        at = rows_at(i)
        branch = dot(mixed[at, :], w_out[...]) + biases[2:3, :]
        u, scale = norm(tokens[at, :].astype(F32) + branch)
        unit[at, :] = u
        inv[at, :] = scale
        low[at, :] = (u * gains[0:1, :] + biases[4:5, :]).astype(BF)
        acc[at, :] = jnp.zeros((step, acc.shape[1]), F32)

    @pl.loop(0, parts)
    def _(j):
        cols = columns_at(j)
        for i in range(rows // step):
            at = slice(i * step, (i + 1) * step)
            inner = dot(low[at, :], w_up[:, cols]) + ff_bias[:, cols]
            act, der = gelu_pair(inner)
            act = act.astype(BF)
            hidden[at, cols] = act
            slope[at, cols] = der.astype(BF)
            acc[at, :] += dot(act, w_down[cols, :])

    @pl.loop(0, rows // step)
    def _(i):
        at = rows_at(i)
        first = unit[at, :] * gains[0:1, :] + biases[4:5, :]
        u, scale = norm(first + acc[at, :] + biases[3:4, :])
        out[at, :] = (u * gains[1:2, :] + biases[5:6, :]).astype(BF)
        g = cot[at, :].astype(F32)
        tally(1, g * u)
        tally(5, g)
        g = back(g * gains[1:2, :], u, scale)
        acc[at, :] = g
        g = g.astype(BF)
        low2[at, :] = g
        tally(3, g.astype(F32))

    @pl.loop(0, parts)
    def _(j):
        cols = columns_at(j)
        total = None
        for i in range(rows // step):
            at = slice(i * step, (i + 1) * step)
            g = dot(low2[at, :], w_down[cols, :], NT) * slope[at, cols].astype(F32)
            g = g.astype(BF)
            slope[at, cols] = g
            part = jnp.sum(g.astype(F32), axis=0, keepdims=True)
            total = part if total is None else total + part
            acc[at, :] += dot(g, w_up[:, cols], NT)
        d_ffb[:, cols] = total
        d_down[cols, :] = dot(hidden[:, cols], low2[...], TN).astype(BF)
        d_up[:, cols] = dot(low[...], slope[:, cols], TN).astype(BF)

    @pl.loop(0, rows // step)
    def _(i):
        at = rows_at(i)
        g, u = acc[at, :], unit[at, :]
        tally(0, g * u)
        tally(4, g)
        g = back(g * gains[0:1, :], u, inv[at, :])
        acc[at, :] = g
        g = g.astype(BF)
        low2[at, :] = g
        tally(2, g.astype(F32))
        g_mixed[at, :] = dot(g, w_out[...], NT).astype(BF)

    d_out[...] = dot(mixed[...], low2[...], TN).astype(BF)


def middle(mixed, tokens, cot, w_out, w_up, w_down, gains, biases, ff_bias):
    rows, width = mixed.shape
    ff = w_up.shape[1]
    shape = jax.ShapeDtypeStruct
    return pl.pallas_call(
        functools.partial(middle_kernel, 256, 512),
        out_shape=(
            shape((rows, width), BF), shape((rows, width), F32), shape((rows, width), BF),
            shape((width, width), BF), shape((width, ff), BF), shape((ff, width), BF),
            shape((8, width), F32), shape((1, ff), F32),
        ),
        in_specs=[vm()] * 9,
        out_specs=(vm(),) * 8,
        scratch_shapes=[
            pltpu.VMEM((rows, width), F32), pltpu.VMEM((rows, width), BF),
            pltpu.VMEM((rows, width), BF), pltpu.VMEM((rows, ff), BF),
            pltpu.VMEM((rows, ff), BF), pltpu.VMEM((rows, 1), F32),
        ],
        compiler_params=params(),
        name="middle",
    )(mixed, tokens, cot, w_out, w_up, w_down, gains, biases, ff_bias)


def head_kernel(scale, pairs, tab, *refs):
    n = 5
    shards, tokens = refs[:n], refs[n]
    fulls = refs[n + 1 : 2 * n + 1]
    projected, mixed, long_hbm, short_hbm = refs[2 * n + 1 : 2 * n + 5]
    ssem, rsem, lsem, osem, bias, long_buf, short_buf = refs[2 * n + 5 :]
    z, y, x, c = place_of()
    zs, yp, xp, cp = peers(z, y, x, c)
    greet(zs, yp, xp, cp)
    width = tokens.shape[1]
    two = 2 * HD
    sent = []

    def go(w, i, src, dst, peer):
        copy = remote(src, dst, ssem.at[w, i], rsem.at[w, i], peer)
        copy.start()
        sent.append(copy)

    def arrive(w, i, ref):
        remote(ref, ref, ssem.at[w, i], rsem.at[w, i], cp).wait_recv()

    def local(w):
        return pltpu.make_async_copy(shards[w], fulls[w].at[z, y], lsem.at[w])

    def near(w):
        local(w).start()
        src = shards[w].at[c, pl.ds(x, 2)]
        dst = fulls[w].at[z, y, c, pl.ds(x, 2)]
        for k in range(3):
            go(w, k, src, dst, zs[k])
        go(w, 3, src, dst, yp)

    def mid_at(w, k):
        zk = (z + 3 - k) % 4
        part = fulls[w].at[zk, y, c, pl.ds(x, 2)]
        arrive(w, k, part)
        go(w, 4 + k, part, part, yp)
        q = fulls[w].at[zk, y, c, 2 * x]
        go(w, 7 + k, q, q, xp)

    def far_at(w, k):
        zk = (z + 4 - k) % 4
        part = fulls[w].at[zk, 1 - y, c, pl.ds(x, 2)]
        arrive(w, 3 + k, part)
        q = fulls[w].at[zk, 1 - y, c, 2 * x]
        go(w, 10 + k, q, q, xp)

    def mid(w):
        for k in range(3):
            mid_at(w, k)

    def far(w):
        for k in range(4):
            far_at(w, k)

    def across(w):
        for k in range(7):
            zk, yk = ((z + 3 - k) % 4, y) if k < 3 else ((z + 7 - k) % 4, 1 - y)
            arrive(w, 7 + k, fulls[w].at[zk, yk, c, 2 * (1 - x)])
            part = fulls[w].at[zk, yk, c]
            go(w, 14 + k, part, part, cp)

    def last(w):
        for k in range(7):
            zk, yk = ((z + 3 - k) % 4, y) if k < 3 else ((z + 7 - k) % 4, 1 - y)
            arrive(w, 14 + k, fulls[w].at[zk, yk, 1 - c])
        local(w).wait()

    def project():
        cut = width // 8
        rows = [fulls[0][i // 2, i % 2, 0, 0].astype(F32) for i in range(8)]
        bias[...] = jnp.zeros_like(bias)
        bias[:, 0:width] = jnp.concatenate([r[0:1, 0:cut] for r in rows], 1)
        bias[:, 2 * width :] = jnp.concatenate([r[1:2, 0:cut] for r in rows], 1)
        span = width // 2

        @pl.loop(0, 6)
        def _(j):
            cols = pl.ds(pl.multiple_of(j * span, span), span)
            part = fulls[1][:, :, :, :, :, cols].reshape(width, span)
            projected[:, cols] = (dot(tokens[...], part) + bias[:, cols]).astype(BF)

    def store(i):
        return (
            pltpu.make_async_copy(long_buf.at[i % 2], long_hbm.at[2 * i : 2 * i + 2], osem.at[i % 2]),
            pltpu.make_async_copy(short_buf.at[i % 2], short_hbm.at[2 * i : 2 * i + 2], osem.at[2 + i % 2]),
        )

    def attend_at(i):
        if i >= 2:
            for copy in store(i - 2):
                copy.wait()
        at = pl.ds(i * two, two)
        attend_kernel(
            scale, tab,
            projected.at[:, at],
            projected.at[:, pl.ds(width + i * two, two)],
            projected.at[:, pl.ds(2 * width + i * two, two)],
            mixed.at[:, at], long_buf.at[i % 2], short_buf.at[i % 2],
        )
        for copy in store(i):
            copy.start()

    for w in range(n):
        near(w)
    mid(0)
    mid(1)
    far(0)
    far(1)
    across(0)
    across(1)
    mid(2)
    last(0)
    last(1)
    far(2)
    project()
    across(2)
    attend_at(0)
    mid_at(3, 0)
    attend_at(1)
    mid_at(3, 1)
    attend_at(2)
    far_at(3, 0)
    mid_at(3, 2)
    attend_at(3)
    far_at(3, 1)
    attend_at(4)
    far_at(3, 2)
    mid_at(4, 0)
    attend_at(5)
    far_at(3, 3)
    last(2)
    mid_at(4, 1)
    far_at(4, 0)
    across(3)
    mid_at(4, 2)
    far_at(4, 1)
    far_at(4, 2)
    far_at(4, 3)
    last(3)
    across(4)
    last(4)
    for i in (pairs - 2, pairs - 1):
        for copy in store(i):
            copy.wait()
    for copy in sent:
        copy.wait_send()


def head(tab, shards, tokens):
    n = len(shards)
    views = [blocks(s) for s in shards]
    rows, width = tokens.shape
    pairs = width // (2 * HD)
    shape = jax.ShapeDtypeStruct
    anywhere = pl.BlockSpec(memory_space=pl.ANY)
    results = pl.pallas_call(
        functools.partial(head_kernel, HD ** (-0.5), pairs),
        out_shape=[shape((4, 2) + v.shape, v.dtype) for v in views]
        + [
            shape((rows, 3 * width), BF), shape((rows, width), BF),
            shape((2 * pairs, LONG, LONG), BF), shape((2 * pairs, rows - LONG, 2 * SHORT), BF),
        ],
        in_specs=[sm()] + [vm()] * (n + 1),
        out_specs=[vm()] * 2 + [anywhere] * 3 + [vm()] * 2 + [anywhere] * 2,
        scratch_shapes=[
            pltpu.SemaphoreType.DMA((n, 21)), pltpu.SemaphoreType.DMA((n, 21)),
            pltpu.SemaphoreType.DMA((n,)), pltpu.SemaphoreType.DMA((4,)),
            pltpu.VMEM((1, 3 * width), F32),
            pltpu.VMEM((2, 2, LONG, LONG), BF), pltpu.VMEM((2, 2, rows - LONG, 2 * SHORT), BF),
        ],
        compiler_params=params(collective_id=0, has_side_effects=True),
        name="head",
    )(tab, *views, tokens)
    return [f.reshape(8 * s.shape[0], s.shape[1]) for f, s in zip(results, shards)], results[n:]


def tail_kernel(scale, pairs, *refs):
    d_down, d_up, d_out, small_in, projected, g_mixed, tokens, grad_one, long_hbm, short_hbm, w_hbm = refs[:11]
    outs, grad_tokens = refs[11:16], refs[16]
    own = refs[17:]
    n = 5
    half, rx, rpy, rqy, rpz, rqz, rpx, fin, got = (own[i * n : (i + 1) * n] for i in range(9))
    ssem, rsem, lsem, d_qkv, small, heads, long_buf, short_buf, w_qkv = own[9 * n :]
    grads = [d_down, d_up, d_out, d_qkv, small]
    z, y, x, c = place_of()
    zs, yp, xp, cp = peers(z, y, x, c)
    width = tokens.shape[1]
    two = 2 * HD
    sent = []

    def fetch(i):
        return (
            pltpu.make_async_copy(long_hbm.at[2 * i : 2 * i + 2], long_buf.at[i % 2], lsem.at[i % 2]),
            pltpu.make_async_copy(short_hbm.at[2 * i : 2 * i + 2], short_buf.at[i % 2], lsem.at[2 + i % 2]),
        )

    weights = pltpu.make_async_copy(w_hbm, w_qkv, lsem.at[4])
    weights.start()
    for copy in fetch(0):
        copy.start()
    small[...] = small_in[...]
    greet(zs, yp, xp, cp)

    def go(w, i, src, dst, peer):
        copy = remote(src, dst, ssem.at[w, i], rsem.at[w, i], peer)
        copy.start()
        sent.append(copy)

    def arrive(w, i, ref):
        remote(ref, ref, ssem.at[w, i], rsem.at[w, i], cp).wait_recv()

    def add(*parts):
        total = parts[0].astype(F32)
        for part in parts[1:]:
            total = total + part.astype(F32)
        return total

    def s0(w):
        go(w, 0, grads[w].at[:, :, 1 - c], half[w], cp)

    def s1(w):
        arrive(w, 0, half[w])
        a = half[w]

        @pl.loop(0, 4)
        def _(i):
            for j in range(2):
                for k in range(3):
                    a[i, j, k] = add(grads[w][i, j, c, k], a[i, j, k]).astype(a.dtype)

        go(w, 1, a.at[:, :, 2 * (1 - x)], rx[w], xp)
        go(w, 2, a.at[:, 1 - y, 1], rpy[w], yp)

    def s2p(w):
        a = half[w]
        arrive(w, 2, rpy[w])

        @pl.loop(0, 4)
        def _(i):
            a[i, y, 1] = add(a[i, y, 1], rpy[w][i]).astype(a.dtype)

        for k in range(3):
            go(w, 3 + k, a.at[(z + k + 1) % 4, y, 1], rpz[w].at[k], zs[k])

    def s2q(w):
        a = half[w]
        arrive(w, 1, rx[w])

        @pl.loop(0, 4)
        def _(i):
            for j in range(2):
                a[i, j, 2 * x] = add(a[i, j, 2 * x], rx[w][i, j]).astype(a.dtype)

        go(w, 6, a.at[:, 1 - y, 2 * x], rqy[w], yp)

    def s3p(w):
        a = half[w]
        for k in range(3):
            arrive(w, 3 + k, rpz[w].at[k])
        a[z, y, 1] = add(a[z, y, 1], rpz[w][0], rpz[w][1], rpz[w][2]).astype(a.dtype)
        go(w, 10, a.at[z, y, 1], rpx[w], xp)

    def s3q(w):
        a = half[w]
        arrive(w, 6, rqy[w])

        @pl.loop(0, 4)
        def _(i):
            a[i, y, 2 * x] = add(a[i, y, 2 * x], rqy[w][i]).astype(a.dtype)

        for k in range(3):
            go(w, 7 + k, a.at[(z + k + 1) % 4, y, 2 * x], rqz[w].at[k], zs[k])

    def s4p(w):
        a = half[w]
        arrive(w, 10, rpx[w])
        fin[w][1] = add(a[z, y, 1], rpx[w][...]).astype(a.dtype)
        go(w, 14, fin[w].at[1], got[w].at[c, 1], cp)

    def s4q(w):
        a = half[w]
        for k in range(3):
            arrive(w, 7 + k, rqz[w].at[k])
        fin[w][0] = add(a[z, y, 2 * x], rqz[w][0], rqz[w][1], rqz[w][2]).astype(a.dtype)
        go(w, 11, fin[w].at[0], got[w].at[c, 2 * x], xp)
        go(w, 13, fin[w].at[0], got[w].at[c, 2 * x], cp)

    def s5(w):
        arrive(w, 11, got[w].at[c, 2 * (1 - x)])
        piece = got[w].at[c, 2 * (1 - x)]
        go(w, 12, piece, piece, cp)
        outs[w][c, 2 * x] = fin[w][0].astype(F32)
        outs[w][c, 1] = fin[w][1].astype(F32)
        outs[w][c, 2 * (1 - x)] = got[w][c, 2 * (1 - x)].astype(F32)

    def s6(w):
        arrive(w, 12, got[w].at[1 - c, 2 * (1 - x)])
        arrive(w, 13, got[w].at[1 - c, 2 * x])
        arrive(w, 14, got[w].at[1 - c, 1])
        for k in range(3):
            outs[w][1 - c, k] = got[w][1 - c, k].astype(F32)

    def back(i):
        if i + 1 < pairs:
            for copy in fetch(i + 1):
                copy.start()
        for copy in fetch(i):
            copy.wait()
        at = pl.ds(i * two, two)
        attend_back_kernel(
            scale,
            projected.at[:, at],
            projected.at[:, pl.ds(width + i * two, two)],
            projected.at[:, pl.ds(2 * width + i * two, two)],
            g_mixed.at[:, at],
            long_buf.at[i % 2], short_buf.at[i % 2],
            heads.at[:, :, at],
        )

    def weight(k):
        part = 256
        for j in range(width // part):
            at = slice(j * part, (j + 1) * part)
            value = dot(tokens[...], heads[k, :, at], TN).astype(BF)
            d_qkv[:, :, :, :, :, k * width + j * part : k * width + (j + 1) * part] = value.reshape(
                d_qkv.shape[:5] + (part,)
            )
        if k != 1:
            total = jnp.sum(heads[k].astype(F32), axis=0, keepdims=True)
            cut = width // 8
            for i in range(8):
                row = k // 2
                small[i // 2, i % 2, 0, 0, row : row + 1, 0:cut] = total[:, i * cut : (i + 1) * cut]

    def rows_back(i):
        step = tokens.shape[0] // 4
        at = slice(i * step, (i + 1) * step)
        total = grad_one[at, :]
        for k in range(3):
            total = total + dot(heads[k, at, :], w_qkv[:, k * width : (k + 1) * width], NT)
        grad_tokens[at, :] = total

    def run(*steps):
        for f, *which in steps:
            for w in which:
                f(w)

    run(
        (s0, 0, 1, 2), (back, 0, 1), (s1, 0), (back, 2), (s1, 1), (back, 3, 4), (s2p, 0), (back, 5),
        (s2p, 1), (weight, 0), (s2q, 0), (weight, 1, 2), (s0, 3, 4), (s3p, 0), (s3q, 0),
    )
    weights.wait()
    run(
        (rows_back, 0), (s1, 3, 2, 4), (s3p, 1), (s4q, 0), (s4p, 0), (rows_back, 1), (s2q, 1),
        (s2p, 3, 2, 4), (rows_back, 2), (s3q, 1), (s4p, 1), (s5, 0), (rows_back, 3), (s2q, 3),
        (s3p, 3, 2, 4), (s4q, 1), (s2q, 2, 4), (s3q, 3), (s5, 1), (s3q, 2, 4), (s4p, 3, 2, 4),
        (s6, 0), (s4q, 3), (s6, 1), (s4q, 2, 4), (s5, 3, 2, 4), (s6, 3, 2, 4),
    )
    for copy in sent:
        copy.wait_send()


def tail(d_down, d_up, d_out, small, projected, g_mixed, tokens, grad_one, long_probs, short_probs, w_qkv):
    rows, wide = projected.shape
    width = wide // 3
    pairs = width // (2 * HD)

    def view(shape):
        return (4, 2, 2, 3, shape[0] // 48, shape[1])

    views = [g.reshape(view(g.shape)) for g in (d_down, d_up, d_out)] + [small.reshape(view(small.shape))]
    qkv_view = view(w_qkv.shape)
    kinds = [(v.shape, v.dtype) for v in views[:3]] + [(qkv_view, BF), (views[3].shape, F32)]
    lead = ((4, 2, 3), (4, 2), (4,), (4,), (3,), (3,), (), (2,), (2, 3))
    scratch = [pltpu.VMEM(s + v[4:], t) for s in lead for v, t in kinds]
    anywhere = pl.BlockSpec(memory_space=pl.ANY)
    results = pl.pallas_call(
        functools.partial(tail_kernel, HD ** (-0.5), pairs),
        out_shape=[jax.ShapeDtypeStruct(v[2:], F32) for v, _ in kinds]
        + [jax.ShapeDtypeStruct((rows, width), F32)],
        in_specs=[vm()] * 8 + [anywhere] * 3,
        out_specs=[vm()] * 6,
        scratch_shapes=scratch
        + [
            pltpu.SemaphoreType.DMA((5, 15)), pltpu.SemaphoreType.DMA((5, 15)),
            pltpu.SemaphoreType.DMA((5,)),
            pltpu.VMEM(qkv_view, BF), pltpu.VMEM(views[3].shape, F32),
            pltpu.VMEM((3, rows, width), BF),
            pltpu.VMEM((2, 2) + long_probs.shape[1:], BF),
            pltpu.VMEM((2, 2) + short_probs.shape[1:], BF),
            pltpu.VMEM(w_qkv.shape, BF),
        ],
        compiler_params=params(collective_id=1, has_side_effects=True),
        name="tail",
    )(*views, projected, g_mixed, tokens, grad_one, long_probs, short_probs, w_qkv)
    flat = [o.reshape(-1, o.shape[-1]) for o in results[:5]]
    return flat, results[5]


def square():
    return lax.axis_size("dp") == 8 and lax.axis_size("rep") == 4


def front_layer(tab, tokens, qkv_weight, out_weight, up_weight, down_weight, norm_gains, bias_rows, ff_bias):
    width = tokens.shape[1]
    if not square():
        w_qkv, w_out, w_up, w_down = (
            lax.all_gather(w, "dp", axis=0, tiled=True)
            for w in (qkv_weight, out_weight, up_weight, down_weight)
        )
        gains = lax.all_gather(norm_gains, "dp", axis=1, tiled=True)
        biases = lax.all_gather(bias_rows, "dp", axis=1, tiled=True)
        up_bias = lax.all_gather(ff_bias, "dp", axis=0, tiled=True)
        wide = biases.astype(F32)
        bias = jnp.concatenate([wide[0], jnp.zeros((width,), F32), wide[1]])
        projected = (dot(tokens, w_qkv) + bias).astype(BF)
        mixed, *probs = attend(tab, projected)
        return (w_qkv, w_out, w_up, w_down, gains, biases, up_bias, projected, mixed, tuple(probs))

    cut = width // 8
    kept = bias_rows.shape[0] - 2
    rest = jnp.concatenate([bias_rows[2:].reshape(-1), norm_gains.reshape(-1), ff_bias])
    used = rest.shape[0]
    first = jnp.pad(bias_rows[:2], ((0, 14), (0, 128 - cut)))
    rest = jnp.pad(rest, (0, 80 * 128 - used)).reshape(80, 128)
    small = jnp.concatenate([first, rest])
    full, (projected, mixed, *probs) = head(
        tab, [small, qkv_weight, out_weight, up_weight, down_weight], tokens
    )
    rows = full[0].reshape(8, 96, 128)
    lead = rows[:, :2, :cut]
    rows = rows[:, 16:].reshape(8, -1)[:, :used]
    nb, ng = kept * cut, norm_gains.shape[0] * cut
    biases = jnp.concatenate([lead, rows[:, :nb].reshape(8, kept, cut)], 1).transpose(1, 0, 2)
    gains = rows[:, nb : nb + ng].reshape(8, -1, cut).transpose(1, 0, 2)
    return (
        full[1], full[2], full[3], full[4],
        gains.reshape(-1, width), biases.reshape(-1, width), rows[:, nb + ng :].reshape(-1),
        projected, mixed, tuple(probs),
    )


def reduce_layer(d_qkv, d_out, d_up, d_down, d_gains, d_biases, d_up_bias):
    def full(g):
        part = lax.psum_scatter(g, "rep", scatter_dimension=1, tiled=True).astype(F32)
        part = lax.psum_scatter(part, "dp", scatter_dimension=0, tiled=True)
        return lax.all_gather(part.astype(BF), "rep", axis=1, tiled=True).astype(F32)

    small = lax.psum(
        (
            lax.psum_scatter(d_gains, "dp", scatter_dimension=1, tiled=True),
            lax.psum_scatter(d_biases, "dp", scatter_dimension=1, tiled=True),
            lax.psum_scatter(d_up_bias, "dp", scatter_dimension=0, tiled=True),
        ),
        "rep",
    )
    return tuple(full(g.astype(BF)) for g in (d_qkv, d_out, d_up, d_down)) + small


def back_layer(projected, grad_mixed, probs, tokens, grad_one, w_qkv, d_out, d_up, d_down, sums, d_up_bias):
    width = tokens.shape[1]
    if not square():
        parts = attend_back(projected, grad_mixed, *probs)
        grad_heads = jnp.concatenate([parts[0], parts[1], parts[2]], 1)
        d_head = jnp.sum(grad_heads.astype(F32), axis=0)[None]
        d_qkv = dot(tokens, grad_heads, TN)
        grad_tokens = grad_one + dot(grad_heads, w_qkv, NT)
        d_biases = jnp.concatenate([d_head[:, :width], d_head[:, 2 * width :], sums[2:6]])
        return (grad_tokens,) + reduce_layer(d_qkv, d_out, d_up, d_down, sums[0:2], d_biases, d_up_bias)

    def cut(g):
        return g.reshape(g.shape[0], 8, -1).transpose(1, 0, 2).reshape(8, -1)

    rest = jnp.concatenate([cut(sums[0:6]), d_up_bias.reshape(8, -1)], 1)
    n0, n1 = 6 * (width // 8), rest.shape[1]
    small = jnp.pad(rest, ((0, 0), (1024, 5 * 1024 - n1))).reshape(8 * 48, 128)
    (down, up, out, qkv, own), grad_tokens = tail(
        d_down, d_up, d_out, small, projected, grad_mixed, tokens, grad_one, *probs, w_qkv
    )
    own_rest = own[8:].reshape(-1)
    rows = own_rest[:n0].reshape(6, -1)
    biases = jnp.concatenate([own[0:2, : width // 8], rows[2:6]])
    return (grad_tokens, qkv, out, up, down, rows[0:2], biases, own_rest[n0:n1])


def local(
    tokens,
    qkv_weight,
    out_weight,
    up_weight,
    down_weight,
    norm_gains,
    bias_rows,
    ff_bias,
    lengths,
    owners,
    cotangent,
):
    row_count = tokens.shape[0]
    device = lax.axis_index("dp") * lax.axis_size("rep") + lax.axis_index("rep")
    devices = lax.axis_size("dp") * lax.axis_size("rep")
    per = lengths.shape[0] // devices
    assert row_count == LONG + SHORT * (per - 1)
    me = device.astype(jnp.int32).reshape(1)
    tokens, cotangent, tab = prep(me, owners, lengths, tokens, cotangent, per)
    w_qkv, w_out, w_up, w_down, gains, biases, up_bias, projected, mixed_rows, probs = front_layer(
        tab, tokens, qkv_weight, out_weight, up_weight, down_weight, norm_gains, bias_rows, ff_bias
    )
    gain_rows = gains.astype(F32)
    shift_rows = biases.astype(F32)
    up_bias = up_bias.astype(F32)
    final, grad_one, grad_mixed, d_out, d_up, d_down, sums, d_up_bias = middle(
        mixed_rows, tokens, cotangent, w_out, w_up, w_down, gain_rows, shift_rows, up_bias[None]
    )
    d_up_bias = d_up_bias[0]
    output = unperm(tab, final, per)
    grad_tokens, *rest = back_layer(
        projected, grad_mixed, probs, tokens, grad_one, w_qkv,
        d_out, d_up, d_down, sums, d_up_bias,
    )
    return (output, unperm(tab, grad_tokens, per)) + tuple(rest)


def solution(mesh):
    in_specs = (
        P(("dp", "rep"), None),
        P("dp", None),
        P("dp", None),
        P("dp", None),
        P("dp", None),
        P(None, "dp"),
        P(None, "dp"),
        P("dp"),
        P(),
        P(),
        P(("dp", "rep"), None),
    )
    out_specs = (
        P(("dp", "rep"), None),
        P(("dp", "rep"), None),
        P("dp", None),
        P("dp", None),
        P("dp", None),
        P("dp", None),
        P(None, "dp"),
        P(None, "dp"),
        P("dp"),
    )
    return jax.shard_map(local, mesh=mesh, in_specs=in_specs, out_specs=out_specs, check_vma=False)
```

```python
import functools

import jax
import jax.numpy as jnp
from jax import lax
from jax.experimental import pallas as pl
from jax.experimental.pallas import tpu as pltpu
from jax.sharding import PartitionSpec as P

HEADS = 12
HD = 64
LONG = 512
SHORT = 64
norm_eps = 1e-06
masked_score = -1000000000.0
BF = jnp.bfloat16
F32 = jnp.float32
VMEM_LIMIT = 62 * 1024 * 1024

NN = (((1,), (0,)), ((), ()))
NT = (((1,), (1,)), ((), ()))
TN = (((0,), (0,)), ((), ()))


def dot(a, b, dims=NN):
    return lax.dot_general(a, b, dims, preferred_element_type=F32)


def vm():
    return pl.BlockSpec(memory_space=pltpu.VMEM)


def sm():
    return pl.BlockSpec(memory_space=pltpu.SMEM)


def params(**kw):
    return pltpu.CompilerParams(vmem_limit_bytes=VMEM_LIMIT, **kw)


def table_kernel(per, me_ref, own_ref, len_ref, tab_ref):
    total = own_ref.shape[0]
    me = me_ref[0]

    def zero(i, c):
        tab_ref[0, i] = 0
        return c

    lax.fori_loop(0, 128, zero, 0)

    def scan(p, c):
        count, start = c
        hit = own_ref[p] == me
        size = len_ref[p]
        tab_ref[0, count] = start
        tab_ref[0, 16 + count] = size
        return (count + hit.astype(jnp.int32), start + jnp.where(hit, size, 0))

    lax.fori_loop(0, total, scan, (jnp.int32(0), jnp.int32(0)), unroll=8)

    def find(j, c):
        return jnp.where(tab_ref[0, 16 + j] > SHORT, j, c)

    big = lax.fori_loop(0, per, find, jnp.int32(0))

    def place(j, slot):
        is_big = j == big
        tab_ref[0, 32 + j] = jnp.where(is_big, 0, LONG + SHORT * slot)
        tab_ref[0, 48 + j] = jnp.where(is_big, LONG // SHORT, 1)
        at = jnp.where(is_big, 0, slot + 1)
        tab_ref[0, 64 + at] = tab_ref[0, 16 + j]
        tab_ref[0, 80 + at] = tab_ref[0, j]
        return slot + jnp.where(is_big, 0, 1)

    lax.fori_loop(0, per, place, jnp.int32(0))


def slot_table(me, owners, lengths, per):
    return pl.pallas_call(
        functools.partial(table_kernel, per),
        out_shape=jax.ShapeDtypeStruct((1, 128), jnp.int32),
        in_specs=[sm(), sm(), sm()],
        out_specs=sm(),
        compiler_params=params(),
        name="table",
    )(me, owners, lengths)


def slot_source(tab_ref, block, shape, dim):
    at = lax.broadcasted_iota(jnp.int32, shape, dim)
    if block == 0:
        return jnp.where(at < tab_ref[0, 64], tab_ref[0, 80] + at, -1)
    source = jnp.full(shape, -1, jnp.int32)
    for s in range(LONG // SHORT):
        inner = at - s * SHORT
        good = (inner >= 0) & (inner < tab_ref[0, 65 + s])
        source = jnp.where(good, tab_ref[0, 81 + s] + inner, source)
    return source


def fill_selection(tab_ref, pick, back):
    for a in range(2):
        for b in range(2):
            slot, row = (b, a) if back else (a, b)
            source = slot_source(tab_ref, slot, (1, LONG) if back else (LONG, 1), 1 if back else 0)
            want = lax.broadcasted_iota(jnp.int32, (LONG, LONG), 0 if back else 1) + row * LONG
            pick[a, b] = jnp.where(source == want, 1.0, 0.0).astype(BF)


def move_rows(pick, srcs, dst):
    for a in range(2):
        total = None
        for b in range(2):
            for src in srcs:
                part = dot(pick[a, b], src[b * LONG : (b + 1) * LONG, :])
                total = part if total is None else total + part
        dst[a * LONG : (a + 1) * LONG, :] = total.astype(dst.dtype)


def permute_kernel(back, tab_ref, src_ref, out_ref, pick):
    fill_selection(tab_ref, pick, back)
    if out_ref.dtype == BF:
        return move_rows(pick, [src_ref], out_ref)
    value = src_ref[...]
    for k in range(3):
        part = value.astype(BF)
        value = value - part.astype(F32)
        for a in range(2):
            at = slice(a * LONG, (a + 1) * LONG)
            old = jnp.zeros((LONG, value.shape[1]), F32) if k == 0 else out_ref[at, :]
            for b in range(2):
                old = old + dot(pick[a, b], part[b * LONG : (b + 1) * LONG, :])
            out_ref[at, :] = old


def permute(tab, src, back):
    return pl.pallas_call(
        functools.partial(permute_kernel, back),
        out_shape=jax.ShapeDtypeStruct(src.shape, src.dtype),
        in_specs=[sm(), vm()],
        out_specs=vm(),
        scratch_shapes=[pltpu.VMEM((2, 2, LONG, LONG), BF)],
        compiler_params=params(),
        name="permute",
    )(tab, src)


def place_of():
    dp, rep = lax.axis_index("dp"), lax.axis_index("rep")
    return dp // 2, dp % 2, rep // 2, rep % 2


def peers(z, y, x, c):
    def at(z2, y2, x2, c2):
        return (z2 * 2 + y2, x2 * 2 + c2)

    return (
        [at((z + k) % 4, y, x, c) for k in (1, 2, 3)],
        at(z, 1 - y, x, c),
        at(z, y, 1 - x, c),
        at(z, y, x, 1 - c),
    )


def greet(zs, yp, xp, cp):
    barrier = pltpu.get_barrier_semaphore()
    for peer in (*zs, yp, xp, cp):
        pl.semaphore_signal(barrier, inc=1, device_id=peer, device_id_type=pl.DeviceIdType.MESH)
    pl.semaphore_wait(barrier, 6)


def remote(src, dst, ssem, rsem, peer):
    return pltpu.make_async_remote_copy(
        src_ref=src, dst_ref=dst, send_sem=ssem, recv_sem=rsem,
        device_id=peer, device_id_type=pl.DeviceIdType.MESH,
    )


def blocks(shard):
    rows, columns = shard.shape
    return shard.reshape(2, 3, rows // 6, columns)


def head_lanes(block, head):
    lane = lax.broadcasted_iota(jnp.int32, (1, block.shape[1]), 1)
    keep = jnp.where(lane >= HD, float(head), 1.0 - head)
    return block * keep.astype(BF)


def softmax_keys(scores, valid):
    scores = jnp.where(valid, scores, masked_score)
    weights = jnp.exp(scores - jnp.max(scores, axis=0, keepdims=True))
    return weights * (1.0 / jnp.sum(weights, axis=0, keepdims=True))


def short_valid(tab_ref, pair, size):
    key = lax.broadcasted_iota(jnp.int32, (size, size), 0)
    query = lax.broadcasted_iota(jnp.int32, (size, size), 1)
    low, high = tab_ref[0, 65 + 2 * pair], tab_ref[0, 66 + 2 * pair]
    bound = jnp.where(key >= SHORT, SHORT + high, low)
    return (key < bound) & (key // SHORT == query // SHORT)


def attend_kernel(scale, tab_ref, q_ref, k_ref, v_ref, out_ref, long_ref, short_ref):
    two = 2 * SHORT
    key = lax.broadcasted_iota(jnp.int32, (LONG, LONG), 0)
    valid = key < tab_ref[0, 64]
    shorts = (q_ref.shape[0] - LONG) // two
    keeps = [short_valid(tab_ref, b, two) for b in range(shorts)]
    total = None
    tails = [None] * shorts
    for h in range(2):
        scores = dot(head_lanes(k_ref[0:LONG], h), q_ref[0:LONG], NT) * scale
        probs = softmax_keys(scores, valid).astype(BF)
        long_ref[h] = probs
        part = dot(probs, head_lanes(v_ref[0:LONG], h), TN)
        total = part if total is None else total + part
        for b in range(shorts):
            rows = slice(LONG + b * two, LONG + (b + 1) * two)
            scores = dot(head_lanes(k_ref[rows], h), q_ref[rows], NT) * scale
            probs = softmax_keys(scores, keeps[b]).astype(BF)
            short_ref[h, b * two : (b + 1) * two] = probs
            part = dot(probs, head_lanes(v_ref[rows], h), TN)
            tails[b] = part if tails[b] is None else tails[b] + part
    out_ref[0:LONG] = total.astype(BF)
    for b in range(shorts):
        out_ref[LONG + b * two : LONG + (b + 1) * two] = tails[b].astype(BF)


def attend(tab, projected):
    rows, wide = projected.shape
    width = wide // 3
    pairs = width // (2 * HD)
    column = lambda off: pl.BlockSpec((rows, 2 * HD), lambda i, off=off: (0, off + i))
    return pl.pallas_call(
        functools.partial(attend_kernel, HD ** (-0.5)),
        grid=(pairs,),
        out_shape=(
            jax.ShapeDtypeStruct((rows, width), BF),
            jax.ShapeDtypeStruct((2 * pairs, LONG, LONG), BF),
            jax.ShapeDtypeStruct((2 * pairs, rows - LONG, 2 * SHORT), BF),
        ),
        in_specs=[sm(), column(0), column(pairs), column(2 * pairs)],
        out_specs=(
            column(0),
            pl.BlockSpec((2, LONG, LONG), lambda i: (i, 0, 0)),
            pl.BlockSpec((2, rows - LONG, 2 * SHORT), lambda i: (i, 0, 0)),
        ),
        compiler_params=params(),
        name="attend",
    )(tab, projected, projected, projected)


def attend_back_kernel(scale, q_ref, k_ref, v_ref, g_ref, long_ref, short_ref, out_ref):
    two = 2 * SHORT
    shorts = (q_ref.shape[0] - LONG) // two
    spans = [(slice(0, LONG), None)]
    spans += [(slice(LONG + b * two, LONG + (b + 1) * two), b) for b in range(shorts)]
    for rows, b in spans:
        sums = None
        for h in range(2):
            probs = long_ref[h] if b is None else short_ref[h, b * two : (b + 1) * two]
            grad = head_lanes(g_ref[rows], h)
            wide = probs.astype(F32)
            grad_probs = dot(v_ref[rows], grad, NT)
            mean = jnp.sum(grad_probs * wide, axis=0, keepdims=True)
            grad_scores = (wide * (grad_probs - mean)).astype(BF)
            parts = (
                dot(grad_scores, head_lanes(k_ref[rows], h), TN),
                dot(grad_scores, head_lanes(q_ref[rows], h)),
                dot(probs, grad),
            )
            sums = parts if sums is None else tuple(a + p for a, p in zip(sums, parts))
        out_ref[0, rows] = (sums[0] * scale).astype(BF)
        out_ref[1, rows] = (sums[1] * scale).astype(BF)
        out_ref[2, rows] = sums[2].astype(BF)


def attend_back(projected, grad_mixed, long_probs, short_probs):
    rows, wide = projected.shape
    width = wide // 3
    pairs = width // (2 * HD)
    column = lambda off: pl.BlockSpec((rows, 2 * HD), lambda i, off=off: (0, off + i))
    return pl.pallas_call(
        functools.partial(attend_back_kernel, HD ** (-0.5)),
        grid=(pairs,),
        out_shape=jax.ShapeDtypeStruct((3, rows, width), BF),
        in_specs=[
            column(0), column(pairs), column(2 * pairs), column(0),
            pl.BlockSpec((2, LONG, LONG), lambda i: (i, 0, 0)),
            pl.BlockSpec((2, rows - LONG, 2 * SHORT), lambda i: (i, 0, 0)),
        ],
        out_specs=pl.BlockSpec((3, rows, 2 * HD), lambda i: (0, 0, i)),
        compiler_params=params(),
        name="attend_back",
    )(projected, projected, projected, grad_mixed, long_probs, short_probs)


def gelu_pair(value):
    size = jnp.abs(value)
    bell = jnp.exp(-0.5 * value * value)
    t = 1.0 / (1.0 + 0.23164189 * size)
    tail = t * (0.127414796 + t * (-0.142248368 + t * (0.7107068705 + t * (-0.7265760135 + t * 0.5307027145))))
    tail = tail * bell
    whole = jnp.where(value >= 0.0, 1.0 - tail, tail)
    return (value * whole, whole + value * bell * 0.3989422804)


def middle_kernel(
    step, span, mixed, tokens, cot, w_out, w_up, w_down, gains, biases, ff_bias,
    out, acc, g_mixed, d_out, d_up, d_down, sums, d_ffb, unit, low, low2, hidden, slope, inv
):
    rows = mixed.shape[0]
    parts = w_up.shape[1] // span
    sums[...] = jnp.zeros_like(sums)

    def rows_at(i):
        return pl.ds(pl.multiple_of(i * step, step), step)

    def columns_at(j):
        return pl.ds(pl.multiple_of(j * span, span), span)

    def mean(a):
        return jnp.mean(a, axis=-1, keepdims=True)

    def tally(i, a):
        sums[i : i + 1, :] += jnp.sum(a, axis=0, keepdims=True)

    def norm(r):
        center = r - mean(r)
        scale = lax.rsqrt(mean(center * center) + norm_eps)
        return center * scale, scale

    def back(s, u, scale):
        return scale * (s - mean(s) - u * mean(s * u))

    @pl.loop(0, rows // step)
    def _(i):
        at = rows_at(i)
        branch = dot(mixed[at, :], w_out[...]) + biases[2:3, :]
        u, scale = norm(tokens[at, :].astype(F32) + branch)
        unit[at, :] = u
        inv[at, :] = scale
        low[at, :] = (u * gains[0:1, :] + biases[4:5, :]).astype(BF)
        acc[at, :] = jnp.zeros((step, acc.shape[1]), F32)

    @pl.loop(0, parts)
    def _(j):
        cols = columns_at(j)
        for i in range(rows // step):
            at = slice(i * step, (i + 1) * step)
            inner = dot(low[at, :], w_up[:, cols]) + ff_bias[:, cols]
            act, der = gelu_pair(inner)
            act = act.astype(BF)
            hidden[at, cols] = act
            slope[at, cols] = der.astype(BF)
            acc[at, :] += dot(act, w_down[cols, :])

    @pl.loop(0, rows // step)
    def _(i):
        at = rows_at(i)
        first = unit[at, :] * gains[0:1, :] + biases[4:5, :]
        u, scale = norm(first + acc[at, :] + biases[3:4, :])
        out[at, :] = (u * gains[1:2, :] + biases[5:6, :]).astype(BF)
        g = cot[at, :].astype(F32)
        tally(1, g * u)
        tally(5, g)
        g = back(g * gains[1:2, :], u, scale)
        acc[at, :] = g
        g = g.astype(BF)
        low2[at, :] = g
        tally(3, g.astype(F32))

    @pl.loop(0, parts)
    def _(j):
        cols = columns_at(j)
        total = None
        for i in range(rows // step):
            at = slice(i * step, (i + 1) * step)
            g = dot(low2[at, :], w_down[cols, :], NT) * slope[at, cols].astype(F32)
            g = g.astype(BF)
            slope[at, cols] = g
            part = jnp.sum(g.astype(F32), axis=0, keepdims=True)
            total = part if total is None else total + part
            acc[at, :] += dot(g, w_up[:, cols], NT)
        d_ffb[:, cols] = total
        d_down[cols, :] = dot(hidden[:, cols], low2[...], TN).astype(BF)
        d_up[:, cols] = dot(low[...], slope[:, cols], TN).astype(BF)

    @pl.loop(0, rows // step)
    def _(i):
        at = rows_at(i)
        g, u = acc[at, :], unit[at, :]
        tally(0, g * u)
        tally(4, g)
        g = back(g * gains[0:1, :], u, inv[at, :])
        acc[at, :] = g
        g = g.astype(BF)
        low2[at, :] = g
        tally(2, g.astype(F32))
        g_mixed[at, :] = dot(g, w_out[...], NT).astype(BF)

    d_out[...] = dot(mixed[...], low2[...], TN).astype(BF)


def middle(mixed, tokens, cot, w_out, w_up, w_down, gains, biases, ff_bias):
    rows, width = mixed.shape
    ff = w_up.shape[1]
    shape = jax.ShapeDtypeStruct
    return pl.pallas_call(
        functools.partial(middle_kernel, 256, 512),
        out_shape=(
            shape((rows, width), BF), shape((rows, width), F32), shape((rows, width), BF),
            shape((width, width), BF), shape((width, ff), BF), shape((ff, width), BF),
            shape((8, width), F32), shape((1, ff), F32),
        ),
        in_specs=[vm()] * 9,
        out_specs=(vm(),) * 8,
        scratch_shapes=[
            pltpu.VMEM((rows, width), F32), pltpu.VMEM((rows, width), BF),
            pltpu.VMEM((rows, width), BF), pltpu.VMEM((rows, ff), BF),
            pltpu.VMEM((rows, ff), BF), pltpu.VMEM((rows, 1), F32),
        ],
        compiler_params=params(),
        name="middle",
    )(mixed, tokens, cot, w_out, w_up, w_down, gains, biases, ff_bias)


def head_kernel(scale, pairs, tab, *refs):
    n = 5
    shards, raw, raw_cot = refs[:n], refs[n], refs[n + 1]
    fulls = refs[n + 2 : 2 * n + 2]
    projected, mixed, long_hbm, short_hbm, tokens, cot = refs[2 * n + 2 : 2 * n + 8]
    ssem, rsem, lsem, osem, bias, long_buf, short_buf = refs[2 * n + 8 :]
    z, y, x, c = place_of()
    zs, yp, xp, cp = peers(z, y, x, c)
    greet(zs, yp, xp, cp)
    width = tokens.shape[1]
    two = 2 * HD
    sent = []

    def go(w, i, src, dst, peer):
        copy = remote(src, dst, ssem.at[w, i], rsem.at[w, i], peer)
        copy.start()
        sent.append(copy)

    def arrive(w, i, ref):
        remote(ref, ref, ssem.at[w, i], rsem.at[w, i], cp).wait_recv()

    def local(w):
        return pltpu.make_async_copy(shards[w], fulls[w].at[z, y], lsem.at[w])

    def near(w):
        local(w).start()
        src = shards[w].at[c, pl.ds(x, 2)]
        dst = fulls[w].at[z, y, c, pl.ds(x, 2)]
        for k in range(3):
            go(w, k, src, dst, zs[k])
        go(w, 3, src, dst, yp)

    def mid_at(w, k):
        zk = (z + 3 - k) % 4
        part = fulls[w].at[zk, y, c, pl.ds(x, 2)]
        arrive(w, k, part)
        go(w, 4 + k, part, part, yp)
        q = fulls[w].at[zk, y, c, 2 * x]
        go(w, 7 + k, q, q, xp)

    def far_at(w, k):
        zk = (z + 4 - k) % 4
        part = fulls[w].at[zk, 1 - y, c, pl.ds(x, 2)]
        arrive(w, 3 + k, part)
        q = fulls[w].at[zk, 1 - y, c, 2 * x]
        go(w, 10 + k, q, q, xp)

    def mid(w):
        for k in range(3):
            mid_at(w, k)

    def far(w):
        for k in range(4):
            far_at(w, k)

    def across(w):
        for k in range(7):
            zk, yk = ((z + 3 - k) % 4, y) if k < 3 else ((z + 7 - k) % 4, 1 - y)
            arrive(w, 7 + k, fulls[w].at[zk, yk, c, 2 * (1 - x)])
            part = fulls[w].at[zk, yk, c]
            go(w, 14 + k, part, part, cp)

    def last(w):
        for k in range(7):
            zk, yk = ((z + 3 - k) % 4, y) if k < 3 else ((z + 7 - k) % 4, 1 - y)
            arrive(w, 14 + k, fulls[w].at[zk, yk, 1 - c])
        local(w).wait()

    def project():
        cut = width // 8
        rows = [fulls[0][i // 2, i % 2, 0, 0].astype(F32) for i in range(8)]
        bias[...] = jnp.zeros_like(bias)
        bias[:, 0:width] = jnp.concatenate([r[0:1, 0:cut] for r in rows], 1)
        bias[:, 2 * width :] = jnp.concatenate([r[1:2, 0:cut] for r in rows], 1)
        span = width // 2

        @pl.loop(0, 6)
        def _(j):
            cols = pl.ds(pl.multiple_of(j * span, span), span)
            part = fulls[1][:, :, :, :, :, cols].reshape(width, span)
            projected[:, cols] = (dot(tokens[...], part) + bias[:, cols]).astype(BF)

    def store(i):
        return (
            pltpu.make_async_copy(long_buf.at[i % 2], long_hbm.at[2 * i : 2 * i + 2], osem.at[i % 2]),
            pltpu.make_async_copy(short_buf.at[i % 2], short_hbm.at[2 * i : 2 * i + 2], osem.at[2 + i % 2]),
        )

    def attend_at(i):
        if i >= 2:
            for copy in store(i - 2):
                copy.wait()
        at = pl.ds(i * two, two)
        attend_kernel(
            scale, tab,
            projected.at[:, at],
            projected.at[:, pl.ds(width + i * two, two)],
            projected.at[:, pl.ds(2 * width + i * two, two)],
            mixed.at[:, at], long_buf.at[i % 2], short_buf.at[i % 2],
        )
        for copy in store(i):
            copy.start()

    for w in range(n):
        near(w)
    fill_selection(tab, long_buf, False)
    move_rows(long_buf, [raw], tokens)
    move_rows(long_buf, [raw_cot], cot)
    mid(0)
    mid(1)
    far(0)
    far(1)
    across(0)
    across(1)
    mid(2)
    last(0)
    last(1)
    far(2)
    project()
    across(2)
    attend_at(0)
    mid_at(3, 0)
    attend_at(1)
    mid_at(3, 1)
    attend_at(2)
    far_at(3, 0)
    mid_at(3, 2)
    attend_at(3)
    far_at(3, 1)
    attend_at(4)
    far_at(3, 2)
    mid_at(4, 0)
    attend_at(5)
    far_at(3, 3)
    last(2)
    mid_at(4, 1)
    far_at(4, 0)
    across(3)
    mid_at(4, 2)
    far_at(4, 1)
    far_at(4, 2)
    far_at(4, 3)
    last(3)
    across(4)
    last(4)
    for i in (pairs - 2, pairs - 1):
        for copy in store(i):
            copy.wait()
    for copy in sent:
        copy.wait_send()


def head(tab, shards, tokens, cotangent):
    n = len(shards)
    views = [blocks(s) for s in shards]
    rows, width = tokens.shape
    pairs = width // (2 * HD)
    shape = jax.ShapeDtypeStruct
    anywhere = pl.BlockSpec(memory_space=pl.ANY)
    results = pl.pallas_call(
        functools.partial(head_kernel, HD ** (-0.5), pairs),
        out_shape=[shape((4, 2) + v.shape, v.dtype) for v in views]
        + [
            shape((rows, 3 * width), BF), shape((rows, width), BF),
            shape((2 * pairs, LONG, LONG), BF), shape((2 * pairs, rows - LONG, 2 * SHORT), BF),
            shape((rows, width), BF), shape((rows, width), BF),
        ],
        in_specs=[sm()] + [vm()] * (n + 2),
        out_specs=[vm()] * 2 + [anywhere] * 3 + [vm()] * 2 + [anywhere] * 2 + [vm()] * 2,
        scratch_shapes=[
            pltpu.SemaphoreType.DMA((n, 21)), pltpu.SemaphoreType.DMA((n, 21)),
            pltpu.SemaphoreType.DMA((n,)), pltpu.SemaphoreType.DMA((4,)),
            pltpu.VMEM((1, 3 * width), F32),
            pltpu.VMEM((2, 2, LONG, LONG), BF), pltpu.VMEM((2, 2, rows - LONG, 2 * SHORT), BF),
        ],
        compiler_params=params(collective_id=0, has_side_effects=True),
        name="head",
    )(tab, *views, tokens, cotangent)
    return [f.reshape(8 * s.shape[0], s.shape[1]) for f, s in zip(results, shards)], results[n:]


def tail_kernel(scale, pairs, tab, *refs):
    d_down, d_up, d_out, small_in, projected, g_mixed, tokens, grad_one, long_hbm, short_hbm, w_hbm = refs[:11]
    outs, grad_tokens = refs[11:16], refs[16]
    own = refs[17:]
    n = 5
    half, rx, rpy, rqy, rpz, rqz, rpx, fin, got = (own[i * n : (i + 1) * n] for i in range(9))
    ssem, rsem, lsem, d_qkv, small, heads, long_buf, short_buf, w_qkv = own[9 * n :]
    grads = [d_down, d_up, d_out, d_qkv, small]
    z, y, x, c = place_of()
    zs, yp, xp, cp = peers(z, y, x, c)
    width = tokens.shape[1]
    two = 2 * HD
    sent = []

    def fetch(i):
        return (
            pltpu.make_async_copy(long_hbm.at[2 * i : 2 * i + 2], long_buf.at[i % 2], lsem.at[i % 2]),
            pltpu.make_async_copy(short_hbm.at[2 * i : 2 * i + 2], short_buf.at[i % 2], lsem.at[2 + i % 2]),
        )

    weights = pltpu.make_async_copy(w_hbm, w_qkv, lsem.at[4])
    weights.start()
    for copy in fetch(0):
        copy.start()
    small[...] = small_in[...]
    greet(zs, yp, xp, cp)

    def go(w, i, src, dst, peer):
        copy = remote(src, dst, ssem.at[w, i], rsem.at[w, i], peer)
        copy.start()
        sent.append(copy)

    def arrive(w, i, ref):
        remote(ref, ref, ssem.at[w, i], rsem.at[w, i], cp).wait_recv()

    def add(*parts):
        total = parts[0].astype(F32)
        for part in parts[1:]:
            total = total + part.astype(F32)
        return total

    def s0(w):
        go(w, 0, grads[w].at[:, :, 1 - c], half[w], cp)

    def s1(w):
        arrive(w, 0, half[w])
        a = half[w]

        @pl.loop(0, 4)
        def _(i):
            for j in range(2):
                for k in range(3):
                    a[i, j, k] = add(grads[w][i, j, c, k], a[i, j, k]).astype(a.dtype)

        go(w, 1, a.at[:, :, 2 * (1 - x)], rx[w], xp)
        go(w, 2, a.at[:, 1 - y, 1], rpy[w], yp)

    def s2p(w):
        a = half[w]
        arrive(w, 2, rpy[w])

        @pl.loop(0, 4)
        def _(i):
            a[i, y, 1] = add(a[i, y, 1], rpy[w][i]).astype(a.dtype)

        for k in range(3):
            go(w, 3 + k, a.at[(z + k + 1) % 4, y, 1], rpz[w].at[k], zs[k])

    def s2q(w):
        a = half[w]
        arrive(w, 1, rx[w])

        @pl.loop(0, 4)
        def _(i):
            for j in range(2):
                a[i, j, 2 * x] = add(a[i, j, 2 * x], rx[w][i, j]).astype(a.dtype)

        go(w, 6, a.at[:, 1 - y, 2 * x], rqy[w], yp)

    def s3p(w):
        a = half[w]
        for k in range(3):
            arrive(w, 3 + k, rpz[w].at[k])
        a[z, y, 1] = add(a[z, y, 1], rpz[w][0], rpz[w][1], rpz[w][2]).astype(a.dtype)
        go(w, 10, a.at[z, y, 1], rpx[w], xp)

    def s3q(w):
        a = half[w]
        arrive(w, 6, rqy[w])

        @pl.loop(0, 4)
        def _(i):
            a[i, y, 2 * x] = add(a[i, y, 2 * x], rqy[w][i]).astype(a.dtype)

        for k in range(3):
            go(w, 7 + k, a.at[(z + k + 1) % 4, y, 2 * x], rqz[w].at[k], zs[k])

    def s4p(w):
        a = half[w]
        arrive(w, 10, rpx[w])
        fin[w][1] = add(a[z, y, 1], rpx[w][...]).astype(a.dtype)
        go(w, 14, fin[w].at[1], got[w].at[c, 1], cp)

    def s4q(w):
        a = half[w]
        for k in range(3):
            arrive(w, 7 + k, rqz[w].at[k])
        fin[w][0] = add(a[z, y, 2 * x], rqz[w][0], rqz[w][1], rqz[w][2]).astype(a.dtype)
        go(w, 11, fin[w].at[0], got[w].at[c, 2 * x], xp)
        go(w, 13, fin[w].at[0], got[w].at[c, 2 * x], cp)

    def s5(w):
        arrive(w, 11, got[w].at[c, 2 * (1 - x)])
        piece = got[w].at[c, 2 * (1 - x)]
        go(w, 12, piece, piece, cp)
        outs[w][c, 2 * x] = fin[w][0].astype(F32)
        outs[w][c, 1] = fin[w][1].astype(F32)
        outs[w][c, 2 * (1 - x)] = got[w][c, 2 * (1 - x)].astype(F32)

    def s6(w):
        arrive(w, 12, got[w].at[1 - c, 2 * (1 - x)])
        arrive(w, 13, got[w].at[1 - c, 2 * x])
        arrive(w, 14, got[w].at[1 - c, 1])
        for k in range(3):
            outs[w][1 - c, k] = got[w][1 - c, k].astype(F32)

    def back(i):
        if i + 1 < pairs:
            for copy in fetch(i + 1):
                copy.start()
        for copy in fetch(i):
            copy.wait()
        at = pl.ds(i * two, two)
        attend_back_kernel(
            scale,
            projected.at[:, at],
            projected.at[:, pl.ds(width + i * two, two)],
            projected.at[:, pl.ds(2 * width + i * two, two)],
            g_mixed.at[:, at],
            long_buf.at[i % 2], short_buf.at[i % 2],
            heads.at[:, :, at],
        )

    def weight(k):
        part = 256
        for j in range(width // part):
            at = slice(j * part, (j + 1) * part)
            value = dot(tokens[...], heads[k, :, at], TN).astype(BF)
            d_qkv[:, :, :, :, :, k * width + j * part : k * width + (j + 1) * part] = value.reshape(
                d_qkv.shape[:5] + (part,)
            )
        if k != 1:
            total = jnp.sum(heads[k].astype(F32), axis=0, keepdims=True)
            cut = width // 8
            for i in range(8):
                row = k // 2
                small[i // 2, i % 2, 0, 0, row : row + 1, 0:cut] = total[:, i * cut : (i + 1) * cut]

    def rows_back(i):
        step = tokens.shape[0] // 4
        at = slice(i * step, (i + 1) * step)
        total = grad_one[at, :]
        for k in range(3):
            total = total + dot(heads[k, at, :], w_qkv[:, k * width : (k + 1) * width], NT)
        for k in range(3):
            part = total.astype(BF)
            total = total - part.astype(F32)
            heads[k, at, :] = part

    def select(_):
        fill_selection(tab, long_buf, True)

    def token_rows(_):
        move_rows(long_buf, [heads.at[0], heads.at[1], heads.at[2]], grad_tokens)

    def run(*steps):
        for f, *which in steps:
            for w in which:
                f(w)

    run(
        (s0, 0, 1, 2), (back, 0, 1), (s1, 0), (back, 2), (s1, 1), (back, 3, 4), (s2p, 0), (back, 5),
        (s2p, 1), (weight, 0), (s2q, 0), (weight, 1, 2), (s0, 3, 4), (s3p, 0), (s3q, 0), (select, 0),
    )
    weights.wait()
    run(
        (rows_back, 0), (s1, 3, 2, 4), (s3p, 1), (s4q, 0), (s4p, 0), (rows_back, 1), (s2q, 1),
        (s2p, 3, 2, 4), (rows_back, 2), (s3q, 1), (s4p, 1), (s5, 0), (rows_back, 3), (token_rows, 0), (s2q, 3),
        (s3p, 3, 2, 4), (s4q, 1), (s2q, 2, 4), (s3q, 3), (s5, 1), (s3q, 2, 4), (s4p, 3, 2, 4),
        (s6, 0), (s4q, 3), (s6, 1), (s4q, 2, 4), (s5, 3, 2, 4), (s6, 3, 2, 4),
    )
    for copy in sent:
        copy.wait_send()


def tail(tab, d_down, d_up, d_out, small, projected, g_mixed, tokens, grad_one, long_probs, short_probs, w_qkv):
    rows, wide = projected.shape
    width = wide // 3
    pairs = width // (2 * HD)

    def view(shape):
        return (4, 2, 2, 3, shape[0] // 48, shape[1])

    views = [g.reshape(view(g.shape)) for g in (d_down, d_up, d_out)] + [small.reshape(view(small.shape))]
    qkv_view = view(w_qkv.shape)
    kinds = [(v.shape, v.dtype) for v in views[:3]] + [(qkv_view, BF), (views[3].shape, F32)]
    lead = ((4, 2, 3), (4, 2), (4,), (4,), (3,), (3,), (), (2,), (2, 3))
    scratch = [pltpu.VMEM(s + v[4:], t) for s in lead for v, t in kinds]
    anywhere = pl.BlockSpec(memory_space=pl.ANY)
    results = pl.pallas_call(
        functools.partial(tail_kernel, HD ** (-0.5), pairs),
        out_shape=[jax.ShapeDtypeStruct(v[2:], F32) for v, _ in kinds]
        + [jax.ShapeDtypeStruct((rows, width), F32)],
        in_specs=[sm()] + [vm()] * 8 + [anywhere] * 3,
        out_specs=[vm()] * 6,
        scratch_shapes=scratch
        + [
            pltpu.SemaphoreType.DMA((5, 15)), pltpu.SemaphoreType.DMA((5, 15)),
            pltpu.SemaphoreType.DMA((5,)),
            pltpu.VMEM(qkv_view, BF), pltpu.VMEM(views[3].shape, F32),
            pltpu.VMEM((3, rows, width), BF),
            pltpu.VMEM((2, 2) + long_probs.shape[1:], BF),
            pltpu.VMEM((2, 2) + short_probs.shape[1:], BF),
            pltpu.VMEM(w_qkv.shape, BF),
        ],
        compiler_params=params(collective_id=1, has_side_effects=True),
        name="tail",
    )(tab, *views, projected, g_mixed, tokens, grad_one, long_probs, short_probs, w_qkv)
    flat = [o.reshape(-1, o.shape[-1]) for o in results[:5]]
    return flat, results[5]


def square():
    return lax.axis_size("dp") == 8 and lax.axis_size("rep") == 4


def front_layer(tab, tokens, cotangent, qkv_weight, out_weight, up_weight, down_weight, norm_gains, bias_rows, ff_bias):
    width = tokens.shape[1]
    if not square():
        tokens, cotangent = permute(tab, tokens, False), permute(tab, cotangent, False)
        w_qkv, w_out, w_up, w_down = (
            lax.all_gather(w, "dp", axis=0, tiled=True)
            for w in (qkv_weight, out_weight, up_weight, down_weight)
        )
        gains = lax.all_gather(norm_gains, "dp", axis=1, tiled=True)
        biases = lax.all_gather(bias_rows, "dp", axis=1, tiled=True)
        up_bias = lax.all_gather(ff_bias, "dp", axis=0, tiled=True)
        wide = biases.astype(F32)
        bias = jnp.concatenate([wide[0], jnp.zeros((width,), F32), wide[1]])
        projected = (dot(tokens, w_qkv) + bias).astype(BF)
        mixed, *probs = attend(tab, projected)
        return (
            w_qkv, w_out, w_up, w_down, gains, biases, up_bias,
            tokens, cotangent, projected, mixed, tuple(probs),
        )

    cut = width // 8
    kept = bias_rows.shape[0] - 2
    rest = jnp.concatenate([bias_rows[2:].reshape(-1), norm_gains.reshape(-1), ff_bias])
    used = rest.shape[0]
    first = jnp.pad(bias_rows[:2], ((0, 14), (0, 128 - cut)))
    rest = jnp.pad(rest, (0, 80 * 128 - used)).reshape(80, 128)
    small = jnp.concatenate([first, rest])
    full, (projected, mixed, *probs, tokens, cotangent) = head(
        tab, [small, qkv_weight, out_weight, up_weight, down_weight], tokens, cotangent
    )
    rows = full[0].reshape(8, 96, 128)
    lead = rows[:, :2, :cut]
    rows = rows[:, 16:].reshape(8, -1)[:, :used]
    nb, ng = kept * cut, norm_gains.shape[0] * cut
    biases = jnp.concatenate([lead, rows[:, :nb].reshape(8, kept, cut)], 1).transpose(1, 0, 2)
    gains = rows[:, nb : nb + ng].reshape(8, -1, cut).transpose(1, 0, 2)
    return (
        full[1], full[2], full[3], full[4],
        gains.reshape(-1, width), biases.reshape(-1, width), rows[:, nb + ng :].reshape(-1),
        tokens, cotangent, projected, mixed, tuple(probs),
    )


def reduce_layer(d_qkv, d_out, d_up, d_down, d_gains, d_biases, d_up_bias):
    def full(g):
        part = lax.psum_scatter(g, "rep", scatter_dimension=1, tiled=True).astype(F32)
        part = lax.psum_scatter(part, "dp", scatter_dimension=0, tiled=True)
        return lax.all_gather(part.astype(BF), "rep", axis=1, tiled=True).astype(F32)

    small = lax.psum(
        (
            lax.psum_scatter(d_gains, "dp", scatter_dimension=1, tiled=True),
            lax.psum_scatter(d_biases, "dp", scatter_dimension=1, tiled=True),
            lax.psum_scatter(d_up_bias, "dp", scatter_dimension=0, tiled=True),
        ),
        "rep",
    )
    return tuple(full(g.astype(BF)) for g in (d_qkv, d_out, d_up, d_down)) + small


def back_layer(tab, final, projected, grad_mixed, probs, tokens, grad_one, w_qkv, d_out, d_up, d_down, sums, d_up_bias):
    width = tokens.shape[1]
    if not square():
        parts = attend_back(projected, grad_mixed, *probs)
        grad_heads = jnp.concatenate([parts[0], parts[1], parts[2]], 1)
        d_head = jnp.sum(grad_heads.astype(F32), axis=0)[None]
        d_qkv = dot(tokens, grad_heads, TN)
        grad_tokens = grad_one + dot(grad_heads, w_qkv, NT)
        d_biases = jnp.concatenate([d_head[:, :width], d_head[:, 2 * width :], sums[2:6]])
        moved = (permute(tab, final, True), permute(tab, grad_tokens, True))
        return moved + reduce_layer(d_qkv, d_out, d_up, d_down, sums[0:2], d_biases, d_up_bias)

    def cut(g):
        return g.reshape(g.shape[0], 8, -1).transpose(1, 0, 2).reshape(8, -1)

    rest = jnp.concatenate([cut(sums[0:6]), d_up_bias.reshape(8, -1)], 1)
    n0, n1 = 6 * (width // 8), rest.shape[1]
    small = jnp.pad(rest, ((0, 0), (1024, 5 * 1024 - n1))).reshape(8 * 48, 128)
    (down, up, out, qkv, own), grad_tokens = tail(
        tab, d_down, d_up, d_out, small, projected, grad_mixed, tokens, grad_one, *probs, w_qkv
    )
    own_rest = own[8:].reshape(-1)
    rows = own_rest[:n0].reshape(6, -1)
    biases = jnp.concatenate([own[0:2, : width // 8], rows[2:6]])
    return (permute(tab, final, True), grad_tokens, qkv, out, up, down, rows[0:2], biases, own_rest[n0:n1])


def local(
    tokens,
    qkv_weight,
    out_weight,
    up_weight,
    down_weight,
    norm_gains,
    bias_rows,
    ff_bias,
    lengths,
    owners,
    cotangent,
):
    row_count = tokens.shape[0]
    device = lax.axis_index("dp") * lax.axis_size("rep") + lax.axis_index("rep")
    devices = lax.axis_size("dp") * lax.axis_size("rep")
    per = lengths.shape[0] // devices
    assert row_count == LONG + SHORT * (per - 1) == 2 * LONG
    me = device.astype(jnp.int32).reshape(1)
    tab = slot_table(me, owners, lengths, per)
    w_qkv, w_out, w_up, w_down, gains, biases, up_bias, tokens, cotangent, projected, mixed_rows, probs = front_layer(
        tab, tokens, cotangent, qkv_weight, out_weight, up_weight, down_weight, norm_gains, bias_rows, ff_bias
    )
    gain_rows = gains.astype(F32)
    shift_rows = biases.astype(F32)
    up_bias = up_bias.astype(F32)
    final, grad_one, grad_mixed, d_out, d_up, d_down, sums, d_up_bias = middle(
        mixed_rows, tokens, cotangent, w_out, w_up, w_down, gain_rows, shift_rows, up_bias[None]
    )
    d_up_bias = d_up_bias[0]
    return back_layer(
        tab, final, projected, grad_mixed, probs, tokens, grad_one, w_qkv,
        d_out, d_up, d_down, sums, d_up_bias,
    )


def solution(mesh):
    in_specs = (
        P(("dp", "rep"), None),
        P("dp", None),
        P("dp", None),
        P("dp", None),
        P("dp", None),
        P(None, "dp"),
        P(None, "dp"),
        P("dp"),
        P(),
        P(),
        P(("dp", "rep"), None),
    )
    out_specs = (
        P(("dp", "rep"), None),
        P(("dp", "rep"), None),
        P("dp", None),
        P("dp", None),
        P("dp", None),
        P("dp", None),
        P(None, "dp"),
        P(None, "dp"),
        P("dp"),
    )
    return jax.shard_map(local, mesh=mesh, in_specs=in_specs, out_specs=out_specs, check_vma=False)
```

```python
import functools

import jax
import jax.numpy as jnp
from jax import lax
from jax.experimental import pallas as pl
from jax.experimental.pallas import tpu as pltpu
from jax.sharding import PartitionSpec as P

HEADS = 12
HD = 64
LONG = 512
SHORT = 64
norm_eps = 1e-06
masked_score = -1000000000.0
BF = jnp.bfloat16
F32 = jnp.float32
VMEM_LIMIT = 62 * 1024 * 1024

NN = (((1,), (0,)), ((), ()))
NT = (((1,), (1,)), ((), ()))
TN = (((0,), (0,)), ((), ()))


def dot(a, b, dims=NN):
    return lax.dot_general(a, b, dims, preferred_element_type=F32)


def vm():
    return pl.BlockSpec(memory_space=pltpu.VMEM)


def sm():
    return pl.BlockSpec(memory_space=pltpu.SMEM)


def params(**kw):
    return pltpu.CompilerParams(vmem_limit_bytes=VMEM_LIMIT, **kw)


def table_kernel(per, me_ref, own_ref, len_ref, tab_ref):
    total = own_ref.shape[0]
    me = me_ref[0]

    def zero(i, c):
        tab_ref[0, i] = 0
        return c

    lax.fori_loop(0, 128, zero, 0)

    def scan(p, c):
        count, start = c
        hit = own_ref[p] == me
        size = len_ref[p]
        tab_ref[0, count] = start
        tab_ref[0, 16 + count] = size
        return (count + hit.astype(jnp.int32), start + jnp.where(hit, size, 0))

    lax.fori_loop(0, total, scan, (jnp.int32(0), jnp.int32(0)), unroll=8)

    def find(j, c):
        return jnp.where(tab_ref[0, 16 + j] > SHORT, j, c)

    big = lax.fori_loop(0, per, find, jnp.int32(0))

    def place(j, slot):
        is_big = j == big
        tab_ref[0, 32 + j] = jnp.where(is_big, 0, LONG + SHORT * slot)
        tab_ref[0, 48 + j] = jnp.where(is_big, LONG // SHORT, 1)
        at = jnp.where(is_big, 0, slot + 1)
        tab_ref[0, 64 + at] = tab_ref[0, 16 + j]
        tab_ref[0, 80 + at] = tab_ref[0, j]
        return slot + jnp.where(is_big, 0, 1)

    lax.fori_loop(0, per, place, jnp.int32(0))


def slot_table(me, owners, lengths, per):
    return pl.pallas_call(
        functools.partial(table_kernel, per),
        out_shape=jax.ShapeDtypeStruct((1, 128), jnp.int32),
        in_specs=[sm(), sm(), sm()],
        out_specs=sm(),
        compiler_params=params(),
        name="table",
    )(me, owners, lengths)


def slot_source(tab_ref, block, shape, dim):
    at = lax.broadcasted_iota(jnp.int32, shape, dim)
    if block == 0:
        return jnp.where(at < tab_ref[0, 64], tab_ref[0, 80] + at, -1)
    source = jnp.full(shape, -1, jnp.int32)
    for s in range(LONG // SHORT):
        inner = at - s * SHORT
        good = (inner >= 0) & (inner < tab_ref[0, 65 + s])
        source = jnp.where(good, tab_ref[0, 81 + s] + inner, source)
    return source


def fill_selection(tab_ref, pick, back):
    for a in range(2):
        for b in range(2):
            slot, row = (b, a) if back else (a, b)
            source = slot_source(tab_ref, slot, (1, LONG) if back else (LONG, 1), 1 if back else 0)
            want = lax.broadcasted_iota(jnp.int32, (LONG, LONG), 0 if back else 1) + row * LONG
            pick[a, b] = jnp.where(source == want, 1.0, 0.0).astype(BF)


def move_rows(pick, srcs, dst):
    for a in range(2):
        total = None
        for b in range(2):
            for src in srcs:
                part = dot(pick[a, b], src[b * LONG : (b + 1) * LONG, :])
                total = part if total is None else total + part
        dst[a * LONG : (a + 1) * LONG, :] = total.astype(dst.dtype)


def permute_kernel(back, tab_ref, src_ref, out_ref, pick):
    fill_selection(tab_ref, pick, back)
    if out_ref.dtype == BF:
        return move_rows(pick, [src_ref], out_ref)
    value = src_ref[...]
    for k in range(3):
        part = value.astype(BF)
        value = value - part.astype(F32)
        for a in range(2):
            at = slice(a * LONG, (a + 1) * LONG)
            old = jnp.zeros((LONG, value.shape[1]), F32) if k == 0 else out_ref[at, :]
            for b in range(2):
                old = old + dot(pick[a, b], part[b * LONG : (b + 1) * LONG, :])
            out_ref[at, :] = old


def permute(tab, src, back):
    return pl.pallas_call(
        functools.partial(permute_kernel, back),
        out_shape=jax.ShapeDtypeStruct(src.shape, src.dtype),
        in_specs=[sm(), vm()],
        out_specs=vm(),
        scratch_shapes=[pltpu.VMEM((2, 2, LONG, LONG), BF)],
        compiler_params=params(),
        name="permute",
    )(tab, src)


def place_of():
    dp, rep = lax.axis_index("dp"), lax.axis_index("rep")
    return dp // 2, dp % 2, rep // 2, rep % 2


def peers(z, y, x, c):
    def at(z2, y2, x2, c2):
        return (z2 * 2 + y2, x2 * 2 + c2)

    return (
        [at((z + k) % 4, y, x, c) for k in (1, 2, 3)],
        at(z, 1 - y, x, c),
        at(z, y, 1 - x, c),
        at(z, y, x, 1 - c),
    )


def greet(zs, yp, xp, cp):
    barrier = pltpu.get_barrier_semaphore()
    for peer in (*zs, yp, xp, cp):
        pl.semaphore_signal(barrier, inc=1, device_id=peer, device_id_type=pl.DeviceIdType.MESH)
    pl.semaphore_wait(barrier, 6)


def remote(src, dst, ssem, rsem, peer):
    return pltpu.make_async_remote_copy(
        src_ref=src, dst_ref=dst, send_sem=ssem, recv_sem=rsem,
        device_id=peer, device_id_type=pl.DeviceIdType.MESH,
    )


def blocks(shard):
    rows, columns = shard.shape
    return shard.reshape(2, 3, rows // 6, columns)


def head_lanes(block, head):
    lane = lax.broadcasted_iota(jnp.int32, (1, block.shape[1]), 1)
    keep = jnp.where(lane >= HD, float(head), 1.0 - head)
    return block * keep.astype(BF)


def softmax_keys(scores, valid):
    scores = jnp.where(valid, scores, masked_score)
    weights = jnp.exp(scores - jnp.max(scores, axis=0, keepdims=True))
    return weights * (1.0 / jnp.sum(weights, axis=0, keepdims=True))


def short_valid(tab_ref, pair, size):
    key = lax.broadcasted_iota(jnp.int32, (size, size), 0)
    query = lax.broadcasted_iota(jnp.int32, (size, size), 1)
    low, high = tab_ref[0, 65 + 2 * pair], tab_ref[0, 66 + 2 * pair]
    bound = jnp.where(key >= SHORT, SHORT + high, low)
    return (key < bound) & (key // SHORT == query // SHORT)


def attend_kernel(scale, tab_ref, q_ref, k_ref, v_ref, out_ref, long_ref, short_ref):
    two = 2 * SHORT
    key = lax.broadcasted_iota(jnp.int32, (LONG, LONG), 0)
    valid = key < tab_ref[0, 64]
    shorts = (q_ref.shape[0] - LONG) // two
    keeps = [short_valid(tab_ref, b, two) for b in range(shorts)]
    total = None
    tails = [None] * shorts
    for h in range(2):
        scores = dot(head_lanes(k_ref[0:LONG], h), q_ref[0:LONG], NT) * scale
        probs = softmax_keys(scores, valid).astype(BF)
        long_ref[h] = probs
        part = dot(probs, head_lanes(v_ref[0:LONG], h), TN)
        total = part if total is None else total + part
        for b in range(shorts):
            rows = slice(LONG + b * two, LONG + (b + 1) * two)
            scores = dot(head_lanes(k_ref[rows], h), q_ref[rows], NT) * scale
            probs = softmax_keys(scores, keeps[b]).astype(BF)
            short_ref[h, b * two : (b + 1) * two] = probs
            part = dot(probs, head_lanes(v_ref[rows], h), TN)
            tails[b] = part if tails[b] is None else tails[b] + part
    out_ref[0:LONG] = total.astype(BF)
    for b in range(shorts):
        out_ref[LONG + b * two : LONG + (b + 1) * two] = tails[b].astype(BF)


def attend(tab, projected):
    rows, wide = projected.shape
    width = wide // 3
    pairs = width // (2 * HD)
    column = lambda off: pl.BlockSpec((rows, 2 * HD), lambda i, off=off: (0, off + i))
    return pl.pallas_call(
        functools.partial(attend_kernel, HD ** (-0.5)),
        grid=(pairs,),
        out_shape=(
            jax.ShapeDtypeStruct((rows, width), BF),
            jax.ShapeDtypeStruct((2 * pairs, LONG, LONG), BF),
            jax.ShapeDtypeStruct((2 * pairs, rows - LONG, 2 * SHORT), BF),
        ),
        in_specs=[sm(), column(0), column(pairs), column(2 * pairs)],
        out_specs=(
            column(0),
            pl.BlockSpec((2, LONG, LONG), lambda i: (i, 0, 0)),
            pl.BlockSpec((2, rows - LONG, 2 * SHORT), lambda i: (i, 0, 0)),
        ),
        compiler_params=params(),
        name="attend",
    )(tab, projected, projected, projected)


def attend_back_kernel(scale, q_ref, k_ref, v_ref, g_ref, long_ref, short_ref, out_ref):
    two = 2 * SHORT
    shorts = (q_ref.shape[0] - LONG) // two
    spans = [(slice(0, LONG), None)]
    spans += [(slice(LONG + b * two, LONG + (b + 1) * two), b) for b in range(shorts)]
    for rows, b in spans:
        sums = None
        for h in range(2):
            probs = long_ref[h] if b is None else short_ref[h, b * two : (b + 1) * two]
            grad = head_lanes(g_ref[rows], h)
            wide = probs.astype(F32)
            grad_probs = dot(v_ref[rows], grad, NT)
            mean = jnp.sum(grad_probs * wide, axis=0, keepdims=True)
            grad_scores = (wide * (grad_probs - mean)).astype(BF)
            parts = (
                dot(grad_scores, head_lanes(k_ref[rows], h), TN),
                dot(grad_scores, head_lanes(q_ref[rows], h)),
                dot(probs, grad),
            )
            sums = parts if sums is None else tuple(a + p for a, p in zip(sums, parts))
        out_ref[0, rows] = (sums[0] * scale).astype(BF)
        out_ref[1, rows] = (sums[1] * scale).astype(BF)
        out_ref[2, rows] = sums[2].astype(BF)


def attend_back(projected, grad_mixed, long_probs, short_probs):
    rows, wide = projected.shape
    width = wide // 3
    pairs = width // (2 * HD)
    column = lambda off: pl.BlockSpec((rows, 2 * HD), lambda i, off=off: (0, off + i))
    return pl.pallas_call(
        functools.partial(attend_back_kernel, HD ** (-0.5)),
        grid=(pairs,),
        out_shape=jax.ShapeDtypeStruct((3, rows, width), BF),
        in_specs=[
            column(0), column(pairs), column(2 * pairs), column(0),
            pl.BlockSpec((2, LONG, LONG), lambda i: (i, 0, 0)),
            pl.BlockSpec((2, rows - LONG, 2 * SHORT), lambda i: (i, 0, 0)),
        ],
        out_specs=pl.BlockSpec((3, rows, 2 * HD), lambda i: (0, 0, i)),
        compiler_params=params(),
        name="attend_back",
    )(projected, projected, projected, grad_mixed, long_probs, short_probs)


def gelu_pair(value):
    size = jnp.abs(value)
    bell = jnp.exp(-0.5 * value * value)
    t = 1.0 / (1.0 + 0.23164189 * size)
    tail = t * (0.127414796 + t * (-0.142248368 + t * (0.7107068705 + t * (-0.7265760135 + t * 0.5307027145))))
    tail = tail * bell
    whole = jnp.where(value >= 0.0, 1.0 - tail, tail)
    return (value * whole, whole + value * bell * 0.3989422804)


def middle_kernel(
    step, span, mixed, tokens, cot, w_out, w_up, w_down, vectors, ff_bias,
    out, acc, g_mixed, d_out, d_up, d_down, sums, d_ffb, unit, low, low2, hidden, slope, inv
):
    rows = mixed.shape[0]
    parts = w_up.shape[1] // span
    sums[...] = jnp.zeros_like(sums)

    def rows_at(i):
        return pl.ds(pl.multiple_of(i * step, step), step)

    def columns_at(j):
        return pl.ds(pl.multiple_of(j * span, span), span)

    def mean(a):
        return jnp.mean(a, axis=-1, keepdims=True)

    def tally(i, a):
        sums[i : i + 1, :] += jnp.sum(a, axis=0, keepdims=True)

    def norm(r):
        center = r - mean(r)
        scale = lax.rsqrt(mean(center * center) + norm_eps)
        return center * scale, scale

    def back(s, u, scale):
        return scale * (s - mean(s) - u * mean(s * u))

    @pl.loop(0, rows // step)
    def _(i):
        at = rows_at(i)
        branch = dot(mixed[at, :], w_out[...]) + vectors[2:3, :]
        u, scale = norm(tokens[at, :].astype(F32) + branch)
        unit[at, :] = u
        inv[at, :] = scale
        low[at, :] = (u * vectors[6:7, :] + vectors[4:5, :]).astype(BF)
        acc[at, :] = jnp.zeros((step, acc.shape[1]), F32)

    @pl.loop(0, parts)
    def _(j):
        cols = columns_at(j)
        for i in range(rows // step):
            at = slice(i * step, (i + 1) * step)
            inner = dot(low[at, :], w_up[:, cols]) + ff_bias[:, cols]
            act, der = gelu_pair(inner)
            act = act.astype(BF)
            hidden[at, cols] = act
            slope[at, cols] = der.astype(BF)
            acc[at, :] += dot(act, w_down[cols, :])

    @pl.loop(0, rows // step)
    def _(i):
        at = rows_at(i)
        first = unit[at, :] * vectors[6:7, :] + vectors[4:5, :]
        u, scale = norm(first + acc[at, :] + vectors[3:4, :])
        out[at, :] = (u * vectors[7:8, :] + vectors[5:6, :]).astype(BF)
        g = cot[at, :].astype(F32)
        tally(1, g * u)
        tally(5, g)
        g = back(g * vectors[7:8, :], u, scale)
        acc[at, :] = g
        g = g.astype(BF)
        low2[at, :] = g
        tally(3, g.astype(F32))

    @pl.loop(0, parts)
    def _(j):
        cols = columns_at(j)
        total = None
        for i in range(rows // step):
            at = slice(i * step, (i + 1) * step)
            g = dot(low2[at, :], w_down[cols, :], NT) * slope[at, cols].astype(F32)
            g = g.astype(BF)
            slope[at, cols] = g
            part = jnp.sum(g.astype(F32), axis=0, keepdims=True)
            total = part if total is None else total + part
            acc[at, :] += dot(g, w_up[:, cols], NT)
        d_ffb[:, cols] = total
        d_down[cols, :] = dot(hidden[:, cols], low2[...], TN).astype(BF)
        d_up[:, cols] = dot(low[...], slope[:, cols], TN).astype(BF)

    @pl.loop(0, rows // step)
    def _(i):
        at = rows_at(i)
        g, u = acc[at, :], unit[at, :]
        tally(0, g * u)
        tally(4, g)
        g = back(g * vectors[6:7, :], u, inv[at, :])
        acc[at, :] = g
        g = g.astype(BF)
        low2[at, :] = g
        tally(2, g.astype(F32))
        g_mixed[at, :] = dot(g, w_out[...], NT).astype(BF)

    d_out[...] = dot(mixed[...], low2[...], TN).astype(BF)


def middle(mixed, tokens, cot, w_out, w_up, w_down, vectors, ff_bias):
    rows, width = mixed.shape
    ff = w_up.shape[1]
    shape = jax.ShapeDtypeStruct
    return pl.pallas_call(
        functools.partial(middle_kernel, 256, 512),
        out_shape=(
            shape((rows, width), BF), shape((rows, width), F32), shape((rows, width), BF),
            shape((width, width), BF), shape((width, ff), BF), shape((ff, width), BF),
            shape((8, width), F32), shape((1, ff), F32),
        ),
        in_specs=[vm()] * 8,
        out_specs=(vm(),) * 8,
        scratch_shapes=[
            pltpu.VMEM((rows, width), F32), pltpu.VMEM((rows, width), BF),
            pltpu.VMEM((rows, width), BF), pltpu.VMEM((rows, ff), BF),
            pltpu.VMEM((rows, ff), BF), pltpu.VMEM((rows, 1), F32),
        ],
        compiler_params=params(),
        name="middle",
    )(mixed, tokens, cot, w_out, w_up, w_down, vectors, ff_bias)


def head_kernel(scale, pairs, tab, *refs):
    n = 5
    bias_rows, norm_gains, ff_bias, raw, raw_cot = refs[:5]
    shards = (None,) + refs[5 : n + 4]
    fulls = (None,) + refs[n + 4 : 2 * n + 3]
    projected, mixed, long_hbm, short_hbm, tokens, cot, vectors, wide_bias = refs[2 * n + 3 : 2 * n + 11]
    ssem, rsem, lsem, osem, bias, long_buf, short_buf, tile, small, small_full = refs[2 * n + 11 :]
    shards = (small,) + shards[1:]
    fulls = (small_full,) + fulls[1:]
    kept, cut = bias_rows.shape
    tile[...] = jnp.zeros_like(tile)
    tile[0:kept, 0:cut] = bias_rows[...].astype(F32)
    tile[kept : kept + 2, 0:cut] = norm_gains[...].astype(F32)
    pieces = ff_bias.shape[1] // 128
    for j in range(pieces):
        tile[8 + j : 9 + j, :] = ff_bias[:, j * 128 : (j + 1) * 128].astype(F32)
    small[...] = jnp.zeros_like(small)
    small[0, 0] = tile[...].astype(BF)
    z, y, x, c = place_of()
    zs, yp, xp, cp = peers(z, y, x, c)
    greet(zs, yp, xp, cp)
    width = tokens.shape[1]
    two = 2 * HD
    sent = []

    def go(w, i, src, dst, peer):
        copy = remote(src, dst, ssem.at[w, i], rsem.at[w, i], peer)
        copy.start()
        sent.append(copy)

    def arrive(w, i, ref):
        remote(ref, ref, ssem.at[w, i], rsem.at[w, i], cp).wait_recv()

    def local(w):
        return pltpu.make_async_copy(shards[w], fulls[w].at[z, y], lsem.at[w])

    def near(w):
        local(w).start()
        src = shards[w].at[c, pl.ds(x, 2)]
        dst = fulls[w].at[z, y, c, pl.ds(x, 2)]
        for k in range(3):
            go(w, k, src, dst, zs[k])
        go(w, 3, src, dst, yp)

    def mid_at(w, k):
        zk = (z + 3 - k) % 4
        part = fulls[w].at[zk, y, c, pl.ds(x, 2)]
        arrive(w, k, part)
        go(w, 4 + k, part, part, yp)
        q = fulls[w].at[zk, y, c, 2 * x]
        go(w, 7 + k, q, q, xp)

    def far_at(w, k):
        zk = (z + 4 - k) % 4
        part = fulls[w].at[zk, 1 - y, c, pl.ds(x, 2)]
        arrive(w, 3 + k, part)
        q = fulls[w].at[zk, 1 - y, c, 2 * x]
        go(w, 10 + k, q, q, xp)

    def mid(w):
        for k in range(3):
            mid_at(w, k)

    def far(w):
        for k in range(4):
            far_at(w, k)

    def across(w):
        for k in range(7):
            zk, yk = ((z + 3 - k) % 4, y) if k < 3 else ((z + 7 - k) % 4, 1 - y)
            arrive(w, 7 + k, fulls[w].at[zk, yk, c, 2 * (1 - x)])
            part = fulls[w].at[zk, yk, c]
            go(w, 14 + k, part, part, cp)

    def last(w):
        for k in range(7):
            zk, yk = ((z + 3 - k) % 4, y) if k < 3 else ((z + 7 - k) % 4, 1 - y)
            arrive(w, 14 + k, fulls[w].at[zk, yk, 1 - c])
        local(w).wait()

    def project():
        rows = [fulls[0][i // 2, i % 2, 0, 0].astype(F32) for i in range(8)]
        vectors[...] = jnp.concatenate([r[0:8, 0:cut] for r in rows], 1)
        wide_bias[...] = jnp.concatenate([r[8 + j : 9 + j, :] for r in rows for j in range(pieces)], 1)
        bias[...] = jnp.zeros_like(bias)
        bias[:, 0:width] = vectors[0:1, :]
        bias[:, 2 * width :] = vectors[1:2, :]
        span = width // 2

        @pl.loop(0, 6)
        def _(j):
            cols = pl.ds(pl.multiple_of(j * span, span), span)
            part = fulls[1][:, :, :, :, :, cols].reshape(width, span)
            projected[:, cols] = (dot(tokens[...], part) + bias[:, cols]).astype(BF)

    def store(i):
        return (
            pltpu.make_async_copy(long_buf.at[i % 2], long_hbm.at[2 * i : 2 * i + 2], osem.at[i % 2]),
            pltpu.make_async_copy(short_buf.at[i % 2], short_hbm.at[2 * i : 2 * i + 2], osem.at[2 + i % 2]),
        )

    def attend_at(i):
        if i >= 2:
            for copy in store(i - 2):
                copy.wait()
        at = pl.ds(i * two, two)
        attend_kernel(
            scale, tab,
            projected.at[:, at],
            projected.at[:, pl.ds(width + i * two, two)],
            projected.at[:, pl.ds(2 * width + i * two, two)],
            mixed.at[:, at], long_buf.at[i % 2], short_buf.at[i % 2],
        )
        for copy in store(i):
            copy.start()

    for w in range(n):
        near(w)
    fill_selection(tab, long_buf, False)
    move_rows(long_buf, [raw], tokens)
    move_rows(long_buf, [raw_cot], cot)
    mid(0)
    mid(1)
    far(0)
    far(1)
    across(0)
    across(1)
    mid(2)
    last(0)
    last(1)
    far(2)
    project()
    across(2)
    attend_at(0)
    mid_at(3, 0)
    attend_at(1)
    mid_at(3, 1)
    attend_at(2)
    far_at(3, 0)
    mid_at(3, 2)
    attend_at(3)
    far_at(3, 1)
    attend_at(4)
    far_at(3, 2)
    mid_at(4, 0)
    attend_at(5)
    far_at(3, 3)
    last(2)
    mid_at(4, 1)
    far_at(4, 0)
    across(3)
    mid_at(4, 2)
    far_at(4, 1)
    far_at(4, 2)
    far_at(4, 3)
    last(3)
    across(4)
    last(4)
    for i in (pairs - 2, pairs - 1):
        for copy in store(i):
            copy.wait()
    for copy in sent:
        copy.wait_send()


def head(tab, bias_rows, norm_gains, ff_bias, shards, tokens, cotangent):
    n = len(shards) + 1
    views = [blocks(s) for s in shards]
    rows, width = tokens.shape
    pairs = width // (2 * HD)
    shape = jax.ShapeDtypeStruct
    anywhere = pl.BlockSpec(memory_space=pl.ANY)
    results = pl.pallas_call(
        functools.partial(head_kernel, HD ** (-0.5), pairs),
        out_shape=[shape((4, 2) + v.shape, v.dtype) for v in views]
        + [
            shape((rows, 3 * width), BF), shape((rows, width), BF),
            shape((2 * pairs, LONG, LONG), BF), shape((2 * pairs, rows - LONG, 2 * SHORT), BF),
            shape((rows, width), BF), shape((rows, width), BF),
            shape((8, width), F32), shape((1, 8 * ff_bias.shape[0]), F32),
        ],
        in_specs=[sm()] + [vm()] * (n + 4),
        out_specs=[vm()] + [anywhere] * 3 + [vm()] * 2 + [anywhere] * 2 + [vm()] * 4,
        scratch_shapes=[
            pltpu.SemaphoreType.DMA((n, 21)), pltpu.SemaphoreType.DMA((n, 21)),
            pltpu.SemaphoreType.DMA((n,)), pltpu.SemaphoreType.DMA((4,)),
            pltpu.VMEM((1, 3 * width), F32),
            pltpu.VMEM((2, 2, LONG, LONG), BF), pltpu.VMEM((2, 2, rows - LONG, 2 * SHORT), BF),
            pltpu.VMEM((16, 128), F32), pltpu.VMEM((2, 3, 16, 128), BF),
            pltpu.VMEM((4, 2, 2, 3, 16, 128), BF),
        ],
        compiler_params=params(collective_id=0, has_side_effects=True),
        name="head",
    )(tab, bias_rows, norm_gains, ff_bias[None], tokens, cotangent, *views)
    return [f.reshape(8 * s.shape[0], s.shape[1]) for f, s in zip(results, shards)], results[n - 1 :]


def tail_kernel(scale, pairs, tab, *refs):
    d_down, d_up, d_out, sums, d_ffb, projected, g_mixed, tokens, grad_one, long_hbm, short_hbm, w_hbm = refs[:12]
    outs, grad_tokens = refs[12:17], refs[17]
    own = refs[18:]
    n = 5
    half, rx, rpy, rqy, rpz, rqz, rpx, fin, got = (own[i * n : (i + 1) * n] for i in range(9))
    ssem, rsem, lsem, d_qkv, small, heads, long_buf, short_buf, w_qkv = own[9 * n :]
    grads = [d_down, d_up, d_out, d_qkv, small]
    z, y, x, c = place_of()
    zs, yp, xp, cp = peers(z, y, x, c)
    width = tokens.shape[1]
    two = 2 * HD
    sent = []

    def fetch(i):
        return (
            pltpu.make_async_copy(long_hbm.at[2 * i : 2 * i + 2], long_buf.at[i % 2], lsem.at[i % 2]),
            pltpu.make_async_copy(short_hbm.at[2 * i : 2 * i + 2], short_buf.at[i % 2], lsem.at[2 + i % 2]),
        )

    weights = pltpu.make_async_copy(w_hbm, w_qkv, lsem.at[4])
    weights.start()
    for copy in fetch(0):
        copy.start()
    small[...] = jnp.zeros_like(small)
    cut, long_cut = sums.shape[1] // 8, d_ffb.shape[1] // 8
    for i in range(8):
        at = slice(i * cut, (i + 1) * cut)
        small[i // 2, i % 2, 0, 0, 2:6, 0:cut] = sums[2:6, at]
        small[i // 2, i % 2, 0, 0, 6:8, 0:cut] = sums[0:2, at]
        for j in range(long_cut // 128):
            first = i * long_cut + j * 128
            small[i // 2, i % 2, 0, 1, j : j + 1, :] = d_ffb[:, first : first + 128]
    greet(zs, yp, xp, cp)

    def go(w, i, src, dst, peer):
        copy = remote(src, dst, ssem.at[w, i], rsem.at[w, i], peer)
        copy.start()
        sent.append(copy)

    def arrive(w, i, ref):
        remote(ref, ref, ssem.at[w, i], rsem.at[w, i], cp).wait_recv()

    def add(*parts):
        total = parts[0].astype(F32)
        for part in parts[1:]:
            total = total + part.astype(F32)
        return total

    def s0(w):
        go(w, 0, grads[w].at[:, :, 1 - c], half[w], cp)

    def s1(w):
        arrive(w, 0, half[w])
        a = half[w]

        @pl.loop(0, 4)
        def _(i):
            for j in range(2):
                for k in range(3):
                    a[i, j, k] = add(grads[w][i, j, c, k], a[i, j, k]).astype(a.dtype)

        go(w, 1, a.at[:, :, 2 * (1 - x)], rx[w], xp)
        go(w, 2, a.at[:, 1 - y, 1], rpy[w], yp)

    def s2p(w):
        a = half[w]
        arrive(w, 2, rpy[w])

        @pl.loop(0, 4)
        def _(i):
            a[i, y, 1] = add(a[i, y, 1], rpy[w][i]).astype(a.dtype)

        for k in range(3):
            go(w, 3 + k, a.at[(z + k + 1) % 4, y, 1], rpz[w].at[k], zs[k])

    def s2q(w):
        a = half[w]
        arrive(w, 1, rx[w])

        @pl.loop(0, 4)
        def _(i):
            for j in range(2):
                a[i, j, 2 * x] = add(a[i, j, 2 * x], rx[w][i, j]).astype(a.dtype)

        go(w, 6, a.at[:, 1 - y, 2 * x], rqy[w], yp)

    def s3p(w):
        a = half[w]
        for k in range(3):
            arrive(w, 3 + k, rpz[w].at[k])
        a[z, y, 1] = add(a[z, y, 1], rpz[w][0], rpz[w][1], rpz[w][2]).astype(a.dtype)
        go(w, 10, a.at[z, y, 1], rpx[w], xp)

    def s3q(w):
        a = half[w]
        arrive(w, 6, rqy[w])

        @pl.loop(0, 4)
        def _(i):
            a[i, y, 2 * x] = add(a[i, y, 2 * x], rqy[w][i]).astype(a.dtype)

        for k in range(3):
            go(w, 7 + k, a.at[(z + k + 1) % 4, y, 2 * x], rqz[w].at[k], zs[k])

    def s4p(w):
        a = half[w]
        arrive(w, 10, rpx[w])
        fin[w][1] = add(a[z, y, 1], rpx[w][...]).astype(a.dtype)
        go(w, 14, fin[w].at[1], got[w].at[c, 1], cp)

    def s4q(w):
        a = half[w]
        for k in range(3):
            arrive(w, 7 + k, rqz[w].at[k])
        fin[w][0] = add(a[z, y, 2 * x], rqz[w][0], rqz[w][1], rqz[w][2]).astype(a.dtype)
        go(w, 11, fin[w].at[0], got[w].at[c, 2 * x], xp)
        go(w, 13, fin[w].at[0], got[w].at[c, 2 * x], cp)

    def s5(w):
        arrive(w, 11, got[w].at[c, 2 * (1 - x)])
        piece = got[w].at[c, 2 * (1 - x)]
        go(w, 12, piece, piece, cp)
        outs[w][c, 2 * x] = fin[w][0].astype(F32)
        outs[w][c, 1] = fin[w][1].astype(F32)
        outs[w][c, 2 * (1 - x)] = got[w][c, 2 * (1 - x)].astype(F32)

    def s6(w):
        arrive(w, 12, got[w].at[1 - c, 2 * (1 - x)])
        arrive(w, 13, got[w].at[1 - c, 2 * x])
        arrive(w, 14, got[w].at[1 - c, 1])
        for k in range(3):
            outs[w][1 - c, k] = got[w][1 - c, k].astype(F32)

    def back(i):
        if i + 1 < pairs:
            for copy in fetch(i + 1):
                copy.start()
        for copy in fetch(i):
            copy.wait()
        at = pl.ds(i * two, two)
        attend_back_kernel(
            scale,
            projected.at[:, at],
            projected.at[:, pl.ds(width + i * two, two)],
            projected.at[:, pl.ds(2 * width + i * two, two)],
            g_mixed.at[:, at],
            long_buf.at[i % 2], short_buf.at[i % 2],
            heads.at[:, :, at],
        )

    def weight(k):
        part = 256
        for j in range(width // part):
            at = slice(j * part, (j + 1) * part)
            value = dot(tokens[...], heads[k, :, at], TN).astype(BF)
            d_qkv[:, :, :, :, :, k * width + j * part : k * width + (j + 1) * part] = value.reshape(
                d_qkv.shape[:5] + (part,)
            )
        if k != 1:
            total = jnp.sum(heads[k].astype(F32), axis=0, keepdims=True)
            for i in range(8):
                row = k // 2
                small[i // 2, i % 2, 0, 0, row : row + 1, 0:cut] = total[:, i * cut : (i + 1) * cut]

    def rows_back(i):
        step = tokens.shape[0] // 4
        at = slice(i * step, (i + 1) * step)
        total = grad_one[at, :]
        for k in range(3):
            total = total + dot(heads[k, at, :], w_qkv[:, k * width : (k + 1) * width], NT)
        for k in range(3):
            part = total.astype(BF)
            total = total - part.astype(F32)
            heads[k, at, :] = part

    def select(_):
        fill_selection(tab, long_buf, True)

    def token_rows(_):
        move_rows(long_buf, [heads.at[0], heads.at[1], heads.at[2]], grad_tokens)

    def run(*steps):
        for f, *which in steps:
            for w in which:
                f(w)

    run(
        (s0, 0, 1, 2), (back, 0, 1), (s1, 0), (back, 2), (s1, 1), (back, 3, 4), (s2p, 0), (back, 5),
        (s2p, 1), (weight, 0), (s2q, 0), (weight, 1, 2), (s0, 3, 4), (s3p, 0), (s3q, 0), (select, 0),
    )
    weights.wait()
    run(
        (rows_back, 0), (s1, 3, 2, 4), (s3p, 1), (s4q, 0), (s4p, 0), (rows_back, 1), (s2q, 1),
        (s2p, 3, 2, 4), (rows_back, 2), (s3q, 1), (s4p, 1), (s5, 0), (rows_back, 3), (token_rows, 0), (s2q, 3),
        (s3p, 3, 2, 4), (s4q, 1), (s2q, 2, 4), (s3q, 3), (s5, 1), (s3q, 2, 4), (s4p, 3, 2, 4),
        (s6, 0), (s4q, 3), (s6, 1), (s4q, 2, 4), (s5, 3, 2, 4), (s6, 3, 2, 4),
    )
    for copy in sent:
        copy.wait_send()


def tail(tab, d_down, d_up, d_out, sums, d_ffb, projected, g_mixed, tokens, grad_one, long_probs, short_probs, w_qkv):
    rows, wide = projected.shape
    width = wide // 3
    pairs = width // (2 * HD)

    def view(shape):
        return (4, 2, 2, 3, shape[0] // 48, shape[1])

    views = [g.reshape(view(g.shape)) for g in (d_down, d_up, d_out)]
    small_view = (4, 2, 2, 3, 8, 128)
    qkv_view = view(w_qkv.shape)
    kinds = [(v.shape, v.dtype) for v in views[:3]] + [(qkv_view, BF), (small_view, F32)]
    lead = ((4, 2, 3), (4, 2), (4,), (4,), (3,), (3,), (), (2,), (2, 3))
    scratch = [pltpu.VMEM(s + v[4:], t) for s in lead for v, t in kinds]
    anywhere = pl.BlockSpec(memory_space=pl.ANY)
    results = pl.pallas_call(
        functools.partial(tail_kernel, HD ** (-0.5), pairs),
        out_shape=[jax.ShapeDtypeStruct(v[2:], F32) for v, _ in kinds]
        + [jax.ShapeDtypeStruct((rows, width), F32)],
        in_specs=[sm()] + [vm()] * 9 + [anywhere] * 3,
        out_specs=[vm()] * 6,
        scratch_shapes=scratch
        + [
            pltpu.SemaphoreType.DMA((5, 15)), pltpu.SemaphoreType.DMA((5, 15)),
            pltpu.SemaphoreType.DMA((5,)),
            pltpu.VMEM(qkv_view, BF), pltpu.VMEM(small_view, F32),
            pltpu.VMEM((3, rows, width), BF),
            pltpu.VMEM((2, 2) + long_probs.shape[1:], BF),
            pltpu.VMEM((2, 2) + short_probs.shape[1:], BF),
            pltpu.VMEM(w_qkv.shape, BF),
        ],
        compiler_params=params(collective_id=1, has_side_effects=True),
        name="tail",
    )(tab, *views, sums, d_ffb, projected, g_mixed, tokens, grad_one, long_probs, short_probs, w_qkv)
    flat = [o.reshape(-1, o.shape[-1]) for o in results[:5]]
    return flat, results[5]


def square():
    return lax.axis_size("dp") == 8 and lax.axis_size("rep") == 4


def front_layer(tab, tokens, cotangent, qkv_weight, out_weight, up_weight, down_weight, norm_gains, bias_rows, ff_bias):
    width = tokens.shape[1]
    if not square():
        tokens, cotangent = permute(tab, tokens, False), permute(tab, cotangent, False)
        w_qkv, w_out, w_up, w_down = (
            lax.all_gather(w, "dp", axis=0, tiled=True)
            for w in (qkv_weight, out_weight, up_weight, down_weight)
        )
        gains = lax.all_gather(norm_gains, "dp", axis=1, tiled=True)
        biases = lax.all_gather(bias_rows, "dp", axis=1, tiled=True)
        up_bias = lax.all_gather(ff_bias, "dp", axis=0, tiled=True)
        wide = biases.astype(F32)
        bias = jnp.concatenate([wide[0], jnp.zeros((width,), F32), wide[1]])
        projected = (dot(tokens, w_qkv) + bias).astype(BF)
        mixed, *probs = attend(tab, projected)
        return (
            w_qkv, w_out, w_up, w_down,
            jnp.concatenate([biases, gains]).astype(F32), up_bias.astype(F32)[None],
            tokens, cotangent, projected, mixed, tuple(probs),
        )

    full, (projected, mixed, *probs, tokens, cotangent, vectors, up_bias) = head(
        tab, bias_rows, norm_gains, ff_bias, [qkv_weight, out_weight, up_weight, down_weight], tokens, cotangent
    )
    return (*full, vectors, up_bias, tokens, cotangent, projected, mixed, tuple(probs))


def reduce_layer(d_qkv, d_out, d_up, d_down, d_gains, d_biases, d_up_bias):
    def full(g):
        part = lax.psum_scatter(g, "rep", scatter_dimension=1, tiled=True).astype(F32)
        part = lax.psum_scatter(part, "dp", scatter_dimension=0, tiled=True)
        return lax.all_gather(part.astype(BF), "rep", axis=1, tiled=True).astype(F32)

    small = lax.psum(
        (
            lax.psum_scatter(d_gains, "dp", scatter_dimension=1, tiled=True),
            lax.psum_scatter(d_biases, "dp", scatter_dimension=1, tiled=True),
            lax.psum_scatter(d_up_bias, "dp", scatter_dimension=0, tiled=True),
        ),
        "rep",
    )
    return tuple(full(g.astype(BF)) for g in (d_qkv, d_out, d_up, d_down)) + small


def back_layer(tab, final, projected, grad_mixed, probs, tokens, grad_one, w_qkv, d_out, d_up, d_down, sums, d_up_bias):
    width = tokens.shape[1]
    if not square():
        parts = attend_back(projected, grad_mixed, *probs)
        grad_heads = jnp.concatenate([parts[0], parts[1], parts[2]], 1)
        d_head = jnp.sum(grad_heads.astype(F32), axis=0)[None]
        d_qkv = dot(tokens, grad_heads, TN)
        grad_tokens = grad_one + dot(grad_heads, w_qkv, NT)
        d_biases = jnp.concatenate([d_head[:, :width], d_head[:, 2 * width :], sums[2:6]])
        moved = (permute(tab, final, True), permute(tab, grad_tokens, True))
        return moved + reduce_layer(d_qkv, d_out, d_up, d_down, sums[0:2], d_biases, d_up_bias[0])

    (down, up, out, qkv, own), grad_tokens = tail(
        tab, d_down, d_up, d_out, sums, d_up_bias, projected, grad_mixed, tokens, grad_one, *probs, w_qkv
    )
    cut, pieces = width // 8, d_up_bias.shape[1] // (8 * 128)
    return (
        permute(tab, final, True), grad_tokens, qkv, out, up, down,
        own[6:8, :cut], own[0:6, :cut], own[8 : 8 + pieces].reshape(-1),
    )


def local(
    tokens,
    qkv_weight,
    out_weight,
    up_weight,
    down_weight,
    norm_gains,
    bias_rows,
    ff_bias,
    lengths,
    owners,
    cotangent,
):
    row_count = tokens.shape[0]
    device = lax.axis_index("dp") * lax.axis_size("rep") + lax.axis_index("rep")
    devices = lax.axis_size("dp") * lax.axis_size("rep")
    per = lengths.shape[0] // devices
    assert row_count == LONG + SHORT * (per - 1) == 2 * LONG
    me = device.astype(jnp.int32).reshape(1)
    tab = slot_table(me, owners, lengths, per)
    w_qkv, w_out, w_up, w_down, vectors, up_bias, tokens, cotangent, projected, mixed_rows, probs = front_layer(
        tab, tokens, cotangent, qkv_weight, out_weight, up_weight, down_weight, norm_gains, bias_rows, ff_bias
    )
    final, grad_one, grad_mixed, d_out, d_up, d_down, sums, d_up_bias = middle(
        mixed_rows, tokens, cotangent, w_out, w_up, w_down, vectors, up_bias
    )
    return back_layer(
        tab, final, projected, grad_mixed, probs, tokens, grad_one, w_qkv,
        d_out, d_up, d_down, sums, d_up_bias,
    )


def solution(mesh):
    in_specs = (
        P(("dp", "rep"), None),
        P("dp", None),
        P("dp", None),
        P("dp", None),
        P("dp", None),
        P(None, "dp"),
        P(None, "dp"),
        P("dp"),
        P(),
        P(),
        P(("dp", "rep"), None),
    )
    out_specs = (
        P(("dp", "rep"), None),
        P(("dp", "rep"), None),
        P("dp", None),
        P("dp", None),
        P("dp", None),
        P("dp", None),
        P(None, "dp"),
        P(None, "dp"),
        P("dp"),
    )
    return jax.shard_map(local, mesh=mesh, in_specs=in_specs, out_specs=out_specs, check_vma=False)
```

```python
import functools

import jax
import jax.numpy as jnp
from jax import lax
from jax.experimental import pallas as pl
from jax.experimental.pallas import tpu as pltpu
from jax.sharding import PartitionSpec as P

HEADS = 12
HD = 64
LONG = 512
SHORT = 64
norm_eps = 1e-06
masked_score = -1000000000.0
BF = jnp.bfloat16
F32 = jnp.float32
VMEM_LIMIT = 62 * 1024 * 1024

NN = (((1,), (0,)), ((), ()))
NT = (((1,), (1,)), ((), ()))
TN = (((0,), (0,)), ((), ()))


def dot(a, b, dims=NN):
    return lax.dot_general(a, b, dims, preferred_element_type=F32)


def vm():
    return pl.BlockSpec(memory_space=pltpu.VMEM)


def sm():
    return pl.BlockSpec(memory_space=pltpu.SMEM)


def params(**kw):
    return pltpu.CompilerParams(vmem_limit_bytes=VMEM_LIMIT, **kw)


def table_kernel(per, me_ref, own_ref, len_ref, tab_ref):
    total = own_ref.shape[0]
    me = me_ref[0]

    def zero(i, c):
        tab_ref[0, i] = 0
        return c

    lax.fori_loop(0, 128, zero, 0)

    def scan(p, c):
        count, start = c
        hit = own_ref[p] == me
        size = len_ref[p]
        tab_ref[0, count] = start
        tab_ref[0, 16 + count] = size
        return (count + hit.astype(jnp.int32), start + jnp.where(hit, size, 0))

    lax.fori_loop(0, total, scan, (jnp.int32(0), jnp.int32(0)), unroll=8)

    def find(j, c):
        return jnp.where(tab_ref[0, 16 + j] > SHORT, j, c)

    big = lax.fori_loop(0, per, find, jnp.int32(0))

    def place(j, slot):
        is_big = j == big
        tab_ref[0, 32 + j] = jnp.where(is_big, 0, LONG + SHORT * slot)
        tab_ref[0, 48 + j] = jnp.where(is_big, LONG // SHORT, 1)
        at = jnp.where(is_big, 0, slot + 1)
        tab_ref[0, 64 + at] = tab_ref[0, 16 + j]
        tab_ref[0, 80 + at] = tab_ref[0, j]
        return slot + jnp.where(is_big, 0, 1)

    lax.fori_loop(0, per, place, jnp.int32(0))


def slot_table(me, owners, lengths, per):
    return pl.pallas_call(
        functools.partial(table_kernel, per),
        out_shape=jax.ShapeDtypeStruct((1, 128), jnp.int32),
        in_specs=[sm(), sm(), sm()],
        out_specs=sm(),
        compiler_params=params(),
        name="table",
    )(me, owners, lengths)


def slot_source(tab_ref, block, shape, dim):
    at = lax.broadcasted_iota(jnp.int32, shape, dim)
    if block == 0:
        return jnp.where(at < tab_ref[0, 64], tab_ref[0, 80] + at, -1)
    source = jnp.full(shape, -1, jnp.int32)
    for s in range(LONG // SHORT):
        inner = at - s * SHORT
        good = (inner >= 0) & (inner < tab_ref[0, 65 + s])
        source = jnp.where(good, tab_ref[0, 81 + s] + inner, source)
    return source


def fill_selection(tab_ref, pick, back):
    for a in range(2):
        for b in range(2):
            slot, row = (b, a) if back else (a, b)
            source = slot_source(tab_ref, slot, (1, LONG) if back else (LONG, 1), 1 if back else 0)
            want = lax.broadcasted_iota(jnp.int32, (LONG, LONG), 0 if back else 1) + row * LONG
            pick[a, b] = jnp.where(source == want, 1.0, 0.0).astype(BF)


def move_rows(pick, srcs, dst):
    for a in range(2):
        total = None
        for b in range(2):
            for src in srcs:
                part = dot(pick[a, b], src[b * LONG : (b + 1) * LONG, :])
                total = part if total is None else total + part
        dst[a * LONG : (a + 1) * LONG, :] = total.astype(dst.dtype)


def permute_kernel(back, tab_ref, src_ref, out_ref, pick):
    fill_selection(tab_ref, pick, back)
    if out_ref.dtype == BF:
        return move_rows(pick, [src_ref], out_ref)
    value = src_ref[...]
    for k in range(3):
        part = value.astype(BF)
        value = value - part.astype(F32)
        for a in range(2):
            at = slice(a * LONG, (a + 1) * LONG)
            old = jnp.zeros((LONG, value.shape[1]), F32) if k == 0 else out_ref[at, :]
            for b in range(2):
                old = old + dot(pick[a, b], part[b * LONG : (b + 1) * LONG, :])
            out_ref[at, :] = old


def permute(tab, src, back):
    return pl.pallas_call(
        functools.partial(permute_kernel, back),
        out_shape=jax.ShapeDtypeStruct(src.shape, src.dtype),
        in_specs=[sm(), vm()],
        out_specs=vm(),
        scratch_shapes=[pltpu.VMEM((2, 2, LONG, LONG), BF)],
        compiler_params=params(),
        name="permute",
    )(tab, src)


def place_of():
    dp, rep = lax.axis_index("dp"), lax.axis_index("rep")
    return dp // 2, dp % 2, rep // 2, rep % 2


def peers(z, y, x, c):
    def at(z2, y2, x2, c2):
        return (z2 * 2 + y2, x2 * 2 + c2)

    return (
        [at((z + k) % 4, y, x, c) for k in (1, 2, 3)],
        at(z, 1 - y, x, c),
        at(z, y, 1 - x, c),
        at(z, y, x, 1 - c),
    )


def greet(zs, yp, xp, cp):
    barrier = pltpu.get_barrier_semaphore()
    for peer in (*zs, yp, xp, cp):
        pl.semaphore_signal(barrier, inc=1, device_id=peer, device_id_type=pl.DeviceIdType.MESH)
    pl.semaphore_wait(barrier, 6)


def remote(src, dst, ssem, rsem, peer):
    return pltpu.make_async_remote_copy(
        src_ref=src, dst_ref=dst, send_sem=ssem, recv_sem=rsem,
        device_id=peer, device_id_type=pl.DeviceIdType.MESH,
    )


def blocks(shard):
    rows, columns = shard.shape
    return shard.reshape(2, 3, rows // 6, columns)


def head_lanes(block, head):
    lane = lax.broadcasted_iota(jnp.int32, (1, block.shape[1]), 1)
    keep = jnp.where(lane >= HD, float(head), 1.0 - head)
    return block * keep.astype(BF)


def softmax_keys(scores, valid):
    scores = jnp.where(valid, scores, masked_score)
    weights = jnp.exp(scores - jnp.max(scores, axis=0, keepdims=True))
    return weights * (1.0 / jnp.sum(weights, axis=0, keepdims=True))


def short_valid(tab_ref, pair, size):
    key = lax.broadcasted_iota(jnp.int32, (size, size), 0)
    query = lax.broadcasted_iota(jnp.int32, (size, size), 1)
    low, high = tab_ref[0, 65 + 2 * pair], tab_ref[0, 66 + 2 * pair]
    bound = jnp.where(key >= SHORT, SHORT + high, low)
    return (key < bound) & (key // SHORT == query // SHORT)


def attend_kernel(scale, tab_ref, q_ref, k_ref, v_ref, out_ref, long_ref, short_ref):
    two = 2 * SHORT
    key = lax.broadcasted_iota(jnp.int32, (LONG, LONG), 0)
    valid = key < tab_ref[0, 64]
    shorts = (q_ref.shape[0] - LONG) // two
    keeps = [short_valid(tab_ref, b, two) for b in range(shorts)]
    total = None
    tails = [None] * shorts
    for h in range(2):
        scores = dot(head_lanes(k_ref[0:LONG], h), q_ref[0:LONG], NT) * scale
        probs = softmax_keys(scores, valid).astype(BF)
        long_ref[h] = probs
        part = dot(probs, head_lanes(v_ref[0:LONG], h), TN)
        total = part if total is None else total + part
        for b in range(shorts):
            rows = slice(LONG + b * two, LONG + (b + 1) * two)
            scores = dot(head_lanes(k_ref[rows], h), q_ref[rows], NT) * scale
            probs = softmax_keys(scores, keeps[b]).astype(BF)
            short_ref[h, b * two : (b + 1) * two] = probs
            part = dot(probs, head_lanes(v_ref[rows], h), TN)
            tails[b] = part if tails[b] is None else tails[b] + part
    out_ref[0:LONG] = total.astype(BF)
    for b in range(shorts):
        out_ref[LONG + b * two : LONG + (b + 1) * two] = tails[b].astype(BF)


def attend(tab, projected):
    rows, wide = projected.shape
    width = wide // 3
    pairs = width // (2 * HD)
    column = lambda off: pl.BlockSpec((rows, 2 * HD), lambda i, off=off: (0, off + i))
    return pl.pallas_call(
        functools.partial(attend_kernel, HD ** (-0.5)),
        grid=(pairs,),
        out_shape=(
            jax.ShapeDtypeStruct((rows, width), BF),
            jax.ShapeDtypeStruct((2 * pairs, LONG, LONG), BF),
            jax.ShapeDtypeStruct((2 * pairs, rows - LONG, 2 * SHORT), BF),
        ),
        in_specs=[sm(), column(0), column(pairs), column(2 * pairs)],
        out_specs=(
            column(0),
            pl.BlockSpec((2, LONG, LONG), lambda i: (i, 0, 0)),
            pl.BlockSpec((2, rows - LONG, 2 * SHORT), lambda i: (i, 0, 0)),
        ),
        compiler_params=params(),
        name="attend",
    )(tab, projected, projected, projected)


def attend_back_kernel(scale, q_ref, k_ref, v_ref, g_ref, long_ref, short_ref, out_ref):
    two = 2 * SHORT
    shorts = (q_ref.shape[0] - LONG) // two
    spans = [(slice(0, LONG), None)]
    spans += [(slice(LONG + b * two, LONG + (b + 1) * two), b) for b in range(shorts)]
    for rows, b in spans:
        sums = None
        for h in range(2):
            probs = long_ref[h] if b is None else short_ref[h, b * two : (b + 1) * two]
            grad = head_lanes(g_ref[rows], h)
            wide = probs.astype(F32)
            grad_probs = dot(v_ref[rows], grad, NT)
            mean = jnp.sum(grad_probs * wide, axis=0, keepdims=True)
            grad_scores = (wide * (grad_probs - mean)).astype(BF)
            parts = (
                dot(grad_scores, head_lanes(k_ref[rows], h), TN),
                dot(grad_scores, head_lanes(q_ref[rows], h)),
                dot(probs, grad),
            )
            sums = parts if sums is None else tuple(a + p for a, p in zip(sums, parts))
        out_ref[0, rows] = (sums[0] * scale).astype(BF)
        out_ref[1, rows] = (sums[1] * scale).astype(BF)
        out_ref[2, rows] = sums[2].astype(BF)


def attend_back(projected, grad_mixed, long_probs, short_probs):
    rows, wide = projected.shape
    width = wide // 3
    pairs = width // (2 * HD)
    column = lambda off: pl.BlockSpec((rows, 2 * HD), lambda i, off=off: (0, off + i))
    return pl.pallas_call(
        functools.partial(attend_back_kernel, HD ** (-0.5)),
        grid=(pairs,),
        out_shape=jax.ShapeDtypeStruct((3, rows, width), BF),
        in_specs=[
            column(0), column(pairs), column(2 * pairs), column(0),
            pl.BlockSpec((2, LONG, LONG), lambda i: (i, 0, 0)),
            pl.BlockSpec((2, rows - LONG, 2 * SHORT), lambda i: (i, 0, 0)),
        ],
        out_specs=pl.BlockSpec((3, rows, 2 * HD), lambda i: (0, 0, i)),
        compiler_params=params(),
        name="attend_back",
    )(projected, projected, projected, grad_mixed, long_probs, short_probs)


def gelu_pair(value):
    size = jnp.abs(value)
    bell = jnp.exp(-0.5 * value * value)
    t = 1.0 / (1.0 + 0.23164189 * size)
    tail = t * (0.127414796 + t * (-0.142248368 + t * (0.7107068705 + t * (-0.7265760135 + t * 0.5307027145))))
    tail = tail * bell
    whole = jnp.where(value >= 0.0, 1.0 - tail, tail)
    return (value * whole, whole + value * bell * 0.3989422804)


def middle_kernel(
    step, span, mixed, tokens, cot, w_out, w_up, w_down, vectors, ff_bias,
    out, acc, g_mixed, d_out, d_up, d_down, sums, d_ffb, unit, low, low2, hidden, slope, inv
):
    rows = mixed.shape[0]
    parts = w_up.shape[1] // span
    sums[...] = jnp.zeros_like(sums)

    def rows_at(i):
        return pl.ds(pl.multiple_of(i * step, step), step)

    def columns_at(j):
        return pl.ds(pl.multiple_of(j * span, span), span)

    def mean(a):
        return jnp.mean(a, axis=-1, keepdims=True)

    def tally(i, a):
        sums[i : i + 1, :] += jnp.sum(a, axis=0, keepdims=True)

    def norm(r):
        center = r - mean(r)
        scale = lax.rsqrt(mean(center * center) + norm_eps)
        return center * scale, scale

    def back(s, u, scale):
        return scale * (s - mean(s) - u * mean(s * u))

    @pl.loop(0, rows // step)
    def _(i):
        at = rows_at(i)
        branch = dot(mixed[at, :], w_out[...]) + vectors[2:3, :]
        u, scale = norm(tokens[at, :].astype(F32) + branch)
        unit[at, :] = u
        inv[at, :] = scale
        low[at, :] = (u * vectors[6:7, :] + vectors[4:5, :]).astype(BF)
        acc[at, :] = jnp.zeros((step, acc.shape[1]), F32)

    @pl.loop(0, parts)
    def _(j):
        cols = columns_at(j)
        for i in range(rows // step):
            at = slice(i * step, (i + 1) * step)
            inner = dot(low[at, :], w_up[:, cols]) + ff_bias[:, cols]
            act, der = gelu_pair(inner)
            act = act.astype(BF)
            hidden[at, cols] = act
            slope[at, cols] = der.astype(BF)
            acc[at, :] += dot(act, w_down[cols, :])

    @pl.loop(0, rows // step)
    def _(i):
        at = rows_at(i)
        first = unit[at, :] * vectors[6:7, :] + vectors[4:5, :]
        u, scale = norm(first + acc[at, :] + vectors[3:4, :])
        out[at, :] = (u * vectors[7:8, :] + vectors[5:6, :]).astype(BF)
        g = cot[at, :].astype(F32)
        tally(1, g * u)
        tally(5, g)
        g = back(g * vectors[7:8, :], u, scale)
        acc[at, :] = g
        g = g.astype(BF)
        low2[at, :] = g
        tally(3, g.astype(F32))

    @pl.loop(0, parts)
    def _(j):
        cols = columns_at(j)
        total = None
        for i in range(rows // step):
            at = slice(i * step, (i + 1) * step)
            g = dot(low2[at, :], w_down[cols, :], NT) * slope[at, cols].astype(F32)
            g = g.astype(BF)
            slope[at, cols] = g
            part = jnp.sum(g.astype(F32), axis=0, keepdims=True)
            total = part if total is None else total + part
            acc[at, :] += dot(g, w_up[:, cols], NT)
        d_ffb[:, cols] = total
        d_down[cols, :] = dot(hidden[:, cols], low2[...], TN).astype(BF)
        d_up[:, cols] = dot(low[...], slope[:, cols], TN).astype(BF)

    @pl.loop(0, rows // step)
    def _(i):
        at = rows_at(i)
        g, u = acc[at, :], unit[at, :]
        tally(0, g * u)
        tally(4, g)
        g = back(g * vectors[6:7, :], u, inv[at, :])
        acc[at, :] = g
        g = g.astype(BF)
        low2[at, :] = g
        tally(2, g.astype(F32))
        g_mixed[at, :] = dot(g, w_out[...], NT).astype(BF)

    d_out[...] = dot(mixed[...], low2[...], TN).astype(BF)


def middle(mixed, tokens, cot, w_out, w_up, w_down, vectors, ff_bias):
    rows, width = mixed.shape
    ff = w_up.shape[1]
    shape = jax.ShapeDtypeStruct
    return pl.pallas_call(
        functools.partial(middle_kernel, 256, 512),
        out_shape=(
            shape((rows, width), BF), shape((rows, width), F32), shape((rows, width), BF),
            shape((width, width), BF), shape((width, ff), BF), shape((ff, width), BF),
            shape((8, width), F32), shape((1, ff), F32),
        ),
        in_specs=[vm()] * 8,
        out_specs=(vm(),) * 8,
        scratch_shapes=[
            pltpu.VMEM((rows, width), F32), pltpu.VMEM((rows, width), BF),
            pltpu.VMEM((rows, width), BF), pltpu.VMEM((rows, ff), BF),
            pltpu.VMEM((rows, ff), BF), pltpu.VMEM((rows, 1), F32),
        ],
        compiler_params=params(),
        name="middle",
    )(mixed, tokens, cot, w_out, w_up, w_down, vectors, ff_bias)


def head_kernel(scale, pairs, tab, *refs):
    n = 5
    bias_rows, norm_gains, ff_bias, raw, raw_cot = refs[:5]
    shards = (None,) + refs[5 : n + 4]
    fulls = (None,) + refs[n + 4 : 2 * n + 3]
    projected, mixed, long_hbm, short_hbm, tokens, cot, vectors, wide_bias = refs[2 * n + 3 : 2 * n + 11]
    ssem, rsem, lsem, osem, bias, long_buf, short_buf, tile, small, small_full = refs[2 * n + 11 :]
    shards = (small,) + shards[1:]
    fulls = (small_full,) + fulls[1:]
    kept, cut = bias_rows.shape
    tile[...] = jnp.zeros_like(tile)
    tile[0:kept, 0:cut] = bias_rows[...].astype(F32)
    tile[kept : kept + 2, 0:cut] = norm_gains[...].astype(F32)
    pieces = ff_bias.shape[1] // 128
    for j in range(pieces):
        tile[8 + j : 9 + j, :] = ff_bias[:, j * 128 : (j + 1) * 128].astype(F32)
    small[...] = jnp.zeros_like(small)
    small[0, 0] = tile[...].astype(BF)
    z, y, x, c = place_of()
    zs, yp, xp, cp = peers(z, y, x, c)
    greet(zs, yp, xp, cp)
    width = tokens.shape[1]
    two = 2 * HD
    sent = []

    def go(w, i, src, dst, peer):
        copy = remote(src, dst, ssem.at[w, i], rsem.at[w, i], peer)
        copy.start()
        sent.append(copy)

    def arrive(w, i, ref):
        remote(ref, ref, ssem.at[w, i], rsem.at[w, i], cp).wait_recv()

    def local(w):
        return pltpu.make_async_copy(shards[w], fulls[w].at[z, y], lsem.at[w])

    def near(w):
        local(w).start()
        src = shards[w].at[c, pl.ds(x, 2)]
        dst = fulls[w].at[z, y, c, pl.ds(x, 2)]
        for k in range(3):
            go(w, k, src, dst, zs[k])
        go(w, 3, src, dst, yp)

    def mid_at(w, k):
        zk = (z + 3 - k) % 4
        part = fulls[w].at[zk, y, c, pl.ds(x, 2)]
        arrive(w, k, part)
        go(w, 4 + k, part, part, yp)
        q = fulls[w].at[zk, y, c, 2 * x]
        go(w, 7 + k, q, q, xp)

    def far_at(w, k):
        zk = (z + 4 - k) % 4
        part = fulls[w].at[zk, 1 - y, c, pl.ds(x, 2)]
        arrive(w, 3 + k, part)
        q = fulls[w].at[zk, 1 - y, c, 2 * x]
        go(w, 10 + k, q, q, xp)

    def mid(w):
        for k in range(3):
            mid_at(w, k)

    def far(w):
        for k in range(4):
            far_at(w, k)

    def across(w):
        for k in range(7):
            zk, yk = ((z + 3 - k) % 4, y) if k < 3 else ((z + 7 - k) % 4, 1 - y)
            arrive(w, 7 + k, fulls[w].at[zk, yk, c, 2 * (1 - x)])
            part = fulls[w].at[zk, yk, c]
            go(w, 14 + k, part, part, cp)

    def last(w):
        for k in range(7):
            zk, yk = ((z + 3 - k) % 4, y) if k < 3 else ((z + 7 - k) % 4, 1 - y)
            arrive(w, 14 + k, fulls[w].at[zk, yk, 1 - c])
        local(w).wait()

    def project():
        rows = [fulls[0][i // 2, i % 2, 0, 0].astype(F32) for i in range(8)]
        vectors[...] = jnp.concatenate([r[0:8, 0:cut] for r in rows], 1)
        wide_bias[...] = jnp.concatenate([r[8 + j : 9 + j, :] for r in rows for j in range(pieces)], 1)
        bias[...] = jnp.zeros_like(bias)
        bias[:, 0:width] = vectors[0:1, :]
        bias[:, 2 * width :] = vectors[1:2, :]
        span = width // 2

        @pl.loop(0, 6)
        def _(j):
            cols = pl.ds(pl.multiple_of(j * span, span), span)
            part = fulls[1][:, :, :, :, :, cols].reshape(width, span)
            projected[:, cols] = (dot(tokens[...], part) + bias[:, cols]).astype(BF)

    def store(i):
        return (
            pltpu.make_async_copy(long_buf.at[i % 2], long_hbm.at[2 * i : 2 * i + 2], osem.at[i % 2]),
            pltpu.make_async_copy(short_buf.at[i % 2], short_hbm.at[2 * i : 2 * i + 2], osem.at[2 + i % 2]),
        )

    def attend_at(i):
        if i >= 2:
            for copy in store(i - 2):
                copy.wait()
        at = pl.ds(i * two, two)
        attend_kernel(
            scale, tab,
            projected.at[:, at],
            projected.at[:, pl.ds(width + i * two, two)],
            projected.at[:, pl.ds(2 * width + i * two, two)],
            mixed.at[:, at], long_buf.at[i % 2], short_buf.at[i % 2],
        )
        for copy in store(i):
            copy.start()

    for w in (0, 1, 3, 4, 2):
        near(w)
    fill_selection(tab, long_buf, False)
    move_rows(long_buf, [raw], tokens)
    move_rows(long_buf, [raw_cot], cot)
    mid(0)
    mid(1)
    far(0)
    far(1)
    across(0)
    across(1)
    last(0)
    last(1)
    project()
    mid_at(3, 0)
    attend_at(0)
    mid_at(3, 1)
    mid_at(3, 2)
    attend_at(1)
    far_at(3, 0)
    attend_at(2)
    far_at(3, 1)
    attend_at(3)
    mid_at(4, 0)
    far_at(3, 2)
    attend_at(4)
    mid_at(4, 1)
    far_at(3, 3)
    attend_at(5)
    far_at(4, 0)
    mid_at(4, 2)
    across(3)
    far_at(4, 1)
    mid(2)
    far_at(4, 2)
    far_at(4, 3)
    far(2)
    last(3)
    across(4)
    across(2)
    last(4)
    last(2)
    for i in (pairs - 2, pairs - 1):
        for copy in store(i):
            copy.wait()
    for copy in sent:
        copy.wait_send()


def head(tab, bias_rows, norm_gains, ff_bias, shards, tokens, cotangent):
    n = len(shards) + 1
    views = [blocks(s) for s in shards]
    rows, width = tokens.shape
    pairs = width // (2 * HD)
    shape = jax.ShapeDtypeStruct
    anywhere = pl.BlockSpec(memory_space=pl.ANY)
    results = pl.pallas_call(
        functools.partial(head_kernel, HD ** (-0.5), pairs),
        out_shape=[shape((4, 2) + v.shape, v.dtype) for v in views]
        + [
            shape((rows, 3 * width), BF), shape((rows, width), BF),
            shape((2 * pairs, LONG, LONG), BF), shape((2 * pairs, rows - LONG, 2 * SHORT), BF),
            shape((rows, width), BF), shape((rows, width), BF),
            shape((8, width), F32), shape((1, 8 * ff_bias.shape[0]), F32),
        ],
        in_specs=[sm()] + [vm()] * (n + 4),
        out_specs=[vm()] + [anywhere] * 3 + [vm()] * 2 + [anywhere] * 2 + [vm()] * 4,
        scratch_shapes=[
            pltpu.SemaphoreType.DMA((n, 21)), pltpu.SemaphoreType.DMA((n, 21)),
            pltpu.SemaphoreType.DMA((n,)), pltpu.SemaphoreType.DMA((4,)),
            pltpu.VMEM((1, 3 * width), F32),
            pltpu.VMEM((2, 2, LONG, LONG), BF), pltpu.VMEM((2, 2, rows - LONG, 2 * SHORT), BF),
            pltpu.VMEM((16, 128), F32), pltpu.VMEM((2, 3, 16, 128), BF),
            pltpu.VMEM((4, 2, 2, 3, 16, 128), BF),
        ],
        compiler_params=params(collective_id=0, has_side_effects=True),
        name="head",
    )(tab, bias_rows, norm_gains, ff_bias[None], tokens, cotangent, *views)
    return [f.reshape(8 * s.shape[0], s.shape[1]) for f, s in zip(results, shards)], results[n - 1 :]


def tail_kernel(scale, pairs, tab, *refs):
    d_down, d_up, d_out, sums, d_ffb, projected, g_mixed, tokens, grad_one, long_hbm, short_hbm, w_hbm = refs[:12]
    outs, grad_tokens = refs[12:17], refs[17]
    own = refs[18:]
    n = 5
    half, rx, rpy, rqy, rpz, rqz, rpx, fin, got = (own[i * n : (i + 1) * n] for i in range(9))
    ssem, rsem, lsem, d_qkv, small, heads, long_buf, short_buf, w_qkv = own[9 * n :]
    grads = [d_down, d_up, d_out, d_qkv, small]
    z, y, x, c = place_of()
    zs, yp, xp, cp = peers(z, y, x, c)
    width = tokens.shape[1]
    two = 2 * HD
    sent = []

    def fetch(i):
        return (
            pltpu.make_async_copy(long_hbm.at[2 * i : 2 * i + 2], long_buf.at[i % 2], lsem.at[i % 2]),
            pltpu.make_async_copy(short_hbm.at[2 * i : 2 * i + 2], short_buf.at[i % 2], lsem.at[2 + i % 2]),
        )

    weights = pltpu.make_async_copy(w_hbm, w_qkv, lsem.at[4])
    weights.start()
    for copy in fetch(0):
        copy.start()
    small[...] = jnp.zeros_like(small)
    cut, long_cut = sums.shape[1] // 8, d_ffb.shape[1] // 8
    for i in range(8):
        at = slice(i * cut, (i + 1) * cut)
        small[i // 2, i % 2, 0, 0, 2:6, 0:cut] = sums[2:6, at]
        small[i // 2, i % 2, 0, 0, 6:8, 0:cut] = sums[0:2, at]
        for j in range(long_cut // 128):
            first = i * long_cut + j * 128
            small[i // 2, i % 2, 0, 1, j : j + 1, :] = d_ffb[:, first : first + 128]
    greet(zs, yp, xp, cp)

    def go(w, i, src, dst, peer):
        copy = remote(src, dst, ssem.at[w, i], rsem.at[w, i], peer)
        copy.start()
        sent.append(copy)

    def arrive(w, i, ref):
        remote(ref, ref, ssem.at[w, i], rsem.at[w, i], cp).wait_recv()

    def add(*parts):
        total = parts[0].astype(F32)
        for part in parts[1:]:
            total = total + part.astype(F32)
        return total

    def s0(w):
        go(w, 0, grads[w].at[:, :, 1 - c], half[w], cp)

    def s1(w):
        arrive(w, 0, half[w])
        a = half[w]

        @pl.loop(0, 4)
        def _(i):
            for j in range(2):
                for k in range(3):
                    a[i, j, k] = add(grads[w][i, j, c, k], a[i, j, k]).astype(a.dtype)

        go(w, 1, a.at[:, :, 2 * (1 - x)], rx[w], xp)
        go(w, 2, a.at[:, 1 - y, 1], rpy[w], yp)

    def s2p(w):
        a = half[w]
        arrive(w, 2, rpy[w])

        @pl.loop(0, 4)
        def _(i):
            a[i, y, 1] = add(a[i, y, 1], rpy[w][i]).astype(a.dtype)

        for k in range(3):
            go(w, 3 + k, a.at[(z + k + 1) % 4, y, 1], rpz[w].at[k], zs[k])

    def s2q(w):
        a = half[w]
        arrive(w, 1, rx[w])

        @pl.loop(0, 4)
        def _(i):
            for j in range(2):
                a[i, j, 2 * x] = add(a[i, j, 2 * x], rx[w][i, j]).astype(a.dtype)

        go(w, 6, a.at[:, 1 - y, 2 * x], rqy[w], yp)

    def s3p(w):
        a = half[w]
        for k in range(3):
            arrive(w, 3 + k, rpz[w].at[k])
        a[z, y, 1] = add(a[z, y, 1], rpz[w][0], rpz[w][1], rpz[w][2]).astype(a.dtype)
        go(w, 10, a.at[z, y, 1], rpx[w], xp)

    def s3q(w):
        a = half[w]
        arrive(w, 6, rqy[w])

        @pl.loop(0, 4)
        def _(i):
            a[i, y, 2 * x] = add(a[i, y, 2 * x], rqy[w][i]).astype(a.dtype)

        for k in range(3):
            go(w, 7 + k, a.at[(z + k + 1) % 4, y, 2 * x], rqz[w].at[k], zs[k])

    def s4p(w):
        a = half[w]
        arrive(w, 10, rpx[w])
        fin[w][1] = add(a[z, y, 1], rpx[w][...]).astype(a.dtype)
        go(w, 14, fin[w].at[1], got[w].at[c, 1], cp)

    def s4q(w):
        a = half[w]
        for k in range(3):
            arrive(w, 7 + k, rqz[w].at[k])
        fin[w][0] = add(a[z, y, 2 * x], rqz[w][0], rqz[w][1], rqz[w][2]).astype(a.dtype)
        go(w, 11, fin[w].at[0], got[w].at[c, 2 * x], xp)
        go(w, 13, fin[w].at[0], got[w].at[c, 2 * x], cp)

    def s5(w):
        arrive(w, 11, got[w].at[c, 2 * (1 - x)])
        piece = got[w].at[c, 2 * (1 - x)]
        go(w, 12, piece, piece, cp)
        outs[w][c, 2 * x] = fin[w][0].astype(F32)
        outs[w][c, 1] = fin[w][1].astype(F32)
        outs[w][c, 2 * (1 - x)] = got[w][c, 2 * (1 - x)].astype(F32)

    def s6(w):
        arrive(w, 12, got[w].at[1 - c, 2 * (1 - x)])
        arrive(w, 13, got[w].at[1 - c, 2 * x])
        arrive(w, 14, got[w].at[1 - c, 1])
        for k in range(3):
            outs[w][1 - c, k] = got[w][1 - c, k].astype(F32)

    def back(i):
        if i + 1 < pairs:
            for copy in fetch(i + 1):
                copy.start()
        for copy in fetch(i):
            copy.wait()
        at = pl.ds(i * two, two)
        attend_back_kernel(
            scale,
            projected.at[:, at],
            projected.at[:, pl.ds(width + i * two, two)],
            projected.at[:, pl.ds(2 * width + i * two, two)],
            g_mixed.at[:, at],
            long_buf.at[i % 2], short_buf.at[i % 2],
            heads.at[:, :, at],
        )

    def weight(k):
        part = 256
        for j in range(width // part):
            at = slice(j * part, (j + 1) * part)
            value = dot(tokens[...], heads[k, :, at], TN).astype(BF)
            d_qkv[:, :, :, :, :, k * width + j * part : k * width + (j + 1) * part] = value.reshape(
                d_qkv.shape[:5] + (part,)
            )
        if k != 1:
            total = jnp.sum(heads[k].astype(F32), axis=0, keepdims=True)
            for i in range(8):
                row = k // 2
                small[i // 2, i % 2, 0, 0, row : row + 1, 0:cut] = total[:, i * cut : (i + 1) * cut]

    def rows_back(i):
        step = tokens.shape[0] // 4
        at = slice(i * step, (i + 1) * step)
        total = grad_one[at, :]
        for k in range(3):
            total = total + dot(heads[k, at, :], w_qkv[:, k * width : (k + 1) * width], NT)
        for k in range(3):
            part = total.astype(BF)
            total = total - part.astype(F32)
            heads[k, at, :] = part

    def select(_):
        fill_selection(tab, long_buf, True)

    def token_rows(_):
        move_rows(long_buf, [heads.at[0], heads.at[1], heads.at[2]], grad_tokens)

    def run(*steps):
        for f, *which in steps:
            for w in which:
                f(w)

    run(
        (s0, 0, 1, 2), (back, 0, 1), (s1, 0), (back, 2), (s1, 1), (back, 3, 4), (s2p, 0), (back, 5),
        (s2p, 1), (weight, 0), (s2q, 0), (weight, 1, 2), (s0, 3, 4), (s3p, 0), (s3q, 0), (select, 0),
    )
    weights.wait()
    run(
        (rows_back, 0), (s1, 3, 2, 4), (s3p, 1), (s4q, 0), (s4p, 0), (rows_back, 1), (s2q, 1),
        (s2p, 3, 2, 4), (rows_back, 2), (s3q, 1), (s4p, 1), (s5, 0), (rows_back, 3), (token_rows, 0), (s2q, 3),
        (s3p, 3, 2, 4), (s4q, 1), (s2q, 2, 4), (s3q, 3), (s5, 1), (s3q, 2, 4), (s4p, 3, 2, 4),
        (s6, 0), (s4q, 3), (s6, 1), (s4q, 2, 4), (s5, 3, 2, 4), (s6, 3, 2, 4),
    )
    for copy in sent:
        copy.wait_send()


def tail(tab, d_down, d_up, d_out, sums, d_ffb, projected, g_mixed, tokens, grad_one, long_probs, short_probs, w_qkv):
    rows, wide = projected.shape
    width = wide // 3
    pairs = width // (2 * HD)

    def view(shape):
        return (4, 2, 2, 3, shape[0] // 48, shape[1])

    views = [g.reshape(view(g.shape)) for g in (d_down, d_up, d_out)]
    small_view = (4, 2, 2, 3, 8, 128)
    qkv_view = view(w_qkv.shape)
    kinds = [(v.shape, v.dtype) for v in views[:3]] + [(qkv_view, BF), (small_view, F32)]
    lead = ((4, 2, 3), (4, 2), (4,), (4,), (3,), (3,), (), (2,), (2, 3))
    scratch = [pltpu.VMEM(s + v[4:], t) for s in lead for v, t in kinds]
    anywhere = pl.BlockSpec(memory_space=pl.ANY)
    results = pl.pallas_call(
        functools.partial(tail_kernel, HD ** (-0.5), pairs),
        out_shape=[jax.ShapeDtypeStruct(v[2:], F32) for v, _ in kinds]
        + [jax.ShapeDtypeStruct((rows, width), F32)],
        in_specs=[sm()] + [vm()] * 9 + [anywhere] * 3,
        out_specs=[vm()] * 6,
        scratch_shapes=scratch
        + [
            pltpu.SemaphoreType.DMA((5, 15)), pltpu.SemaphoreType.DMA((5, 15)),
            pltpu.SemaphoreType.DMA((5,)),
            pltpu.VMEM(qkv_view, BF), pltpu.VMEM(small_view, F32),
            pltpu.VMEM((3, rows, width), BF),
            pltpu.VMEM((2, 2) + long_probs.shape[1:], BF),
            pltpu.VMEM((2, 2) + short_probs.shape[1:], BF),
            pltpu.VMEM(w_qkv.shape, BF),
        ],
        compiler_params=params(collective_id=1, has_side_effects=True),
        name="tail",
    )(tab, *views, sums, d_ffb, projected, g_mixed, tokens, grad_one, long_probs, short_probs, w_qkv)
    flat = [o.reshape(-1, o.shape[-1]) for o in results[:5]]
    return flat, results[5]


def square():
    return lax.axis_size("dp") == 8 and lax.axis_size("rep") == 4


def front_layer(tab, tokens, cotangent, qkv_weight, out_weight, up_weight, down_weight, norm_gains, bias_rows, ff_bias):
    width = tokens.shape[1]
    if not square():
        tokens, cotangent = permute(tab, tokens, False), permute(tab, cotangent, False)
        w_qkv, w_out, w_up, w_down = (
            lax.all_gather(w, "dp", axis=0, tiled=True)
            for w in (qkv_weight, out_weight, up_weight, down_weight)
        )
        gains = lax.all_gather(norm_gains, "dp", axis=1, tiled=True)
        biases = lax.all_gather(bias_rows, "dp", axis=1, tiled=True)
        up_bias = lax.all_gather(ff_bias, "dp", axis=0, tiled=True)
        wide = biases.astype(F32)
        bias = jnp.concatenate([wide[0], jnp.zeros((width,), F32), wide[1]])
        projected = (dot(tokens, w_qkv) + bias).astype(BF)
        mixed, *probs = attend(tab, projected)
        return (
            w_qkv, w_out, w_up, w_down,
            jnp.concatenate([biases, gains]).astype(F32), up_bias.astype(F32)[None],
            tokens, cotangent, projected, mixed, tuple(probs),
        )

    full, (projected, mixed, *probs, tokens, cotangent, vectors, up_bias) = head(
        tab, bias_rows, norm_gains, ff_bias, [qkv_weight, out_weight, up_weight, down_weight], tokens, cotangent
    )
    return (*full, vectors, up_bias, tokens, cotangent, projected, mixed, tuple(probs))


def reduce_layer(d_qkv, d_out, d_up, d_down, d_gains, d_biases, d_up_bias):
    def full(g):
        part = lax.psum_scatter(g, "rep", scatter_dimension=1, tiled=True).astype(F32)
        part = lax.psum_scatter(part, "dp", scatter_dimension=0, tiled=True)
        return lax.all_gather(part.astype(BF), "rep", axis=1, tiled=True).astype(F32)

    small = lax.psum(
        (
            lax.psum_scatter(d_gains, "dp", scatter_dimension=1, tiled=True),
            lax.psum_scatter(d_biases, "dp", scatter_dimension=1, tiled=True),
            lax.psum_scatter(d_up_bias, "dp", scatter_dimension=0, tiled=True),
        ),
        "rep",
    )
    return tuple(full(g.astype(BF)) for g in (d_qkv, d_out, d_up, d_down)) + small


def back_layer(tab, final, projected, grad_mixed, probs, tokens, grad_one, w_qkv, d_out, d_up, d_down, sums, d_up_bias):
    width = tokens.shape[1]
    if not square():
        parts = attend_back(projected, grad_mixed, *probs)
        grad_heads = jnp.concatenate([parts[0], parts[1], parts[2]], 1)
        d_head = jnp.sum(grad_heads.astype(F32), axis=0)[None]
        d_qkv = dot(tokens, grad_heads, TN)
        grad_tokens = grad_one + dot(grad_heads, w_qkv, NT)
        d_biases = jnp.concatenate([d_head[:, :width], d_head[:, 2 * width :], sums[2:6]])
        moved = (permute(tab, final, True), permute(tab, grad_tokens, True))
        return moved + reduce_layer(d_qkv, d_out, d_up, d_down, sums[0:2], d_biases, d_up_bias[0])

    (down, up, out, qkv, own), grad_tokens = tail(
        tab, d_down, d_up, d_out, sums, d_up_bias, projected, grad_mixed, tokens, grad_one, *probs, w_qkv
    )
    cut, pieces = width // 8, d_up_bias.shape[1] // (8 * 128)
    return (
        permute(tab, final, True), grad_tokens, qkv, out, up, down,
        own[6:8, :cut], own[0:6, :cut], own[8 : 8 + pieces].reshape(-1),
    )


def local(
    tokens,
    qkv_weight,
    out_weight,
    up_weight,
    down_weight,
    norm_gains,
    bias_rows,
    ff_bias,
    lengths,
    owners,
    cotangent,
):
    row_count = tokens.shape[0]
    device = lax.axis_index("dp") * lax.axis_size("rep") + lax.axis_index("rep")
    devices = lax.axis_size("dp") * lax.axis_size("rep")
    per = lengths.shape[0] // devices
    assert row_count == LONG + SHORT * (per - 1) == 2 * LONG
    me = device.astype(jnp.int32).reshape(1)
    tab = slot_table(me, owners, lengths, per)
    w_qkv, w_out, w_up, w_down, vectors, up_bias, tokens, cotangent, projected, mixed_rows, probs = front_layer(
        tab, tokens, cotangent, qkv_weight, out_weight, up_weight, down_weight, norm_gains, bias_rows, ff_bias
    )
    final, grad_one, grad_mixed, d_out, d_up, d_down, sums, d_up_bias = middle(
        mixed_rows, tokens, cotangent, w_out, w_up, w_down, vectors, up_bias
    )
    return back_layer(
        tab, final, projected, grad_mixed, probs, tokens, grad_one, w_qkv,
        d_out, d_up, d_down, sums, d_up_bias,
    )


def solution(mesh):
    in_specs = (
        P(("dp", "rep"), None),
        P("dp", None),
        P("dp", None),
        P("dp", None),
        P("dp", None),
        P(None, "dp"),
        P(None, "dp"),
        P("dp"),
        P(),
        P(),
        P(("dp", "rep"), None),
    )
    out_specs = (
        P(("dp", "rep"), None),
        P(("dp", "rep"), None),
        P("dp", None),
        P("dp", None),
        P("dp", None),
        P("dp", None),
        P(None, "dp"),
        P(None, "dp"),
        P("dp"),
    )
    return jax.shard_map(local, mesh=mesh, in_specs=in_specs, out_specs=out_specs, check_vma=False)
```
